8 devices in a mesh: fsdp: 8 (over z, y, x, core).
Axes of the slice: x: 2, y: 2, z: 1, core: 2. Of those that a mesh axis runs over, the one named last changes fastest.
Arguments:
- w_query: float32 [2, 576, 576], P(None, 'fsdp')
- w_key: float32 [2, 576, 192], P(None, 'fsdp')
- w_value: float32 [2, 576, 192], P(None, 'fsdp')
- w_out: float32 [2, 576, 576], P(None, 'fsdp')
- w_gate: float32 [2, 576, 1536], P(None, 'fsdp')
- w_up: float32 [2, 576, 1536], P(None, 'fsdp')
- w_down: float32 [2, 1536, 576], P(None, 'fsdp')
- gain_attn: float32 [2, 576], P(None, 'fsdp')
- gain_mlp: float32 [2, 576], P(None, 'fsdp')
- rope_cos: float32 [256, 32], replicated
- rope_sin: float32 [256, 32], replicated
- x_in: bfloat16 [32, 256, 576], P('fsdp')
- y_cot: bfloat16 [32, 256, 576], P('fsdp')
Outputs:
- output 1: bfloat16 [32, 256, 576], P('fsdp')
- output 2: bfloat16 [32, 256, 576], P('fsdp')
- output 3: float32 [2, 576, 576], P(None, 'fsdp')
- output 4: float32 [2, 576, 192], P(None, 'fsdp')
- output 5: float32 [2, 576, 192], P(None, 'fsdp')
- output 6: float32 [2, 576, 576], P(None, 'fsdp')
- output 7: float32 [2, 576, 1536], P(None, 'fsdp')
- output 8: float32 [2, 576, 1536], P(None, 'fsdp')
- output 9: float32 [2, 1536, 576], P(None, 'fsdp')
- output 10: float32 [2, 576], P(None, 'fsdp')
- output 11: float32 [2, 576], P(None, 'fsdp')
All inputs are finite; a program needn't handle non-finite values.
Results may differ from the reference program's by a relative error of at most 0.02.
Values are sent between devices in bfloat16 or wider.
A program may use at most 1 GiB of HBM per device.

```python
import jax
import jax.numpy as jnp
from jax import lax

MODEL_DIM = 576
FFN_DIM = 1536
HEADS = 9
KV_HEADS = 3
HEAD_DIM = 64
SEQ_LEN = 256
TOTAL_BATCH = 32
LAYERS = 2
NORM_EPS = 1e-5
GROUP_SIZE = HEADS // KV_HEADS
HALF_DIM = HEAD_DIM // 2
Q_WIDTH = HEADS * HEAD_DIM
KV_WIDTH = KV_HEADS * HEAD_DIM


def setup_inputs(seed: int = 0) -> dict:
    key_list = jax.random.split(jax.random.key(seed), 13)

    def draw_weight(rng_key, shape, fan_in):
        return jax.random.normal(rng_key, shape, jnp.float32) * fan_in ** -0.5

    offset = jax.random.randint(key_list[9], (), 0, 4096).astype(jnp.float32)
    jitter = jnp.exp(0.1 * jax.random.normal(key_list[10], (HALF_DIM,), jnp.float32))
    inv_freq = 10000.0 ** (-jnp.arange(HALF_DIM, dtype=jnp.float32) / HALF_DIM) * jitter
    angles = (jnp.arange(SEQ_LEN, dtype=jnp.float32) + offset)[:, None] * inv_freq[None, :]
    tok_shape = (TOTAL_BATCH, SEQ_LEN, MODEL_DIM)
    return {
        "w_query": draw_weight(key_list[0], (LAYERS, MODEL_DIM, Q_WIDTH), MODEL_DIM),
        "w_key": draw_weight(key_list[1], (LAYERS, MODEL_DIM, KV_WIDTH), MODEL_DIM),
        "w_value": draw_weight(key_list[2], (LAYERS, MODEL_DIM, KV_WIDTH), MODEL_DIM),
        "w_out": draw_weight(key_list[3], (LAYERS, Q_WIDTH, MODEL_DIM), Q_WIDTH),
        "w_gate": draw_weight(key_list[4], (LAYERS, MODEL_DIM, FFN_DIM), MODEL_DIM),
        "w_up": draw_weight(key_list[5], (LAYERS, MODEL_DIM, FFN_DIM), MODEL_DIM),
        "w_down": draw_weight(key_list[6], (LAYERS, FFN_DIM, MODEL_DIM), FFN_DIM),
        "gain_attn": 1.0 + 0.2 * jax.random.normal(key_list[7], (LAYERS, MODEL_DIM), jnp.float32),
        "gain_mlp": 1.0 + 0.2 * jax.random.normal(key_list[8], (LAYERS, MODEL_DIM), jnp.float32),
        "rope_cos": jnp.cos(angles),
        "rope_sin": jnp.sin(angles),
        "x_in": jax.random.normal(key_list[11], tok_shape, jnp.float32).astype(jnp.bfloat16),
        "y_cot": jax.random.normal(key_list[12], tok_shape, jnp.float32).astype(jnp.bfloat16),
    }


def rms_norm(values, gain):
    vals32 = values.astype(jnp.float32)
    inv_rms = lax.rsqrt(jnp.mean(vals32 * vals32, axis=-1, keepdims=True) + NORM_EPS)
    return (vals32 * inv_rms * gain.astype(jnp.float32)).astype(jnp.bfloat16)


def apply_rope(heads32, rope_cos, rope_sin):
    first_half = heads32[..., :HALF_DIM]
    second_half = heads32[..., HALF_DIM:]
    cos_b = rope_cos[:, None, :]
    sin_b = rope_sin[:, None, :]
    return jnp.concatenate([first_half * cos_b - second_half * sin_b, second_half * cos_b + first_half * sin_b], axis=-1)


def layer_forward(weights, rope_cos, rope_sin, hidden):
    w_query, w_key, w_value, w_out, w_gate, w_up, w_down, gain_attn, gain_mlp = weights
    normed = rms_norm(hidden, gain_attn)
    q_proj = jnp.dot(normed, w_query, preferred_element_type=jnp.float32).reshape(SEQ_LEN, HEADS, HEAD_DIM)
    q_heads = apply_rope(q_proj, rope_cos, rope_sin).astype(jnp.bfloat16).reshape(SEQ_LEN, KV_HEADS, GROUP_SIZE, HEAD_DIM)
    k_proj = jnp.dot(normed, w_key, preferred_element_type=jnp.float32).reshape(SEQ_LEN, KV_HEADS, HEAD_DIM)
    k_heads = apply_rope(k_proj, rope_cos, rope_sin).astype(jnp.bfloat16)
    v_heads = jnp.dot(normed, w_value, preferred_element_type=jnp.float32).astype(jnp.bfloat16).reshape(SEQ_LEN, KV_HEADS, HEAD_DIM)
    scores = jnp.einsum("qkgd,skd->kgqs", q_heads.astype(jnp.float32), k_heads.astype(jnp.float32)) * HEAD_DIM ** -0.5
    positions = jnp.arange(SEQ_LEN)
    scores = jnp.where(positions[:, None] >= positions[None, :], scores, -1e30)
    attn_probs = jax.nn.softmax(scores, axis=-1).astype(jnp.bfloat16)
    attn_heads = jnp.einsum("kgqs,skd->qkgd", attn_probs.astype(jnp.float32), v_heads.astype(jnp.float32))
    attn_heads = attn_heads.astype(jnp.bfloat16).reshape(SEQ_LEN, Q_WIDTH)
    mid_hidden = (hidden.astype(jnp.float32) + jnp.dot(attn_heads, w_out, preferred_element_type=jnp.float32)).astype(jnp.bfloat16)
    normed_mlp = rms_norm(mid_hidden, gain_mlp)
    gate_pre = jnp.dot(normed_mlp, w_gate, preferred_element_type=jnp.float32)
    up_proj = jnp.dot(normed_mlp, w_up, preferred_element_type=jnp.float32)
    mlp_act = (jax.nn.silu(gate_pre) * up_proj).astype(jnp.bfloat16)
    return (mid_hidden.astype(jnp.float32) + jnp.dot(mlp_act, w_down, preferred_element_type=jnp.float32)).astype(jnp.bfloat16)


def reference(w_query, w_key, w_value, w_out, w_gate, w_up, w_down, gain_attn, gain_mlp, rope_cos, rope_sin, x_in, y_cot):
    masters = (w_query, w_key, w_value, w_out, w_gate, w_up, w_down, gain_attn, gain_mlp)
    params_bf = tuple(master.astype(jnp.bfloat16) for master in masters)

    def stack_forward(params, seq_x):
        def layer_body(hidden, layer_params):
            return layer_forward(layer_params, rope_cos, rope_sin, hidden), None
        return lax.scan(layer_body, seq_x, params)[0]

    def per_sequence(grad_sums, seq_pair):
        seq_x, seq_cot = seq_pair
        seq_y, pullback = jax.vjp(stack_forward, params_bf, seq_x)
        grad_params, grad_x = pullback(seq_cot)
        new_sums = tuple(old_sum + grad_part.astype(jnp.float32) for old_sum, grad_part in zip(grad_sums, grad_params))
        return new_sums, (seq_y, grad_x)

    grad_init = tuple(jnp.zeros(master.shape, jnp.float32) for master in masters)
    grads, outputs = lax.scan(per_sequence, grad_init, (x_in, y_cot))
    return (outputs[0], outputs[1], grads[0], grads[1], grads[2], grads[3], grads[4], grads[5], grads[6], grads[7], grads[8])
```

```python
import jax
import jax.numpy as jnp
from jax import lax
from jax.sharding import PartitionSpec as P

NORM_EPS = 1e-5
MASK_VALUE = -1e30


def rms_forward(values, gain):
    vals32 = values.astype(jnp.float32)
    inv_rms = lax.rsqrt(jnp.mean(vals32 * vals32, axis=-1, keepdims=True) + NORM_EPS)
    normed = (vals32 * inv_rms * gain.astype(jnp.float32)).astype(jnp.bfloat16)
    return normed, inv_rms


def rms_backward(values, inv_rms, gain, grad_normed):
    scaled = values.astype(jnp.float32) * inv_rms
    grad_scaled = grad_normed * gain.astype(jnp.float32)
    grad_gain = jnp.sum(grad_normed * scaled, axis=(0, 1))
    grad_values = inv_rms * (grad_scaled - scaled * jnp.mean(grad_scaled * scaled, axis=-1, keepdims=True))
    return grad_values, grad_gain


def rotary(heads32, rope_cos, rope_sin, sin_sign):
    half_dim = rope_cos.shape[-1]
    first_half = heads32[..., :half_dim]
    second_half = heads32[..., half_dim:]
    cos_b = rope_cos[None, :, None, :]
    sin_b = sin_sign * rope_sin[None, :, None, :]
    return jnp.concatenate([first_half * cos_b - second_half * sin_b, second_half * cos_b + first_half * sin_b], axis=-1)


def layer_forward(weights, rope_cos, rope_sin, hidden):
    w_query, w_key, w_value, w_out, w_gate, w_up, w_down, gain_attn, gain_mlp = weights
    batch_size = hidden.shape[0]
    seq_len = hidden.shape[1]
    head_dim = 2 * rope_cos.shape[-1]
    kv_heads = w_key.shape[1] // head_dim
    num_heads = w_query.shape[1] // head_dim
    group_size = num_heads // kv_heads
    normed, inv_rms_attn = rms_forward(hidden, gain_attn)
    q_proj = jnp.einsum("bsd,df->bsf", normed, w_query, preferred_element_type=jnp.float32)
    q_heads = rotary(q_proj.reshape(batch_size, seq_len, num_heads, head_dim), rope_cos, rope_sin, 1.0)
    q_heads = q_heads.astype(jnp.bfloat16).reshape(batch_size, seq_len, kv_heads, group_size, head_dim)
    k_proj = jnp.einsum("bsd,df->bsf", normed, w_key, preferred_element_type=jnp.float32)
    k_heads = rotary(k_proj.reshape(batch_size, seq_len, kv_heads, head_dim), rope_cos, rope_sin, 1.0).astype(jnp.bfloat16)
    v_heads = jnp.einsum("bsd,df->bsf", normed, w_value, preferred_element_type=jnp.float32)
    v_heads = v_heads.astype(jnp.bfloat16).reshape(batch_size, seq_len, kv_heads, head_dim)
    scores = jnp.einsum("bqkgd,bskd->bkgqs", q_heads, k_heads, preferred_element_type=jnp.float32) * head_dim ** -0.5
    positions = jnp.arange(seq_len)
    scores = jnp.where(positions[:, None] >= positions[None, :], scores, MASK_VALUE)
    attn_probs = jax.nn.softmax(scores, axis=-1).astype(jnp.bfloat16)
    attn_heads = jnp.einsum("bkgqs,bskd->bqkgd", attn_probs, v_heads, preferred_element_type=jnp.float32)
    attn_heads = attn_heads.astype(jnp.bfloat16).reshape(batch_size, seq_len, num_heads * head_dim)
    attn_proj = jnp.einsum("bsf,fd->bsd", attn_heads, w_out, preferred_element_type=jnp.float32)
    mid_hidden = (hidden.astype(jnp.float32) + attn_proj).astype(jnp.bfloat16)
    normed_mlp, inv_rms_mlp = rms_forward(mid_hidden, gain_mlp)
    gate_pre = jnp.einsum("bsd,df->bsf", normed_mlp, w_gate, preferred_element_type=jnp.float32)
    up_proj = jnp.einsum("bsd,df->bsf", normed_mlp, w_up, preferred_element_type=jnp.float32)
    mlp_act = (jax.nn.silu(gate_pre) * up_proj).astype(jnp.bfloat16)
    down_proj = jnp.einsum("bsf,fd->bsd", mlp_act, w_down, preferred_element_type=jnp.float32)
    out_hidden = (mid_hidden.astype(jnp.float32) + down_proj).astype(jnp.bfloat16)
    saved_acts = (hidden, inv_rms_attn, normed, q_heads, k_heads, v_heads, attn_probs, attn_heads, mid_hidden, inv_rms_mlp, normed_mlp, gate_pre, up_proj, mlp_act)
    return out_hidden, saved_acts


def layer_backward(weights, rope_cos, rope_sin, saved_acts, grad_out):
    w_query, w_key, w_value, w_out, w_gate, w_up, w_down, gain_attn, gain_mlp = weights
    (hidden, inv_rms_attn, normed, q_heads, k_heads, v_heads, attn_probs, attn_heads, mid_hidden, inv_rms_mlp, normed_mlp, gate_pre, up_proj, mlp_act) = saved_acts
    batch_size = hidden.shape[0]
    seq_len = hidden.shape[1]
    head_dim = 2 * rope_cos.shape[-1]
    kv_heads = k_heads.shape[2]
    num_heads = kv_heads * q_heads.shape[3]
    grad_w_down = jnp.einsum("bsf,bsd->fd", mlp_act, grad_out, preferred_element_type=jnp.float32)
    grad_act = jnp.einsum("bsd,fd->bsf", grad_out, w_down, preferred_element_type=jnp.float32)
    gate_sig = jax.nn.sigmoid(gate_pre)
    grad_up = (grad_act * gate_pre * gate_sig).astype(jnp.bfloat16)
    grad_gate = (grad_act * up_proj * gate_sig * (1.0 + gate_pre * (1.0 - gate_sig))).astype(jnp.bfloat16)
    grad_w_gate = jnp.einsum("bsd,bsf->df", normed_mlp, grad_gate, preferred_element_type=jnp.float32)
    grad_w_up = jnp.einsum("bsd,bsf->df", normed_mlp, grad_up, preferred_element_type=jnp.float32)
    grad_normed_mlp = (jnp.einsum("bsf,df->bsd", grad_gate, w_gate, preferred_element_type=jnp.float32)
                       + jnp.einsum("bsf,df->bsd", grad_up, w_up, preferred_element_type=jnp.float32))
    grad_mid_norm, grad_gain_mlp = rms_backward(mid_hidden, inv_rms_mlp, gain_mlp, grad_normed_mlp)
    grad_mid = grad_out.astype(jnp.float32) + grad_mid_norm
    grad_mid_bf = grad_mid.astype(jnp.bfloat16)
    grad_w_out = jnp.einsum("bsf,bsd->fd", attn_heads, grad_mid_bf, preferred_element_type=jnp.float32)
    grad_attn = jnp.einsum("bsd,fd->bsf", grad_mid_bf, w_out, preferred_element_type=jnp.float32)
    grad_attn = grad_attn.astype(jnp.bfloat16).reshape(batch_size, seq_len, kv_heads, -1, head_dim)
    grad_v = jnp.einsum("bkgqs,bqkgd->bskd", attn_probs, grad_attn, preferred_element_type=jnp.float32)
    grad_v = grad_v.astype(jnp.bfloat16).reshape(batch_size, seq_len, -1)
    grad_probs = jnp.einsum("bqkgd,bskd->bkgqs", grad_attn, v_heads, preferred_element_type=jnp.float32)
    probs32 = attn_probs.astype(jnp.float32)
    grad_scores = probs32 * (grad_probs - jnp.sum(probs32 * grad_probs, axis=-1, keepdims=True)) * head_dim ** -0.5
    grad_scores = grad_scores.astype(jnp.bfloat16)
    grad_q = jnp.einsum("bkgqs,bskd->bqkgd", grad_scores, k_heads, preferred_element_type=jnp.float32)
    grad_q = rotary(grad_q.reshape(batch_size, seq_len, num_heads, head_dim), rope_cos, rope_sin, -1.0)
    grad_q = grad_q.astype(jnp.bfloat16).reshape(batch_size, seq_len, -1)
    grad_k = jnp.einsum("bkgqs,bqkgd->bskd", grad_scores, q_heads, preferred_element_type=jnp.float32)
    grad_k = rotary(grad_k, rope_cos, rope_sin, -1.0).astype(jnp.bfloat16).reshape(batch_size, seq_len, -1)
    grad_w_query = jnp.einsum("bsd,bsf->df", normed, grad_q, preferred_element_type=jnp.float32)
    grad_w_key = jnp.einsum("bsd,bsf->df", normed, grad_k, preferred_element_type=jnp.float32)
    grad_w_value = jnp.einsum("bsd,bsf->df", normed, grad_v, preferred_element_type=jnp.float32)
    grad_normed = (jnp.einsum("bsf,df->bsd", grad_q, w_query, preferred_element_type=jnp.float32)
                   + jnp.einsum("bsf,df->bsd", grad_k, w_key, preferred_element_type=jnp.float32)
                   + jnp.einsum("bsf,df->bsd", grad_v, w_value, preferred_element_type=jnp.float32))
    grad_hidden_norm, grad_gain_attn = rms_backward(hidden, inv_rms_attn, gain_attn, grad_normed)
    grad_hidden = (grad_mid + grad_hidden_norm).astype(jnp.bfloat16)
    layer_grads = (grad_w_query, grad_w_key, grad_w_value, grad_w_out, grad_w_gate, grad_w_up, grad_w_down, grad_gain_attn, grad_gain_mlp)
    return grad_hidden, layer_grads


def flip(axis_bit):
    return [(dev, dev ^ axis_bit) for dev in range(8)]


def exchange(values, axis_bit):
    return lax.ppermute(values, "fsdp", flip(axis_bit))


def pick(stacked, index, axis):
    return lax.dynamic_index_in_dim(stacked, index, axis, keepdims=False)


def join(own, other, bit):
    first = jnp.where(bit == 0, own, other)
    second = jnp.where(bit == 0, other, own)
    return jnp.stack([first, second])


def gather(shard, bits, x_first):
    core, x_bit, y_bit = bits
    if x_first:
        pair = join(shard, exchange(shard, 2), x_bit)
        quad = join(pair, exchange(pair, 4), y_bit)
    else:
        pair = join(shard, exchange(shard, 4), y_bit)
        quad = jnp.swapaxes(join(pair, exchange(pair, 2), x_bit), 0, 1)
    other = exchange(quad, 1)
    whole = jnp.where(core == 0, jnp.stack([quad, other], 2), jnp.stack([other, quad], 2))
    return whole.reshape((-1,) + shard.shape[1:])


def scatter(full, bits, x_first):
    core, x_bit, y_bit = bits
    blocks = full.reshape((2, 2, 2, full.shape[0] // 8) + full.shape[1:])
    mine = pick(blocks, core, 2)
    recv = exchange(pick(blocks, 1 - core, 2), 1)
    if x_first:
        bit_a, mask_a, axis_a, bit_b, mask_b = x_bit, 2, 1, y_bit, 4
    else:
        bit_a, mask_a, axis_a, bit_b, mask_b = y_bit, 4, 0, x_bit, 2
    recv_a = exchange(pick(mine, 1 - bit_a, axis_a) + pick(recv, 1 - bit_a, axis_a), mask_a)
    keep = pick(mine, bit_a, axis_a) + pick(recv, bit_a, axis_a) + recv_a
    recv_b = exchange(pick(keep, 1 - bit_b, 0), mask_b)
    return pick(keep, bit_b, 0) + recv_b


def solution(mesh):
    shard_spec = P(None, "fsdp")
    batch_spec = P("fsdp")

    def local_step(w_query, w_key, w_value, w_out, w_gate, w_up, w_down, gain_attn, gain_mlp, rope_cos, rope_sin, x_in, y_cot):
        me = lax.axis_index("fsdp")
        bits = (me % 2, (me // 2) % 2, me // 4)
        bf = jnp.bfloat16
        num_layers = w_query.shape[0]
        weights = []
        for i in range(num_layers):
            pad = jnp.zeros((w_query.shape[1], 62), jnp.float32)
            qkv = jnp.concatenate([w_query[i], w_key[i], w_value[i], gain_attn[i][:, None], gain_mlp[i][:, None], pad], 1).astype(bf)
            qkv = gather(qkv, bits, i == 0)
            out = gather(w_out[i].astype(bf), bits, i == 1)
            gate = gather(w_gate[i].astype(bf), bits, True)
            up = gather(w_up[i].astype(bf), bits, False)
            half = w_down.shape[1] // 2
            d0 = gather(w_down[i, :half].astype(bf), bits, True).reshape(8, half, -1)
            d1 = gather(w_down[i, half:].astype(bf), bits, False).reshape(8, half, -1)
            down = jnp.concatenate([d0, d1], 1).reshape(16 * half, -1)
            weights.append((qkv[:, :576], qkv[:, 576:768], qkv[:, 768:960], out, gate, up, down, qkv[:, 960], qkv[:, 961]))
        hidden = x_in
        saved_layers = []
        for layer_idx in range(num_layers):
            hidden, saved_acts = layer_forward(weights[layer_idx], rope_cos, rope_sin, hidden)
            saved_layers.append(saved_acts)
        grad_hidden = y_cot
        grads = [None] * num_layers
        for i in reversed(range(num_layers)):
            grad_hidden, g = layer_backward(weights[i], rope_cos, rope_sin, saved_layers[i], grad_hidden)
            gq, gk, gv, go, gg, gu, gd, ga, gm = g
            pad = jnp.zeros((gq.shape[0], 62), jnp.float32)
            qkv = scatter(jnp.concatenate([gq, gk, gv, ga[:, None], gm[:, None], pad], 1), bits, i == 0)
            out = scatter(go, bits, i == 1)
            gate = scatter(gg, bits, True)
            up = scatter(gu, bits, False)
            half = gd.shape[0] // 16
            gd = gd.reshape(8, 2, half, -1)
            d0 = scatter(gd[:, 0].reshape(8 * half, -1), bits, True)
            d1 = scatter(gd[:, 1].reshape(8 * half, -1), bits, False)
            grads[i] = (qkv[:, :576], qkv[:, 576:768], qkv[:, 768:960], out, gate, up, jnp.concatenate([d0, d1], 0), qkv[:, 960], qkv[:, 961])
        stacked = tuple(jnp.stack(parts) for parts in zip(*grads))
        return (hidden, grad_hidden) + stacked

    in_specs = (shard_spec,) * 9 + (P(), P(), batch_spec, batch_spec)
    out_specs = (batch_spec, batch_spec) + (shard_spec,) * 9
    return jax.shard_map(local_step, mesh=mesh, in_specs=in_specs, out_specs=out_specs, check_vma=False)
```

```python
import functools

import jax
import jax.numpy as jnp
from jax import lax
from jax.experimental import pallas as pl
from jax.experimental.pallas import tpu as pltpu
from jax.sharding import PartitionSpec as P

NORM_EPS = 1e-5
MASK_VALUE = -1e30
HEAD = 64
KV_HEADS = 3
GROUP = 3
SEQ = 256
DIM = 576
FFN = 1536
QKV = 960
BF = jnp.bfloat16
F32 = jnp.float32


def dot(a, b, dims=((1,), (0,))):
    return lax.dot_general(a, b, (dims, ((), ())), preferred_element_type=F32)


def params(**kw):
    return pltpu.CompilerParams(dimension_semantics=("arbitrary",), vmem_limit_bytes=60 * 1024 * 1024, **kw)


def cost(flops, bytes_accessed):
    return pl.CostEstimate(flops=int(flops), bytes_accessed=int(bytes_accessed), transcendentals=0)


def shape(dims, dtype):
    return jax.ShapeDtypeStruct(dims, dtype)


def whole(dims):
    return pl.BlockSpec(dims, lambda i: (0,) * len(dims))


def rows(dims):
    return pl.BlockSpec((1,) + dims, lambda i: (i,) + (0,) * len(dims))


def inv_rms(vals32):
    return lax.rsqrt(jnp.mean(vals32 * vals32, axis=-1, keepdims=True) + NORM_EPS)


def rms_back(vals32, inv, gain, grad_normed):
    scaled = vals32 * inv
    grad_scaled = grad_normed * gain
    grad_gain = jnp.sum(grad_normed * scaled, axis=0, keepdims=True)
    return inv * (grad_scaled - scaled * jnp.mean(grad_scaled * scaled, axis=-1, keepdims=True)), grad_gain


def rope(vals32, cos, sin):
    lane = lax.broadcasted_iota(jnp.int32, vals32.shape, 1)
    swapped = jnp.where(lane % HEAD < HEAD // 2, pltpu.roll(vals32, 96, 1), pltpu.roll(vals32, 32, 1))
    return vals32 * cos + swapped * sin


def attn_fwd_kernel(x_ref, wqkv_ref, wo_ref, gain_ref, cos_ref, sin_ref, h_ref, qkv_ref, p_ref, o_ref):
    x32 = x_ref[0].astype(F32)
    normed = (x32 * inv_rms(x32) * gain_ref[...]).astype(BF)
    proj = dot(normed, wqkv_ref[...])
    cos, sin = cos_ref[...], sin_ref[...]
    for i in range(6):
        qkv_ref[0, :, 128 * i:128 * (i + 1)] = rope(proj[:, 128 * i:128 * (i + 1)], cos, sin).astype(BF)
    qkv_ref[0, :, 768:QKV] = proj[:, 768:QKV].astype(BF)
    half = SEQ // 2
    causal = lax.broadcasted_iota(jnp.int32, (half, half), 0) >= lax.broadcasted_iota(jnp.int32, (half, half), 1)
    for kv in range(KV_HEADS):
        keys = qkv_ref[0, :, DIM + HEAD * kv:DIM + HEAD * (kv + 1)]
        vals = qkv_ref[0, :, 768 + HEAD * kv:768 + HEAD * (kv + 1)]
        for blk in range(2):
            lo, length = half * blk, half * (blk + 1)
            for g in range(GROUP):
                head = GROUP * kv + g
                q = qkv_ref[0, lo:lo + half, HEAD * head:HEAD * (head + 1)]
                s = dot(q, keys[:length], ((1,), (1,))) * HEAD ** -0.5
                diag = jnp.where(causal, s[:, lo:], MASK_VALUE)
                s = diag if blk == 0 else jnp.concatenate([s[:, :lo], diag], axis=1)
                e = jnp.exp(s - jnp.max(s, axis=-1, keepdims=True))
                p = (e * (1.0 / jnp.sum(e, axis=-1, keepdims=True))).astype(BF)
                p_ref[0, head, lo:lo + half, :length] = p
                o_ref[0, lo:lo + half, HEAD * head:HEAD * (head + 1)] = dot(p, vals[:length]).astype(BF)
    h_ref[0] = (x32 + dot(o_ref[0], wo_ref[...])).astype(BF)


def attn_fwd(x, wqkv, wo, gain, cos, sin):
    n = x.shape[0]
    return pl.pallas_call(
        attn_fwd_kernel,
        grid=(n,),
        in_specs=[rows((SEQ, DIM)), whole(wqkv.shape), whole(wo.shape), whole(gain.shape), whole(cos.shape), whole(sin.shape)],
        out_specs=[rows((SEQ, DIM)), rows((SEQ, QKV)), rows((9, SEQ, SEQ)), rows((SEQ, DIM))],
        out_shape=[shape((n, SEQ, DIM), BF), shape((n, SEQ, QKV), BF), shape((n, 9, SEQ, SEQ), BF), shape((n, SEQ, DIM), BF)],
        compiler_params=params(),
        cost_estimate=cost(5e9, 1e7),
        name="attn_fwd",
    )(x, wqkv, wo, gain, cos, sin)


MESH = pl.DeviceIdType.MESH
ANY = pl.BlockSpec(memory_space=pl.ANY)


class Part:
    def __init__(self, x_first, r, c, lo=0):
        self.x_first, self.r, self.c, self.lo = x_first, r, c, lo


def fused(body, steps, ins, in_specs, outs, out_specs, scratch, ca, bs, finish, cid, name, flops):
    n_ca, n_b = len(ca), len(bs)
    n_in, n_out, n_scr = len(ins), len(outs), len(scratch)
    comm = n_ca + n_b > 0
    last = steps - 1

    def kernel(*refs):
        refs = list(refs)
        take = lambda k: [refs.pop(0) for _ in range(k)]
        in_refs = take(n_in)
        ca_in = [take(2) for _ in range(n_ca)]
        b_in = take(n_b)
        out_refs = take(n_out)
        ca_out = take(n_ca)
        b_out = take(n_b)
        scr = take(n_scr)
        ca_scr = [take(4 if finish else 3) for _ in range(n_ca)]
        b_scr = [take(2) for _ in range(n_b)]
        step = pl.program_id(0)
        me = lax.axis_index("fsdp")
        core, x_bit, y_bit = lax.rem(me, 2), lax.rem(me // 2, 2), me // 4
        if not comm:
            body(step, last, core, in_refs, out_refs, scr)
            return
        s_mine, s_cs, s_cr, s_as, s_ar, s_bs, s_br, s_keep = take(8)
        pair, x_dev, y_dev = me + 1 - 2 * core, me + 2 - 4 * x_bit, me + 4 - 8 * y_bit

        def remote(src, dst, send, recv, dev):
            return pltpu.make_async_remote_copy(src_ref=src, dst_ref=dst, send_sem=send, recv_sem=recv, device_id=(dev,), device_id_type=MESH)

        def geometry(part):
            if part.x_first:
                return (lambda j: 2 * j + 1 - x_bit), (lambda j: 2 * j + x_bit), x_dev, y_bit, y_dev
            return (lambda j: 2 * (1 - y_bit) + j), (lambda j: 2 * y_bit + j), y_dev, x_bit, x_dev

        def core_copies(t):
            part, (mine, theirs), bufs = ca[t][0], ca_in[t], ca_scr[t]
            span = pl.ds(part.lo, part.r)
            local = pltpu.make_async_copy(mine.at[:, span], bufs[0], s_mine.at[t])
            return local, remote(theirs.at[:, span], bufs[1], s_cs.at[t], s_cr.at[t], pair)

        def first_copies(t):
            send_block, _, dev, _, _ = geometry(ca[t][0])
            bufs = ca_scr[t]
            return [remote(bufs[1].at[send_block(j)], bufs[2].at[j], s_as.at[t, j], s_ar.at[t, j], dev) for j in range(2)]

        def second_copy(t):
            part = (ca[t] if t < n_ca else bs[t - n_ca])[0]
            _, _, _, bit, dev = geometry(part)
            if t < n_ca:
                return remote(ca_scr[t][2].at[1 - bit], ca_scr[t][3], s_bs.at[t], s_br.at[t], dev)
            return remote(b_in[t - n_ca].at[1 - bit], b_scr[t - n_ca][1], s_bs.at[t], s_br.at[t], dev)

        def keep_copy(t):
            _, _, _, bit, _ = geometry(bs[t][0])
            return pltpu.make_async_copy(b_in[t].at[bit], b_scr[t][0], s_keep.at[t])

        def begin():
            barrier = pltpu.get_barrier_semaphore()
            for dev in (pair, x_dev, y_dev):
                pl.semaphore_signal(barrier, inc=1, device_id=(dev,), device_id_type=MESH)
            pl.semaphore_wait(barrier, 3)
            for t in range(n_b):
                second_copy(n_ca + t).start()
            for t in range(n_ca):
                for copy in core_copies(t):
                    copy.start()
            for t in range(n_b):
                keep_copy(t).start()

        def middle():
            for t in range(n_ca):
                send_block, keep_block, _, _, _ = geometry(ca[t][0])
                for copy in core_copies(t):
                    copy.wait()
                copies = first_copies(t)
                mine_v, sums = ca_scr[t][0], ca_scr[t][1]
                for j in range(2):
                    sums[send_block(j)] = sums[send_block(j)] + mine_v[send_block(j)]
                    copies[j].start()
                for j in range(2):
                    sums[keep_block(j)] = sums[keep_block(j)] + mine_v[keep_block(j)]

        def end():
            for t in range(n_ca):
                _, keep_block, _, bit, _ = geometry(ca[t][0])
                copies = first_copies(t)
                sums, arrived = ca_scr[t][1], ca_scr[t][2]
                for j in range(2):
                    copies[j].wait()
                if not finish:
                    for j in range(2):
                        ca_out[t][j] = arrived[j] + sums[keep_block(j)]
                else:
                    for j in range(2):
                        arrived[j] = arrived[j] + sums[keep_block(j)]
                    second_copy(t).start()
            for t in range(n_b):
                second_copy(n_ca + t).wait()
                keep_copy(t).wait()
                b_out[t][...] = b_scr[t][0][...] + b_scr[t][1][...]
            if finish:
                for t in range(n_ca):
                    _, _, _, bit, _ = geometry(ca[t][0])
                    second_copy(t).wait()
                    ca_out[t][...] = ca_scr[t][2][bit] + ca_scr[t][3][...]

        if steps == 1:
            begin()
            middle()
            end()
            return
        pl.when(step == 0)(begin)
        pl.when(step == 1)(middle)
        body(step, last, core, in_refs, out_refs, scr)
        pl.when(step == last)(end)

    args = list(ins)
    in_specs, out_specs, outs, scratch = list(in_specs), list(out_specs), list(outs), list(scratch)
    for part, mine, theirs in ca:
        args += [mine, theirs]
        in_specs += [ANY, ANY]
        dims = (part.r, part.c) if finish else (2, part.r, part.c)
        outs.append(shape(dims, F32))
        out_specs.append(whole(dims))
        scratch += [pltpu.VMEM((4, part.r, part.c), F32), pltpu.VMEM((4, part.r, part.c), F32), pltpu.VMEM((2, part.r, part.c), F32)]
        if finish:
            scratch.append(pltpu.VMEM((part.r, part.c), F32))
    for part, kept in bs:
        args.append(kept)
        in_specs.append(ANY)
        outs.append(shape((part.r, part.c), F32))
        out_specs.append(whole((part.r, part.c)))
        scratch += [pltpu.VMEM((part.r, part.c), F32), pltpu.VMEM((part.r, part.c), F32)]
    extra = {}
    if comm:
        sem = pltpu.SemaphoreType.DMA
        a, t, k = max(n_ca, 1), n_ca + n_b, max(n_b, 1)
        scratch += [sem((a,)), sem((a,)), sem((a,)), sem((a, 2)), sem((a, 2)), sem((t,)), sem((t,)), sem((k,))]
        extra = dict(collective_id=cid, has_side_effects=True)
    return pl.pallas_call(
        kernel, grid=(steps,), in_specs=in_specs, out_specs=out_specs, out_shape=outs, scratch_shapes=scratch,
        compiler_params=params(**extra), cost_estimate=cost(flops, 2e7), name=name)(*args)


CHUNK = 512


def mlp_fwd_kernel(h_ref, w1_ref, w3_ref, w2_ref, gain_ref, y_ref, act_ref):
    h32 = h_ref[0].astype(F32)
    normed = (h32 * inv_rms(h32) * gain_ref[...]).astype(BF)
    for c in range(0, FFN, CHUNK):
        gate = dot(normed, w1_ref[:, c:c + CHUNK])
        up = dot(normed, w3_ref[:, c:c + CHUNK])
        act_ref[:, c:c + CHUNK] = (gate * jax.nn.sigmoid(gate) * up).astype(BF)
    y_ref[0] = (h32 + dot(act_ref[...], w2_ref[...])).astype(BF)


def mlp_fwd(h, w1, w3, w2, gain):
    n = h.shape[0]
    return pl.pallas_call(
        mlp_fwd_kernel,
        grid=(n,),
        in_specs=[rows((SEQ, DIM)), whole(w1.shape), whole(w3.shape), whole(w2.shape), whole(gain.shape)],
        out_specs=rows((SEQ, DIM)),
        out_shape=shape((n, SEQ, DIM), BF),
        scratch_shapes=[pltpu.VMEM((SEQ, FFN), BF)],
        compiler_params=params(),
        cost_estimate=cost(6e9, 1e7),
        name="mlp_fwd",
    )(h, w1, w3, w2, gain)


def mlp_bwd_body(step, last, core, ins, outs, scratch):
    h_ref, dy_ref, w1_ref, w3_ref, w2_ref, gain_ref = ins
    normed_ref, act_ref, dgate_ref, dup_ref, gm_ref, gg_ref, *y_ref = outs
    h32 = h_ref[0].astype(F32)
    inv = inv_rms(h32)
    gain = gain_ref[...]
    normed = (h32 * inv * gain).astype(BF)
    normed_ref[0] = normed
    dy = dy_ref[0]
    for c in range(0, FFN, CHUNK):
        cols = slice(c, c + CHUNK)
        gate = dot(normed, w1_ref[:, cols])
        up = dot(normed, w3_ref[:, cols])
        grad_act = dot(dy, w2_ref[cols, :], ((1,), (1,)))
        sig = jax.nn.sigmoid(gate)
        silu = gate * sig
        act_ref[0, :, cols] = (silu * up).astype(BF)
        dup_ref[0, :, cols] = (grad_act * silu).astype(BF)
        dgate_ref[0, :, cols] = (grad_act * up * sig * (1.0 + gate * (1.0 - sig))).astype(BF)
    if y_ref:
        y_ref[0][0] = (h32 + dot(act_ref[0], w2_ref[...])).astype(BF)
    grad_normed = dot(dgate_ref[0], w1_ref[...], ((1,), (1,))) + dot(dup_ref[0], w3_ref[...], ((1,), (1,)))
    grad_h, grad_gain = rms_back(h32, inv, gain, grad_normed)
    gm_ref[0] = dy.astype(F32) + grad_h
    gg_ref[0] = grad_gain


def mlp_bwd(h, dy, w1, w3, w2, gain, with_out, ca, bs, cid):
    n = h.shape[0]
    extra = 1 if with_out else 0
    return fused(
        mlp_bwd_body, n, [h, dy, w1, w3, w2, gain],
        [rows((SEQ, DIM)), rows((SEQ, DIM)), whole(w1.shape), whole(w3.shape), whole(w2.shape), whole(gain.shape)],
        [shape((n, SEQ, DIM), BF), shape((n, SEQ, FFN), BF), shape((n, SEQ, FFN), BF), shape((n, SEQ, FFN), BF), shape((n, SEQ, DIM), F32), shape((n, 1, DIM), F32)] + [shape((n, SEQ, DIM), BF)] * extra,
        [rows((SEQ, DIM)), rows((SEQ, FFN)), rows((SEQ, FFN)), rows((SEQ, FFN)), rows((SEQ, DIM)), rows((1, DIM))] + [rows((SEQ, DIM))] * extra,
        [], ca, bs, False, cid, "mlp_bwd", 1.2e10)


def split_rows(full, core, mine_ref, theirs_ref):
    blocks, r = mine_ref.shape[0], mine_ref.shape[1]

    @pl.when(core == 0)
    def _():
        for i in range(blocks):
            mine_ref[i] = full[2 * i * r:(2 * i + 1) * r]
            theirs_ref[i] = full[(2 * i + 1) * r:(2 * i + 2) * r]

    @pl.when(core == 1)
    def _():
        for i in range(blocks):
            theirs_ref[i] = full[2 * i * r:(2 * i + 1) * r]
            mine_ref[i] = full[(2 * i + 1) * r:(2 * i + 2) * r]


def attn_bwd_body(step, last, core, ins, outs, scratch):
    gm_ref, x_ref, qkv_ref, p_ref, o_ref, wqkv_ref, wo_ref, gain_ref, cos_ref, sin_ref = ins
    dx_ref, gg_ref, qkv_mine, qkv_theirs, out_mine, out_theirs = outs
    do_ref, dqk_ref, dqkv_ref, acc_qkv, acc_out = scratch
    gm = gm_ref[0]
    gmb = gm.astype(BF)
    x32 = x_ref[0].astype(F32)
    inv = inv_rms(x32)
    gain = gain_ref[...]
    normed = (x32 * inv * gain).astype(BF)
    do_ref[...] = dot(gmb, wo_ref[...], ((1,), (1,))).astype(BF)
    half = SEQ // 2
    for kv in range(KV_HEADS):
        kcol = DIM + HEAD * kv
        vcol = 768 + HEAD * kv
        keys = qkv_ref[0, :, kcol:kcol + HEAD]
        vals = qkv_ref[0, :, vcol:vcol + HEAD]
        dk = [None, None]
        dv = [None, None]
        for g in range(GROUP):
            head = GROUP * kv + g
            hcol = slice(HEAD * head, HEAD * (head + 1))
            for blk in range(2):
                lo, length = half * blk, half * (blk + 1)
                p = p_ref[0, head, lo:lo + half, :length]
                d_o = do_ref[lo:lo + half, hcol]
                q = qkv_ref[0, lo:lo + half, hcol]
                dp = dot(d_o, vals[:length], ((1,), (1,)))
                p32 = p.astype(F32)
                ds = (p32 * (dp - jnp.sum(p32 * dp, axis=-1, keepdims=True)) * HEAD ** -0.5).astype(BF)
                dqk_ref[lo:lo + half, hcol] = dot(ds, keys[:length])
                dk_part = dot(ds, q, ((0,), (0,)))
                dv_part = dot(p, d_o, ((0,), (0,)))
                for part in range(blk + 1):
                    sl = slice(half * part, half * (part + 1))
                    dk[part] = dk_part[sl] if dk[part] is None else dk[part] + dk_part[sl]
                    dv[part] = dv_part[sl] if dv[part] is None else dv[part] + dv_part[sl]
        for part in range(2):
            sl = slice(half * part, half * (part + 1))
            dqk_ref[sl, kcol:kcol + HEAD] = dk[part]
            dqkv_ref[sl, vcol:vcol + HEAD] = dv[part].astype(BF)
    cos, sin = cos_ref[...], -sin_ref[...]
    for i in range(6):
        cols = slice(128 * i, 128 * (i + 1))
        dqkv_ref[:, cols] = rope(dqk_ref[:, cols], cos, sin).astype(BF)
    grad_normed = dot(dqkv_ref[...], wqkv_ref[:, :QKV], ((1,), (1,)))
    grad_x, grad_gain = rms_back(x32, inv, gain, grad_normed)
    dx_ref[0] = (gm + grad_x).astype(BF)
    gg_ref[0] = grad_gain
    part_qkv = dot(normed, dqkv_ref[...], ((0,), (0,)))
    part_out = dot(o_ref[0], gmb, ((0,), (0,)))

    @pl.when(step == 0)
    def _():
        acc_qkv[...] = part_qkv
        acc_out[...] = part_out

    @pl.when(step > 0)
    def _():
        acc_qkv[...] += part_qkv
        acc_out[...] += part_out

    @pl.when(step == last)
    def _():
        split_rows(acc_qkv, core, qkv_mine, qkv_theirs)
        split_rows(acc_out, core, out_mine, out_theirs)


def attn_bwd(gm, x, qkv, p, o, wqkv, wo, gain, cos, sin, ca, bs, cid):
    n = x.shape[0]
    r = DIM // 8
    return fused(
        attn_bwd_body, n, [gm, x, qkv, p, o, wqkv, wo, gain, cos, sin],
        [rows((SEQ, DIM)), rows((SEQ, DIM)), rows((SEQ, QKV)), rows((9, SEQ, SEQ)), rows((SEQ, DIM)), whole(wqkv.shape), whole(wo.shape), whole(gain.shape), whole(cos.shape), whole(sin.shape)],
        [shape((n, SEQ, DIM), BF), shape((n, 1, DIM), F32), shape((4, r, QKV), F32), shape((4, r, QKV), F32), shape((4, r, DIM), F32), shape((4, r, DIM), F32)],
        [rows((SEQ, DIM)), rows((1, DIM)), whole((4, r, QKV)), whole((4, r, QKV)), whole((4, r, DIM)), whole((4, r, DIM))],
        [pltpu.VMEM((SEQ, DIM), BF), pltpu.VMEM((SEQ, 768), F32), pltpu.VMEM((SEQ, QKV), BF), pltpu.VMEM((DIM, QKV), F32), pltpu.VMEM((DIM, DIM), F32)],
        ca, bs, False, cid, "attn_bwd", 1e10)


def wgrad_kernel(core_ref, a_ref, b_ref, mine_ref, theirs_ref):
    blocks, r = mine_ref.shape[0], mine_ref.shape[1]
    full = dot(a_ref[...], b_ref[...], ((0,), (0,)))

    @pl.when(core_ref[0] == 0)
    def _():
        for i in range(blocks):
            mine_ref[i] = full[2 * i * r:(2 * i + 1) * r]
            theirs_ref[i] = full[(2 * i + 1) * r:(2 * i + 2) * r]

    @pl.when(core_ref[0] == 1)
    def _():
        for i in range(blocks):
            theirs_ref[i] = full[2 * i * r:(2 * i + 1) * r]
            mine_ref[i] = full[(2 * i + 1) * r:(2 * i + 2) * r]


def wgrad(core, a, b, by_rows, tiles):
    tok, m = a.shape
    n = b.shape[1]
    r = m // 8
    if by_rows:
        a_spec = pl.BlockSpec((tok, m // tiles), lambda i, c: (0, i))
        b_spec = pl.BlockSpec((tok, n), lambda i, c: (0, 0))
        o_spec = pl.BlockSpec((4 // tiles, r, n), lambda i, c: (i, 0, 0))
    else:
        a_spec = pl.BlockSpec((tok, m), lambda i, c: (0, 0))
        b_spec = pl.BlockSpec((tok, n // tiles), lambda i, c: (0, i))
        o_spec = pl.BlockSpec((4, r, n // tiles), lambda i, c: (0, 0, i))
    return pl.pallas_call(
        wgrad_kernel,
        grid_spec=pltpu.PrefetchScalarGridSpec(num_scalar_prefetch=1, grid=(tiles,), in_specs=[a_spec, b_spec], out_specs=[o_spec, o_spec]),
        out_shape=[shape((4, r, n), F32)] * 2,
        compiler_params=params(),
        cost_estimate=cost(2 * tok * m * n, 1e7),
        name="wgrad",
    )(core, a, b)


def exchange(values, axis_bit):
    return lax.ppermute(values, "fsdp", [(dev, dev ^ axis_bit) for dev in range(8)])


def pick(stacked, index, axis):
    return lax.dynamic_index_in_dim(stacked, index, axis, keepdims=False)


def join(own, other, bit):
    first = jnp.where(bit == 0, own, other)
    second = jnp.where(bit == 0, other, own)
    return jnp.stack([first, second])


def gather(shard, bits, x_first):
    core, x_bit, y_bit = bits
    if x_first:
        pair = join(shard, exchange(shard, 2), x_bit)
        quad = join(pair, exchange(pair, 4), y_bit)
    else:
        pair = join(shard, exchange(shard, 4), y_bit)
        quad = jnp.swapaxes(join(pair, exchange(pair, 2), x_bit), 0, 1)
    other = exchange(quad, 1)
    both = jnp.where(core == 0, jnp.stack([quad, other], 2), jnp.stack([other, quad], 2))
    return both.reshape((-1,) + shard.shape[1:])


def solution(mesh):
    shard_spec = P(None, "fsdp")
    batch_spec = P("fsdp")

    def local_step(w_query, w_key, w_value, w_out, w_gate, w_up, w_down, gain_attn, gain_mlp, rope_cos, rope_sin, x_in, y_cot):
        me = lax.axis_index("fsdp")
        bits = (me % 2, (me // 2) % 2, me // 4)
        core = bits[0].reshape(1).astype(jnp.int32)
        num_layers = w_query.shape[0]
        batch = x_in.shape[0]
        tok = batch * SEQ
        cos = jnp.tile(rope_cos, (1, 4))
        sin = jnp.concatenate([-rope_sin, rope_sin, -rope_sin, rope_sin], 1)
        weights = []
        for i in range(num_layers):
            pad = jnp.zeros((w_query.shape[1], 62), F32)
            qkv = jnp.concatenate([w_query[i], w_key[i], w_value[i], gain_attn[i][:, None], gain_mlp[i][:, None], pad], 1).astype(BF)
            qkv = gather(qkv, bits, i == 0)
            out = gather(w_out[i].astype(BF), bits, i == 1)
            gate = gather(w_gate[i].astype(BF), bits, True)
            up = gather(w_up[i].astype(BF), bits, False)
            half = w_down.shape[1] // 2
            d0 = gather(w_down[i, :half].astype(BF), bits, True).reshape(8, half, -1)
            d1 = gather(w_down[i, half:].astype(BF), bits, False).reshape(8, half, -1)
            down = jnp.concatenate([d0, d1], 1).reshape(16 * half, -1)
            g1 = qkv[:, QKV].astype(F32).reshape(1, DIM)
            g2 = qkv[:, QKV + 1].astype(F32).reshape(1, DIM)
            weights.append((qkv, out, gate, up, down, g1, g2))
        hidden = x_in
        saved = []
        for i in range(num_layers):
            qkv_w, out_w, gate_w, up_w, down_w, g1, g2 = weights[i]
            mid, qkv, probs, attn = attn_fwd(hidden, qkv_w, out_w, g1, cos, sin)
            saved.append((hidden, mid, qkv, probs, attn))
            if i < num_layers - 1:
                hidden = mlp_fwd(mid, gate_w, up_w, down_w, g2)
        grad = y_cot
        grads = [None] * num_layers
        gain_grads = []
        y_out = None
        r, rd = w_query.shape[1], w_down.shape[1]
        pending = []
        done = {}
        for i in reversed(range(num_layers)):
            qkv_w, out_w, gate_w, up_w, down_w, g1, g2 = weights[i]
            hidden, mid, qkv, probs, attn = saved[i]
            last = i == num_layers - 1
            ca, bs = pending if pending else ([], [])
            res = mlp_bwd(mid, grad, gate_w, up_w, down_w, g2, last, ca, bs, 2 * i)
            normed2, act, dgate, dup, gm, gg2 = res[:6]
            if last:
                y_out = res[6]
            kept = [(p[0], v) for p, v in zip(ca, res[len(res) - len(ca) - len(bs):])]
            done[i + 1, "mlp"] = res[len(res) - len(bs):]
            flat = lambda v: v.reshape(tok, v.shape[-1])
            d_down = wgrad(core, flat(act), flat(grad), True, 4)
            d_gate = wgrad(core, flat(normed2), flat(dgate), False, 3)
            d_up = wgrad(core, flat(normed2), flat(dup), False, 3)
            ca = [(Part(True, rd // 2, DIM, 0), *d_down), (Part(False, rd // 2, DIM, rd // 2), *d_down),
                  (Part(True, r, FFN), *d_gate), (Part(False, r, FFN), *d_up)]
            res = attn_bwd(gm, hidden, qkv, probs, attn, qkv_w, out_w, g1, cos, sin, ca, kept, 2 * i + 1)
            grad, gg1, q_mine, q_theirs, o_mine, o_theirs = res[:6]
            done[i + 1, "attn"] = res[6 + len(ca):]
            bs = [(p[0], v) for p, v in zip(ca, res[6:6 + len(ca)])]
            ca = [(Part(i == 0, r, QKV), q_mine, q_theirs), (Part(i == 1, r, DIM), o_mine, o_theirs)]
            pending = (ca, bs)
            gain_grads = [gg1.sum((0, 1)), gg2.sum((0, 1))] + gain_grads
        gains = jnp.stack(gain_grads).reshape(2 * num_layers, 4, 2, r)
        gains = jnp.pad(gains.transpose(2, 1, 0, 3).reshape(2, 4, 2 * num_layers * r), ((0, 0), (0, 0), (0, 1024 - 2 * num_layers * r))).reshape(2, 4, 8, 128)
        ca, bs = pending
        ca = ca + [(Part(True, 8, 128), pick(gains, bits[0], 0), pick(gains, 1 - bits[0], 0))]
        res = fused(None, 1, [], [], [], [], [], ca, bs, True, 2 * num_layers, "rs_tail", 1e6)
        done[0, "attn"] = res[:2]
        done[0, "mlp"] = res[3:]
        s_gains = res[2].reshape(1024)[:2 * num_layers * r].reshape(2 * num_layers, r)
        for i in range(num_layers):
            s_qkv, s_out = done[i, "attn"]
            down0, down1, s_gate, s_up = done[i, "mlp"]
            grads[i] = (s_qkv[:, :576], s_qkv[:, 576:768], s_qkv[:, 768:960], s_out, s_gate, s_up, jnp.concatenate([down0, down1], 0))
        stacked = tuple(jnp.stack(parts) for parts in zip(*grads))
        return (y_out, grad) + stacked + (s_gains[0::2], s_gains[1::2])

    in_specs = (shard_spec,) * 9 + (P(), P(), batch_spec, batch_spec)
    out_specs = (batch_spec, batch_spec) + (shard_spec,) * 9
    return jax.shard_map(local_step, mesh=mesh, in_specs=in_specs, out_specs=out_specs, check_vma=False)
```

```python
import functools

import jax
import jax.numpy as jnp
from jax import lax
from jax.experimental import pallas as pl
from jax.experimental.pallas import tpu as pltpu
from jax.sharding import PartitionSpec as P

NORM_EPS = 1e-5
MASK_VALUE = -1e30
HEAD = 64
KV_HEADS = 3
GROUP = 3
SEQ = 256
DIM = 576
FFN = 1536
QKV = 960
BF = jnp.bfloat16
F32 = jnp.float32


def dot(a, b, dims=((1,), (0,))):
    return lax.dot_general(a, b, (dims, ((), ())), preferred_element_type=F32)


def params(**kw):
    return pltpu.CompilerParams(dimension_semantics=("arbitrary",), vmem_limit_bytes=60 * 1024 * 1024, **kw)


def cost(flops, bytes_accessed):
    return pl.CostEstimate(flops=int(flops), bytes_accessed=int(bytes_accessed), transcendentals=0)


def shape(dims, dtype):
    return jax.ShapeDtypeStruct(dims, dtype)


def whole(dims):
    return pl.BlockSpec(dims, lambda i: (0,) * len(dims))


def rows(dims):
    return pl.BlockSpec((1,) + dims, lambda i: (i,) + (0,) * len(dims))


def inv_rms(vals32):
    return lax.rsqrt(jnp.mean(vals32 * vals32, axis=-1, keepdims=True) + NORM_EPS)


def rms_back(vals32, inv, gain, grad_normed):
    scaled = vals32 * inv
    grad_scaled = grad_normed * gain
    grad_gain = jnp.sum(grad_normed * scaled, axis=0, keepdims=True)
    return inv * (grad_scaled - scaled * jnp.mean(grad_scaled * scaled, axis=-1, keepdims=True)), grad_gain


def rope(vals32, cos, sin):
    lane = lax.broadcasted_iota(jnp.int32, vals32.shape, 1)
    swapped = jnp.where(lane % HEAD < HEAD // 2, pltpu.roll(vals32, 96, 1), pltpu.roll(vals32, 32, 1))
    return vals32 * cos + swapped * sin


MESH = pl.DeviceIdType.MESH
ANY = pl.BlockSpec(memory_space=pl.ANY)


class Part:
    def __init__(self, x_first, r, c, lo=0):
        self.x_first, self.r, self.c, self.lo = x_first, r, c, lo


class Gather:
    def __init__(self, x_first, r, c, srcs, specs, fill):
        self.x_first, self.r, self.c, self.srcs, self.specs, self.fill = x_first, r, c, srcs, specs, fill


def gather_of(x_first, layer, masters):
    widths = [m.shape[2] for m in masters]

    def fill(refs, dst):
        lo = 0
        for ref, width in zip(refs, widths):
            dst[:, lo:lo + width] = ref[0].astype(BF)
            lo += width

    specs = [pl.BlockSpec((1,) + m.shape[1:], lambda i: (layer, 0, 0)) for m in masters]
    return Gather(x_first, masters[0].shape[1], sum(widths), list(masters), specs, fill)


def gather_gains(gain_attn, gain_mlp):
    layers, r = gain_attn.shape

    def fill(refs, dst):
        dst[...] = jnp.zeros(dst.shape, BF)
        dst[0:layers, 0:r] = refs[0][...].astype(BF)
        dst[layers:2 * layers, 0:r] = refs[1][...].astype(BF)

    return Gather(True, 16, 128, [gain_attn, gain_mlp], [whole((layers, r))] * 2, fill)


def fused(body, steps, ins, in_specs, outs, out_specs, scratch, ca, bs, finish, cid, name, flops, ag=(), forward=2):
    n_ca, n_b = len(ca), len(bs)
    n_in, n_out, n_scr = len(ins), len(outs), len(scratch)
    n_g = len(ag)
    comm = n_ca + n_b + n_g > 0
    last = steps - 1

    def kernel(*refs):
        refs = list(refs)
        take = lambda k: [refs.pop(0) for _ in range(k)]
        in_refs = take(n_in)
        ca_in = [take(2) for _ in range(n_ca)]
        b_in = take(n_b)
        g_in = [take(len(g.srcs)) for g in ag]
        out_refs = take(n_out)
        ca_out = take(n_ca)
        b_out = take(n_b)
        g_out = take(n_g)
        scr = take(n_scr)
        ca_scr = [take(4 if finish else 3) for _ in range(n_ca)]
        b_scr = [take(2) for _ in range(n_b)]
        g_own = take(n_g)
        step = pl.program_id(0)
        me = lax.axis_index("fsdp")
        core, x_bit, y_bit = lax.rem(me, 2), lax.rem(me // 2, 2), me // 4
        if not comm:
            body(step, last, core, in_refs, out_refs, scr)
            return
        s_mine, s_cs, s_cr, s_as, s_ar, s_bs, s_br, s_keep, s_gl, s_gs, s_gr = take(11)
        pair, x_dev, y_dev = me + 1 - 2 * core, me + 2 - 4 * x_bit, me + 4 - 8 * y_bit

        def remote(src, dst, send, recv, dev):
            return pltpu.make_async_remote_copy(src_ref=src, dst_ref=dst, send_sem=send, recv_sem=recv, device_id=(dev,), device_id_type=MESH)

        def geometry(part):
            if part.x_first:
                return (lambda j: 2 * j + 1 - x_bit), (lambda j: 2 * j + x_bit), x_dev, y_bit, y_dev
            return (lambda j: 2 * (1 - y_bit) + j), (lambda j: 2 * y_bit + j), y_dev, x_bit, x_dev

        def core_copies(t):
            part, (mine, theirs), bufs = ca[t][0], ca_in[t], ca_scr[t]
            span = pl.ds(part.lo, part.r)
            local = pltpu.make_async_copy(mine.at[:, span], bufs[0], s_mine.at[t])
            return local, remote(theirs.at[:, span], bufs[1], s_cs.at[t], s_cr.at[t], pair)

        def first_copies(t):
            send_block, _, dev, _, _ = geometry(ca[t][0])
            bufs = ca_scr[t]
            return [remote(bufs[1].at[send_block(j)], bufs[2].at[j], s_as.at[t, j], s_ar.at[t, j], dev) for j in range(2)]

        def second_copy(t):
            part = (ca[t] if t < n_ca else bs[t - n_ca])[0]
            _, _, _, bit, dev = geometry(part)
            if t < n_ca:
                return remote(ca_scr[t][2].at[1 - bit], ca_scr[t][3], s_bs.at[t], s_br.at[t], dev)
            return remote(b_in[t - n_ca].at[1 - bit], b_scr[t - n_ca][1], s_bs.at[t], s_br.at[t], dev)

        def keep_copy(t):
            _, _, _, bit, _ = geometry(bs[t][0])
            return pltpu.make_async_copy(b_in[t].at[bit], b_scr[t][0], s_keep.at[t])

        def g_copy(t, k):
            g, own, full = ag[t], g_own[t], g_out[t]
            one, two = (x_dev, y_dev) if g.x_first else (y_dev, x_dev)
            blk = (me, me, me, one, one, two, one + two - me)[k]
            dev = (one, two, pair, two, pair, pair, pair)[k]
            return remote(own if k < 3 else full.at[blk], full.at[blk], s_gs.at[t, k], s_gr.at[t, k], dev)

        def g_local(t):
            return pltpu.make_async_copy(g_own[t], g_out[t].at[me], s_gl.at[t])

        def g_forward():
            for t in range(n_g):
                g_copy(t, 0).wait_recv()
                g_copy(t, 3).start()
                g_copy(t, 4).start()
            for t in range(n_g):
                g_copy(t, 1).wait_recv()
                g_copy(t, 5).start()

        def g_end():
            for t in range(n_g):
                g_copy(t, 3).wait_recv()
                g_copy(t, 6).start()
            for t in range(n_g):
                for k in (2, 4, 5, 6):
                    g_copy(t, k).wait_recv()
                for k in range(7):
                    g_copy(t, k).wait_send()
                g_local(t).wait()

        def begin():
            for t in range(n_g):
                ag[t].fill(g_in[t], g_own[t])
            barrier = pltpu.get_barrier_semaphore()
            for dev in (pair, x_dev, y_dev):
                pl.semaphore_signal(barrier, inc=1, device_id=(dev,), device_id_type=MESH)
            pl.semaphore_wait(barrier, 3)
            for t in range(n_g):
                for k in range(3):
                    g_copy(t, k).start()
                g_local(t).start()
            for t in range(n_b):
                second_copy(n_ca + t).start()
            for t in range(n_ca):
                for copy in core_copies(t):
                    copy.start()
            for t in range(n_b):
                keep_copy(t).start()

        def middle():
            for t in range(n_ca):
                send_block, keep_block, _, _, _ = geometry(ca[t][0])
                for copy in core_copies(t):
                    copy.wait()
                copies = first_copies(t)
                mine_v, sums = ca_scr[t][0], ca_scr[t][1]
                for j in range(2):
                    sums[send_block(j)] = sums[send_block(j)] + mine_v[send_block(j)]
                    copies[j].start()
                for j in range(2):
                    sums[keep_block(j)] = sums[keep_block(j)] + mine_v[keep_block(j)]

        def end():
            for t in range(n_ca):
                _, keep_block, _, bit, _ = geometry(ca[t][0])
                copies = first_copies(t)
                sums, arrived = ca_scr[t][1], ca_scr[t][2]
                for j in range(2):
                    copies[j].wait()
                if not finish:
                    for j in range(2):
                        ca_out[t][j] = arrived[j] + sums[keep_block(j)]
                else:
                    for j in range(2):
                        arrived[j] = arrived[j] + sums[keep_block(j)]
                    second_copy(t).start()
            for t in range(n_b):
                second_copy(n_ca + t).wait()
                keep_copy(t).wait()
                b_out[t][...] = b_scr[t][0][...] + b_scr[t][1][...]
            if finish:
                for t in range(n_ca):
                    _, _, _, bit, _ = geometry(ca[t][0])
                    second_copy(t).wait()
                    ca_out[t][...] = ca_scr[t][2][bit] + ca_scr[t][3][...]

        if steps == 1:
            begin()
            if n_g:
                g_forward()
            middle()
            end()
            if n_g:
                g_end()
            return
        pl.when(step == 0)(begin)
        if n_ca:
            pl.when(step == 1)(middle)
        if n_g:
            pl.when(step == forward)(g_forward)
        body(step, last, core, in_refs, out_refs, scr)
        if n_ca + n_b:
            pl.when(step == last)(end)
        if n_g:
            pl.when(step == last)(g_end)

    args = list(ins)
    in_specs, out_specs, outs, scratch = list(in_specs), list(out_specs), list(outs), list(scratch)
    for part, mine, theirs in ca:
        args += [mine, theirs]
        in_specs += [ANY, ANY]
        dims = (part.r, part.c) if finish else (2, part.r, part.c)
        outs.append(shape(dims, F32))
        out_specs.append(whole(dims))
        scratch += [pltpu.VMEM((4, part.r, part.c), F32), pltpu.VMEM((4, part.r, part.c), F32), pltpu.VMEM((2, part.r, part.c), F32)]
        if finish:
            scratch.append(pltpu.VMEM((part.r, part.c), F32))
    for part, kept in bs:
        args.append(kept)
        in_specs.append(ANY)
        outs.append(shape((part.r, part.c), F32))
        out_specs.append(whole((part.r, part.c)))
        scratch += [pltpu.VMEM((part.r, part.c), F32), pltpu.VMEM((part.r, part.c), F32)]
    for g in ag:
        args += g.srcs
        in_specs += g.specs
        outs.append(shape((8, g.r, g.c), BF))
        out_specs.append(ANY)
        scratch.append(pltpu.VMEM((g.r, g.c), BF))
    extra = {}
    if comm:
        g_n = max(n_g, 1)
        sem = pltpu.SemaphoreType.DMA
        a, t, k = max(n_ca, 1), max(n_ca + n_b, 1), max(n_b, 1)
        scratch += [sem((a,)), sem((a,)), sem((a,)), sem((a, 2)), sem((a, 2)), sem((t,)), sem((t,)), sem((k,)), sem((g_n,)), sem((g_n, 7)), sem((g_n, 7))]
        extra = dict(collective_id=cid, has_side_effects=True)
    return pl.pallas_call(
        kernel, grid=(steps,), in_specs=in_specs, out_specs=out_specs, out_shape=outs, scratch_shapes=scratch,
        compiler_params=params(**extra), cost_estimate=cost(flops, 2e7), name=name)(*args)


CHUNK = 512


def attn_fwd_body(step, last, core, ins, outs, scratch):
    x_ref, wqkv_ref, wo_ref, gain_ref, cos_ref, sin_ref = ins
    h_ref, qkv_ref, p_ref, o_ref = outs
    x32 = x_ref[0].astype(F32)
    normed = (x32 * inv_rms(x32) * gain_ref[...]).astype(BF)
    proj = dot(normed, wqkv_ref[...])
    cos, sin = cos_ref[...], sin_ref[...]
    for i in range(6):
        qkv_ref[0, :, 128 * i:128 * (i + 1)] = rope(proj[:, 128 * i:128 * (i + 1)], cos, sin).astype(BF)
    qkv_ref[0, :, 768:QKV] = proj[:, 768:QKV].astype(BF)
    half = SEQ // 2
    causal = lax.broadcasted_iota(jnp.int32, (half, half), 0) >= lax.broadcasted_iota(jnp.int32, (half, half), 1)
    for kv in range(KV_HEADS):
        keys = qkv_ref[0, :, DIM + HEAD * kv:DIM + HEAD * (kv + 1)]
        vals = qkv_ref[0, :, 768 + HEAD * kv:768 + HEAD * (kv + 1)]
        for blk in range(2):
            lo, length = half * blk, half * (blk + 1)
            for g in range(GROUP):
                head = GROUP * kv + g
                q = qkv_ref[0, lo:lo + half, HEAD * head:HEAD * (head + 1)]
                s = dot(q, keys[:length], ((1,), (1,))) * HEAD ** -0.5
                diag = jnp.where(causal, s[:, lo:], MASK_VALUE)
                s = diag if blk == 0 else jnp.concatenate([s[:, :lo], diag], axis=1)
                e = jnp.exp(s - jnp.max(s, axis=-1, keepdims=True))
                p = (e * (1.0 / jnp.sum(e, axis=-1, keepdims=True))).astype(BF)
                p_ref[0, head, lo:lo + half, :length] = p
                o_ref[0, lo:lo + half, HEAD * head:HEAD * (head + 1)] = dot(p, vals[:length]).astype(BF)
    h_ref[0] = (x32 + dot(o_ref[0], wo_ref[...])).astype(BF)


def attn_fwd(x, wqkv, wo, gain, cos, sin, ag, cid):
    n = x.shape[0]
    return fused(
        attn_fwd_body, n, [x, wqkv, wo, gain, cos, sin],
        [rows((SEQ, DIM)), whole(wqkv.shape), whole(wo.shape), whole(gain.shape), whole(cos.shape), whole(sin.shape)],
        [shape((n, SEQ, DIM), BF), shape((n, SEQ, QKV), BF), shape((n, 9, SEQ, SEQ), BF), shape((n, SEQ, DIM), BF)],
        [rows((SEQ, DIM)), rows((SEQ, QKV)), rows((9, SEQ, SEQ)), rows((SEQ, DIM))],
        [], [], [], False, cid, "attn_fwd", 5e9, ag)


def mlp_fwd_body(step, last, core, ins, outs, scratch):
    h_ref, w1_ref, w3_ref, w2_ref, gain_ref = ins
    (y_ref,), (act_ref,) = outs, scratch
    h32 = h_ref[0].astype(F32)
    normed = (h32 * inv_rms(h32) * gain_ref[...]).astype(BF)
    for c in range(0, FFN, CHUNK):
        gate = dot(normed, w1_ref[:, c:c + CHUNK])
        up = dot(normed, w3_ref[:, c:c + CHUNK])
        act_ref[:, c:c + CHUNK] = (gate * jax.nn.sigmoid(gate) * up).astype(BF)
    y_ref[0] = (h32 + dot(act_ref[...], w2_ref[...])).astype(BF)


def mlp_fwd(h, w1, w3, w2, gain, ag, cid):
    n = h.shape[0]
    return fused(
        mlp_fwd_body, n, [h, w1, w3, w2, gain],
        [rows((SEQ, DIM)), whole(w1.shape), whole(w3.shape), whole(w2.shape), whole(gain.shape)],
        [shape((n, SEQ, DIM), BF)], [rows((SEQ, DIM))], [pltpu.VMEM((SEQ, FFN), BF)],
        [], [], False, cid, "mlp_fwd", 6e9, ag)


def mlp_bwd_body(step, last, core, ins, outs, scratch):
    h_ref, dy_ref, w1_ref, w3_ref, w2_ref, gain_ref = ins
    normed_ref, act_ref, dgate_ref, dup_ref, gm_ref, gg_ref, *y_ref = outs
    h32 = h_ref[0].astype(F32)
    inv = inv_rms(h32)
    gain = gain_ref[...]
    normed = (h32 * inv * gain).astype(BF)
    normed_ref[0] = normed
    dy = dy_ref[0]
    for c in range(0, FFN, CHUNK):
        cols = slice(c, c + CHUNK)
        gate = dot(normed, w1_ref[:, cols])
        up = dot(normed, w3_ref[:, cols])
        grad_act = dot(dy, w2_ref[cols, :], ((1,), (1,)))
        sig = jax.nn.sigmoid(gate)
        silu = gate * sig
        act_ref[0, :, cols] = (silu * up).astype(BF)
        dup_ref[0, :, cols] = (grad_act * silu).astype(BF)
        dgate_ref[0, :, cols] = (grad_act * up * sig * (1.0 + gate * (1.0 - sig))).astype(BF)
    if y_ref:
        y_ref[0][0] = (h32 + dot(act_ref[0], w2_ref[...])).astype(BF)
    grad_normed = dot(dgate_ref[0], w1_ref[...], ((1,), (1,))) + dot(dup_ref[0], w3_ref[...], ((1,), (1,)))
    grad_h, grad_gain = rms_back(h32, inv, gain, grad_normed)
    gm_ref[0] = dy.astype(F32) + grad_h
    gg_ref[0] = grad_gain


def mlp_bwd(h, dy, w1, w3, w2, gain, with_out, ca, bs, cid):
    n = h.shape[0]
    extra = 1 if with_out else 0
    return fused(
        mlp_bwd_body, n, [h, dy, w1, w3, w2, gain],
        [rows((SEQ, DIM)), rows((SEQ, DIM)), whole(w1.shape), whole(w3.shape), whole(w2.shape), whole(gain.shape)],
        [shape((n, SEQ, DIM), BF), shape((n, SEQ, FFN), BF), shape((n, SEQ, FFN), BF), shape((n, SEQ, FFN), BF), shape((n, SEQ, DIM), F32), shape((n, 1, DIM), F32)] + [shape((n, SEQ, DIM), BF)] * extra,
        [rows((SEQ, DIM)), rows((SEQ, FFN)), rows((SEQ, FFN)), rows((SEQ, FFN)), rows((SEQ, DIM)), rows((1, DIM))] + [rows((SEQ, DIM))] * extra,
        [], ca, bs, False, cid, "mlp_bwd", 1.2e10)


def split_rows(full, core, mine_ref, theirs_ref):
    blocks, r = mine_ref.shape[0], mine_ref.shape[1]

    @pl.when(core == 0)
    def _():
        for i in range(blocks):
            mine_ref[i] = full[2 * i * r:(2 * i + 1) * r]
            theirs_ref[i] = full[(2 * i + 1) * r:(2 * i + 2) * r]

    @pl.when(core == 1)
    def _():
        for i in range(blocks):
            theirs_ref[i] = full[2 * i * r:(2 * i + 1) * r]
            mine_ref[i] = full[(2 * i + 1) * r:(2 * i + 2) * r]


def attn_bwd_body(step, last, core, ins, outs, scratch):
    gm_ref, x_ref, qkv_ref, p_ref, o_ref, wqkv_ref, wo_ref, gain_ref, cos_ref, sin_ref = ins
    dx_ref, gg_ref, qkv_mine, qkv_theirs, out_mine, out_theirs = outs
    do_ref, dqk_ref, dqkv_ref, acc_qkv, acc_out = scratch
    gm = gm_ref[0]
    gmb = gm.astype(BF)
    x32 = x_ref[0].astype(F32)
    inv = inv_rms(x32)
    gain = gain_ref[...]
    normed = (x32 * inv * gain).astype(BF)
    do_ref[...] = dot(gmb, wo_ref[...], ((1,), (1,))).astype(BF)
    half = SEQ // 2
    for kv in range(KV_HEADS):
        kcol = DIM + HEAD * kv
        vcol = 768 + HEAD * kv
        keys = qkv_ref[0, :, kcol:kcol + HEAD]
        vals = qkv_ref[0, :, vcol:vcol + HEAD]
        dk = [None, None]
        dv = [None, None]
        for g in range(GROUP):
            head = GROUP * kv + g
            hcol = slice(HEAD * head, HEAD * (head + 1))
            for blk in range(2):
                lo, length = half * blk, half * (blk + 1)
                p = p_ref[0, head, lo:lo + half, :length]
                d_o = do_ref[lo:lo + half, hcol]
                q = qkv_ref[0, lo:lo + half, hcol]
                dp = dot(d_o, vals[:length], ((1,), (1,)))
                p32 = p.astype(F32)
                ds = (p32 * (dp - jnp.sum(p32 * dp, axis=-1, keepdims=True)) * HEAD ** -0.5).astype(BF)
                dqk_ref[lo:lo + half, hcol] = dot(ds, keys[:length])
                dk_part = dot(ds, q, ((0,), (0,)))
                dv_part = dot(p, d_o, ((0,), (0,)))
                for part in range(blk + 1):
                    sl = slice(half * part, half * (part + 1))
                    dk[part] = dk_part[sl] if dk[part] is None else dk[part] + dk_part[sl]
                    dv[part] = dv_part[sl] if dv[part] is None else dv[part] + dv_part[sl]
        for part in range(2):
            sl = slice(half * part, half * (part + 1))
            dqk_ref[sl, kcol:kcol + HEAD] = dk[part]
            dqkv_ref[sl, vcol:vcol + HEAD] = dv[part].astype(BF)
    cos, sin = cos_ref[...], -sin_ref[...]
    for i in range(6):
        cols = slice(128 * i, 128 * (i + 1))
        dqkv_ref[:, cols] = rope(dqk_ref[:, cols], cos, sin).astype(BF)
    grad_normed = dot(dqkv_ref[...], wqkv_ref[...], ((1,), (1,)))
    grad_x, grad_gain = rms_back(x32, inv, gain, grad_normed)
    dx_ref[0] = (gm + grad_x).astype(BF)
    gg_ref[0] = grad_gain
    part_qkv = dot(normed, dqkv_ref[...], ((0,), (0,)))
    part_out = dot(o_ref[0], gmb, ((0,), (0,)))

    @pl.when(step == 0)
    def _():
        acc_qkv[...] = part_qkv
        acc_out[...] = part_out

    @pl.when(step > 0)
    def _():
        acc_qkv[...] += part_qkv
        acc_out[...] += part_out

    @pl.when(step == last)
    def _():
        split_rows(acc_qkv, core, qkv_mine, qkv_theirs)
        split_rows(acc_out, core, out_mine, out_theirs)


def attn_bwd(gm, x, qkv, p, o, wqkv, wo, gain, cos, sin, ca, bs, cid):
    n = x.shape[0]
    r = DIM // 8
    return fused(
        attn_bwd_body, n, [gm, x, qkv, p, o, wqkv, wo, gain, cos, sin],
        [rows((SEQ, DIM)), rows((SEQ, DIM)), rows((SEQ, QKV)), rows((9, SEQ, SEQ)), rows((SEQ, DIM)), whole(wqkv.shape), whole(wo.shape), whole(gain.shape), whole(cos.shape), whole(sin.shape)],
        [shape((n, SEQ, DIM), BF), shape((n, 1, DIM), F32), shape((4, r, QKV), F32), shape((4, r, QKV), F32), shape((4, r, DIM), F32), shape((4, r, DIM), F32)],
        [rows((SEQ, DIM)), rows((1, DIM)), whole((4, r, QKV)), whole((4, r, QKV)), whole((4, r, DIM)), whole((4, r, DIM))],
        [pltpu.VMEM((SEQ, DIM), BF), pltpu.VMEM((SEQ, 768), F32), pltpu.VMEM((SEQ, QKV), BF), pltpu.VMEM((DIM, QKV), F32), pltpu.VMEM((DIM, DIM), F32)],
        ca, bs, False, cid, "attn_bwd", 1e10)


def wgrad_kernel(core_ref, a_ref, b_ref, mine_ref, theirs_ref):
    blocks, r = mine_ref.shape[0], mine_ref.shape[1]
    full = dot(a_ref[...], b_ref[...], ((0,), (0,)))

    @pl.when(core_ref[0] == 0)
    def _():
        for i in range(blocks):
            mine_ref[i] = full[2 * i * r:(2 * i + 1) * r]
            theirs_ref[i] = full[(2 * i + 1) * r:(2 * i + 2) * r]

    @pl.when(core_ref[0] == 1)
    def _():
        for i in range(blocks):
            theirs_ref[i] = full[2 * i * r:(2 * i + 1) * r]
            mine_ref[i] = full[(2 * i + 1) * r:(2 * i + 2) * r]


def wgrad(core, a, b, by_rows, tiles):
    tok, m = a.shape
    n = b.shape[1]
    r = m // 8
    if by_rows:
        a_spec = pl.BlockSpec((tok, m // tiles), lambda i, c: (0, i))
        b_spec = pl.BlockSpec((tok, n), lambda i, c: (0, 0))
        o_spec = pl.BlockSpec((4 // tiles, r, n), lambda i, c: (i, 0, 0))
    else:
        a_spec = pl.BlockSpec((tok, m), lambda i, c: (0, 0))
        b_spec = pl.BlockSpec((tok, n // tiles), lambda i, c: (0, i))
        o_spec = pl.BlockSpec((4, r, n // tiles), lambda i, c: (0, 0, i))
    return pl.pallas_call(
        wgrad_kernel,
        grid_spec=pltpu.PrefetchScalarGridSpec(num_scalar_prefetch=1, grid=(tiles,), in_specs=[a_spec, b_spec], out_specs=[o_spec, o_spec]),
        out_shape=[shape((4, r, n), F32)] * 2,
        compiler_params=params(),
        cost_estimate=cost(2 * tok * m * n, 1e7),
        name="wgrad",
    )(core, a, b)


def pick(stacked, index, axis):
    return lax.dynamic_index_in_dim(stacked, index, axis, keepdims=False)


def solution(mesh):
    shard_spec = P(None, "fsdp")
    batch_spec = P("fsdp")

    def local_step(w_query, w_key, w_value, w_out, w_gate, w_up, w_down, gain_attn, gain_mlp, rope_cos, rope_sin, x_in, y_cot):
        me = lax.axis_index("fsdp")
        bits = (me % 2, (me // 2) % 2, me // 4)
        core = bits[0].reshape(1).astype(jnp.int32)
        num_layers = w_query.shape[0]
        batch = x_in.shape[0]
        tok = batch * SEQ
        cos = jnp.tile(rope_cos, (1, 4))
        sin = jnp.concatenate([-rope_sin, rope_sin, -rope_sin, rope_sin], 1)
        attn_ag = lambda i: [gather_of(False, i, (w_query, w_key, w_value)), gather_of(True, i, (w_out,))]
        mlp_ag = lambda i: [gather_of(True, i, (w_gate,)), gather_of(False, i, (w_up,)), gather_of(i == 0, i, (w_down,))]
        merge = lambda v: v.reshape(-1, v.shape[2])
        first = fused(None, 1, [], [], [], [], [], [], [], False, 10, "ag_head", 1e6, attn_ag(0) + [gather_gains(gain_attn, gain_mlp)])
        attn_w = [merge(v) for v in first[:2]]
        gains = first[2][:, :2 * num_layers, :w_query.shape[1]].astype(F32).transpose(1, 0, 2).reshape(2 * num_layers, 1, DIM)
        weights = []
        hidden = x_in
        saved = []
        for i in range(num_layers):
            g1, g2 = gains[i], gains[num_layers + i]
            mid, qkv, probs, attn, *mlp_w = attn_fwd(hidden, *attn_w, g1, cos, sin, mlp_ag(i), 11 + 2 * i)
            mlp_w = [merge(v) for v in mlp_w]
            weights.append((*attn_w, *mlp_w, g1, g2))
            saved.append((hidden, mid, qkv, probs, attn))
            if i < num_layers - 1:
                hidden, *attn_w = mlp_fwd(mid, *mlp_w, g2, attn_ag(i + 1), 12 + 2 * i)
                attn_w = [merge(v) for v in attn_w]
        grad = y_cot
        grads = [None] * num_layers
        gain_grads = []
        y_out = None
        r, rd = w_query.shape[1], w_down.shape[1]
        pending = []
        done = {}
        for i in reversed(range(num_layers)):
            qkv_w, out_w, gate_w, up_w, down_w, g1, g2 = weights[i]
            hidden, mid, qkv, probs, attn = saved[i]
            last = i == num_layers - 1
            ca, bs = pending if pending else ([], [])
            res = mlp_bwd(mid, grad, gate_w, up_w, down_w, g2, last, ca, bs, 2 * i)
            normed2, act, dgate, dup, gm, gg2 = res[:6]
            if last:
                y_out = res[6]
            kept = [(p[0], v) for p, v in zip(ca, res[len(res) - len(ca) - len(bs):])]
            done[i + 1, "mlp"] = res[len(res) - len(bs):]
            flat = lambda v: v.reshape(tok, v.shape[-1])
            d_down = wgrad(core, flat(act), flat(grad), True, 4)
            d_gate = wgrad(core, flat(normed2), flat(dgate), False, 3)
            d_up = wgrad(core, flat(normed2), flat(dup), False, 3)
            ca = [(Part(True, rd // 2, DIM, 0), *d_down), (Part(False, rd // 2, DIM, rd // 2), *d_down),
                  (Part(True, r, FFN), *d_gate), (Part(False, r, FFN), *d_up)]
            res = attn_bwd(gm, hidden, qkv, probs, attn, qkv_w, out_w, g1, cos, sin, ca, kept, 2 * i + 1)
            grad, gg1, q_mine, q_theirs, o_mine, o_theirs = res[:6]
            done[i + 1, "attn"] = res[6 + len(ca):]
            bs = [(p[0], v) for p, v in zip(ca, res[6:6 + len(ca)])]
            ca = [(Part(i == 0, r, QKV), q_mine, q_theirs), (Part(i == 1, r, DIM), o_mine, o_theirs)]
            pending = (ca, bs)
            gain_grads = [gg1.sum((0, 1)), gg2.sum((0, 1))] + gain_grads
        gains = jnp.stack(gain_grads).reshape(2 * num_layers, 4, 2, r)
        gains = jnp.pad(gains.transpose(2, 1, 0, 3).reshape(2, 4, 2 * num_layers * r), ((0, 0), (0, 0), (0, 1024 - 2 * num_layers * r))).reshape(2, 4, 8, 128)
        ca, bs = pending
        ca = ca + [(Part(True, 8, 128), pick(gains, bits[0], 0), pick(gains, 1 - bits[0], 0))]
        res = fused(None, 1, [], [], [], [], [], ca, bs, True, 2 * num_layers, "rs_tail", 1e6)
        done[0, "attn"] = res[:2]
        done[0, "mlp"] = res[3:]
        s_gains = res[2].reshape(1024)[:2 * num_layers * r].reshape(2 * num_layers, r)
        for i in range(num_layers):
            s_qkv, s_out = done[i, "attn"]
            down0, down1, s_gate, s_up = done[i, "mlp"]
            grads[i] = (s_qkv[:, :576], s_qkv[:, 576:768], s_qkv[:, 768:960], s_out, s_gate, s_up, jnp.concatenate([down0, down1], 0))
        stacked = tuple(jnp.stack(parts) for parts in zip(*grads))
        return (y_out, grad) + stacked + (s_gains[0::2], s_gains[1::2])

    in_specs = (shard_spec,) * 9 + (P(), P(), batch_spec, batch_spec)
    out_specs = (batch_spec, batch_spec) + (shard_spec,) * 9
    return jax.shard_map(local_step, mesh=mesh, in_specs=in_specs, out_specs=out_specs, check_vma=False)
```

```python
import functools

import jax
import jax.numpy as jnp
from jax import lax
from jax.experimental import pallas as pl
from jax.experimental.pallas import tpu as pltpu
from jax.sharding import PartitionSpec as P

NORM_EPS = 1e-5
MASK_VALUE = -1e30
HEAD = 64
KV_HEADS = 3
GROUP = 3
SEQ = 256
DIM = 576
FFN = 1536
QKV = 960
BF = jnp.bfloat16
F32 = jnp.float32


def dot(a, b, dims=((1,), (0,))):
    return lax.dot_general(a, b, (dims, ((), ())), preferred_element_type=F32)


def params(**kw):
    return pltpu.CompilerParams(dimension_semantics=("arbitrary",), vmem_limit_bytes=60 * 1024 * 1024, **kw)


def cost(flops, bytes_accessed):
    return pl.CostEstimate(flops=int(flops), bytes_accessed=int(bytes_accessed), transcendentals=0)


def shape(dims, dtype):
    return jax.ShapeDtypeStruct(dims, dtype)


def whole(dims):
    return pl.BlockSpec(dims, lambda i: (0,) * len(dims))


def rows(dims):
    return pl.BlockSpec((1,) + dims, lambda i: (i,) + (0,) * len(dims))


def inv_rms(vals32):
    return lax.rsqrt(jnp.mean(vals32 * vals32, axis=-1, keepdims=True) + NORM_EPS)


def rms_back(vals32, inv, gain, grad_normed):
    scaled = vals32 * inv
    grad_scaled = grad_normed * gain
    grad_gain = jnp.sum(grad_normed * scaled, axis=0, keepdims=True)
    return inv * (grad_scaled - scaled * jnp.mean(grad_scaled * scaled, axis=-1, keepdims=True)), grad_gain


def rope(vals32, cos, sin):
    lane = lax.broadcasted_iota(jnp.int32, vals32.shape, 1)
    swapped = jnp.where(lane % HEAD < HEAD // 2, pltpu.roll(vals32, 96, 1), pltpu.roll(vals32, 32, 1))
    return vals32 * cos + swapped * sin


MESH = pl.DeviceIdType.MESH
ANY = pl.BlockSpec(memory_space=pl.ANY)


class Part:
    def __init__(self, x_first, r, c, lo=0):
        self.x_first, self.r, self.c, self.lo = x_first, r, c, lo


class Gather:
    def __init__(self, x_first, r, c, srcs, specs, fill):
        self.x_first, self.r, self.c, self.srcs, self.specs, self.fill = x_first, r, c, srcs, specs, fill


def gather_of(x_first, layer, masters):
    widths = [m.shape[2] for m in masters]

    def fill(refs, dst):
        lo = 0
        for ref, width in zip(refs, widths):
            dst[:, lo:lo + width] = ref[0].astype(BF)
            lo += width

    specs = [pl.BlockSpec((1,) + m.shape[1:], lambda i: (layer, 0, 0)) for m in masters]
    return Gather(x_first, masters[0].shape[1], sum(widths), list(masters), specs, fill)


def gather_gains(gain_attn, gain_mlp):
    layers, r = gain_attn.shape

    def fill(refs, dst):
        dst[...] = jnp.zeros(dst.shape, BF)
        dst[0:layers, 0:r] = refs[0][...].astype(BF)
        dst[layers:2 * layers, 0:r] = refs[1][...].astype(BF)

    return Gather(True, 16, 128, [gain_attn, gain_mlp], [whole((layers, r))] * 2, fill)


def fused(body, steps, ins, in_specs, outs, out_specs, scratch, ca, bs, finish, cid, name, flops, ag=(), forward=2):
    n_ca, n_b = len(ca), len(bs)
    n_in, n_out, n_scr = len(ins), len(outs), len(scratch)
    n_g = len(ag)
    comm = n_ca + n_b + n_g > 0
    last = steps - 1

    def kernel(*refs):
        refs = list(refs)
        take = lambda k: [refs.pop(0) for _ in range(k)]
        in_refs = take(n_in)
        ca_in = [take(2) for _ in range(n_ca)]
        b_in = take(n_b)
        g_in = [take(len(g.srcs)) for g in ag]
        out_refs = take(n_out)
        ca_out = take(n_ca)
        b_out = take(n_b)
        g_out = take(n_g)
        scr = take(n_scr)
        ca_scr = [take(4 if finish else 3) for _ in range(n_ca)]
        b_scr = [take(2) for _ in range(n_b)]
        g_own = take(n_g)
        step = pl.program_id(0)
        me = lax.axis_index("fsdp")
        core, x_bit, y_bit = lax.rem(me, 2), lax.rem(me // 2, 2), me // 4
        if not comm:
            body(step, last, core, in_refs, out_refs, scr)
            return
        s_mine, s_cs, s_cr, s_as, s_ar, s_bs, s_br, s_keep, s_gl, s_gs, s_gr = take(11)
        pair, x_dev, y_dev = me + 1 - 2 * core, me + 2 - 4 * x_bit, me + 4 - 8 * y_bit

        def remote(src, dst, send, recv, dev):
            return pltpu.make_async_remote_copy(src_ref=src, dst_ref=dst, send_sem=send, recv_sem=recv, device_id=(dev,), device_id_type=MESH)

        def geometry(part):
            if part.x_first:
                return (lambda j: 2 * j + 1 - x_bit), (lambda j: 2 * j + x_bit), x_dev, y_bit, y_dev
            return (lambda j: 2 * (1 - y_bit) + j), (lambda j: 2 * y_bit + j), y_dev, x_bit, x_dev

        def core_copies(t):
            part, (mine, theirs), bufs = ca[t][0], ca_in[t], ca_scr[t]
            span = pl.ds(part.lo, part.r)
            local = pltpu.make_async_copy(mine.at[:, span], bufs[0], s_mine.at[t])
            return local, remote(theirs.at[:, span], bufs[1], s_cs.at[t], s_cr.at[t], pair)

        def first_copies(t):
            send_block, _, dev, _, _ = geometry(ca[t][0])
            bufs = ca_scr[t]
            return [remote(bufs[1].at[send_block(j)], bufs[2].at[j], s_as.at[t, j], s_ar.at[t, j], dev) for j in range(2)]

        def second_copy(t):
            part = (ca[t] if t < n_ca else bs[t - n_ca])[0]
            _, _, _, bit, dev = geometry(part)
            if t < n_ca:
                return remote(ca_scr[t][2].at[1 - bit], ca_scr[t][3], s_bs.at[t], s_br.at[t], dev)
            return remote(b_in[t - n_ca].at[1 - bit], b_scr[t - n_ca][1], s_bs.at[t], s_br.at[t], dev)

        def keep_copy(t):
            _, _, _, bit, _ = geometry(bs[t][0])
            return pltpu.make_async_copy(b_in[t].at[bit], b_scr[t][0], s_keep.at[t])

        def g_copy(t, k):
            g, own, full = ag[t], g_own[t], g_out[t]
            one, two = (x_dev, y_dev) if g.x_first else (y_dev, x_dev)
            blk = (me, me, me, one, one, two, one + two - me)[k]
            dev = (one, two, pair, two, pair, pair, pair)[k]
            return remote(own if k < 3 else full.at[blk], full.at[blk], s_gs.at[t, k], s_gr.at[t, k], dev)

        def g_local(t):
            return pltpu.make_async_copy(g_own[t], g_out[t].at[me], s_gl.at[t])

        def g_forward():
            for t in range(n_g):
                g_copy(t, 0).wait_recv()
                g_copy(t, 3).start()
                g_copy(t, 4).start()
            for t in range(n_g):
                g_copy(t, 1).wait_recv()
                g_copy(t, 5).start()

        def g_end():
            for t in range(n_g):
                g_copy(t, 3).wait_recv()
                g_copy(t, 6).start()
            for t in range(n_g):
                for k in (2, 4, 5, 6):
                    g_copy(t, k).wait_recv()
                for k in range(7):
                    g_copy(t, k).wait_send()
                g_local(t).wait()

        def begin():
            for t in range(n_g):
                ag[t].fill(g_in[t], g_own[t])
            barrier = pltpu.get_barrier_semaphore()
            for dev in (pair, x_dev, y_dev):
                pl.semaphore_signal(barrier, inc=1, device_id=(dev,), device_id_type=MESH)
            pl.semaphore_wait(barrier, 3)
            for t in range(n_g):
                for k in range(3):
                    g_copy(t, k).start()
                g_local(t).start()
            for t in range(n_b):
                second_copy(n_ca + t).start()
            for t in range(n_ca):
                for copy in core_copies(t):
                    copy.start()
            for t in range(n_b):
                keep_copy(t).start()

        def middle():
            for t in range(n_ca):
                send_block, keep_block, _, _, _ = geometry(ca[t][0])
                for copy in core_copies(t):
                    copy.wait()
                copies = first_copies(t)
                mine_v, sums = ca_scr[t][0], ca_scr[t][1]
                for j in range(2):
                    sums[send_block(j)] = sums[send_block(j)] + mine_v[send_block(j)]
                    copies[j].start()
                for j in range(2):
                    sums[keep_block(j)] = sums[keep_block(j)] + mine_v[keep_block(j)]

        def end():
            for t in range(n_ca):
                _, keep_block, _, bit, _ = geometry(ca[t][0])
                copies = first_copies(t)
                sums, arrived = ca_scr[t][1], ca_scr[t][2]
                for j in range(2):
                    copies[j].wait()
                if not finish:
                    for j in range(2):
                        ca_out[t][j] = arrived[j] + sums[keep_block(j)]
                else:
                    for j in range(2):
                        arrived[j] = arrived[j] + sums[keep_block(j)]
                    second_copy(t).start()
            for t in range(n_b):
                second_copy(n_ca + t).wait()
                keep_copy(t).wait()
                b_out[t][...] = b_scr[t][0][...] + b_scr[t][1][...]
            if finish:
                for t in range(n_ca):
                    _, _, _, bit, _ = geometry(ca[t][0])
                    second_copy(t).wait()
                    ca_out[t][...] = ca_scr[t][2][bit] + ca_scr[t][3][...]

        if steps == 1:
            begin()
            if n_g:
                g_forward()
            middle()
            end()
            if n_g:
                g_end()
            return
        pl.when(step == 0)(begin)
        if n_ca:
            pl.when(step == 1)(middle)
        if n_g:
            pl.when(step == forward)(g_forward)
        body(step, last, core, in_refs, out_refs, scr)
        if n_ca + n_b:
            pl.when(step == last)(end)
        if n_g:
            pl.when(step == last)(g_end)

    args = list(ins)
    in_specs, out_specs, outs, scratch = list(in_specs), list(out_specs), list(outs), list(scratch)
    for part, mine, theirs in ca:
        args += [mine, theirs]
        in_specs += [ANY, ANY]
        dims = (part.r, part.c) if finish else (2, part.r, part.c)
        outs.append(shape(dims, F32))
        out_specs.append(whole(dims))
        scratch += [pltpu.VMEM((4, part.r, part.c), F32), pltpu.VMEM((4, part.r, part.c), F32), pltpu.VMEM((2, part.r, part.c), F32)]
        if finish:
            scratch.append(pltpu.VMEM((part.r, part.c), F32))
    for part, kept in bs:
        args.append(kept)
        in_specs.append(ANY)
        outs.append(shape((part.r, part.c), F32))
        out_specs.append(whole((part.r, part.c)))
        scratch += [pltpu.VMEM((part.r, part.c), F32), pltpu.VMEM((part.r, part.c), F32)]
    for g in ag:
        args += g.srcs
        in_specs += g.specs
        outs.append(shape((8, g.r, g.c), BF))
        out_specs.append(ANY)
        scratch.append(pltpu.VMEM((g.r, g.c), BF))
    extra = {}
    if comm:
        g_n = max(n_g, 1)
        sem = pltpu.SemaphoreType.DMA
        a, t, k = max(n_ca, 1), max(n_ca + n_b, 1), max(n_b, 1)
        scratch += [sem((a,)), sem((a,)), sem((a,)), sem((a, 2)), sem((a, 2)), sem((t,)), sem((t,)), sem((k,)), sem((g_n,)), sem((g_n, 7)), sem((g_n, 7))]
        extra = dict(collective_id=cid, has_side_effects=True)
    return pl.pallas_call(
        kernel, grid=(steps,), in_specs=in_specs, out_specs=out_specs, out_shape=outs, scratch_shapes=scratch,
        compiler_params=params(**extra), cost_estimate=cost(flops, 2e7), name=name)(*args)


CHUNK = 512


def stack_heads(ref, kv, lo):
    return jnp.concatenate([ref[lo:lo + SEQ // 2, HEAD * head:HEAD * (head + 1)] for head in range(GROUP * kv, GROUP * (kv + 1))], axis=0)


P_DIMS = ((KV_HEADS, GROUP * SEQ // 2, SEQ // 2), (KV_HEADS, GROUP * SEQ // 2, SEQ))


def attn_fwd_body(step, last, core, ins, outs, scratch):
    x_ref, wqkv_ref, wo_ref, gain_ref, cos_ref, sin_ref = ins
    h_ref, qkv_ref, p0_ref, p1_ref, o_ref = outs
    x32 = x_ref[0].astype(F32)
    normed = (x32 * inv_rms(x32) * gain_ref[...]).astype(BF)
    proj = dot(normed, wqkv_ref[...])
    cos, sin = cos_ref[...], sin_ref[...]
    for i in range(6):
        qkv_ref[0, :, 128 * i:128 * (i + 1)] = rope(proj[:, 128 * i:128 * (i + 1)], cos, sin).astype(BF)
    qkv_ref[0, :, 768:QKV] = proj[:, 768:QKV].astype(BF)
    half = SEQ // 2
    causal = lax.broadcasted_iota(jnp.int32, (GROUP * half, half), 0) % half >= lax.broadcasted_iota(jnp.int32, (GROUP * half, half), 1)
    for kv in range(KV_HEADS):
        keys = qkv_ref[0, :, DIM + HEAD * kv:DIM + HEAD * (kv + 1)]
        vals = qkv_ref[0, :, 768 + HEAD * kv:768 + HEAD * (kv + 1)]
        for blk, p_ref in enumerate((p0_ref, p1_ref)):
            lo, length = half * blk, half * (blk + 1)
            s = dot(stack_heads(qkv_ref.at[0], kv, lo), keys[:length], ((1,), (1,))) * HEAD ** -0.5
            diag = jnp.where(causal, s[:, lo:], MASK_VALUE)
            s = diag if blk == 0 else jnp.concatenate([s[:, :lo], diag], axis=1)
            e = jnp.exp(s - jnp.max(s, axis=-1, keepdims=True))
            p = (e * (1.0 / jnp.sum(e, axis=-1, keepdims=True))).astype(BF)
            p_ref[0, kv] = p
            o = dot(p, vals[:length]).astype(BF)
            for g in range(GROUP):
                head = GROUP * kv + g
                o_ref[0, lo:lo + half, HEAD * head:HEAD * (head + 1)] = o[half * g:half * (g + 1)]
    h_ref[0] = (x32 + dot(o_ref[0], wo_ref[...])).astype(BF)


def attn_fwd(x, wqkv, wo, gain, cos, sin, ag, cid):
    n = x.shape[0]
    return fused(
        attn_fwd_body, n, [x, wqkv, wo, gain, cos, sin],
        [rows((SEQ, DIM)), whole(wqkv.shape), whole(wo.shape), whole(gain.shape), whole(cos.shape), whole(sin.shape)],
        [shape((n, SEQ, DIM), BF), shape((n, SEQ, QKV), BF), shape((n,) + P_DIMS[0], BF), shape((n,) + P_DIMS[1], BF), shape((n, SEQ, DIM), BF)],
        [rows((SEQ, DIM)), rows((SEQ, QKV)), rows(P_DIMS[0]), rows(P_DIMS[1]), rows((SEQ, DIM))],
        [], [], [], False, cid, "attn_fwd", 5e9, ag)


def mlp_fwd_body(step, last, core, ins, outs, scratch):
    h_ref, w1_ref, w3_ref, w2_ref, gain_ref = ins
    (y_ref,), (act_ref,) = outs, scratch
    h32 = h_ref[0].astype(F32)
    normed = (h32 * inv_rms(h32) * gain_ref[...]).astype(BF)
    for c in range(0, FFN, CHUNK):
        gate = dot(normed, w1_ref[:, c:c + CHUNK])
        up = dot(normed, w3_ref[:, c:c + CHUNK])
        act_ref[:, c:c + CHUNK] = (gate * jax.nn.sigmoid(gate) * up).astype(BF)
    y_ref[0] = (h32 + dot(act_ref[...], w2_ref[...])).astype(BF)


def mlp_fwd(h, w1, w3, w2, gain, ag, cid):
    n = h.shape[0]
    return fused(
        mlp_fwd_body, n, [h, w1, w3, w2, gain],
        [rows((SEQ, DIM)), whole(w1.shape), whole(w3.shape), whole(w2.shape), whole(gain.shape)],
        [shape((n, SEQ, DIM), BF)], [rows((SEQ, DIM))], [pltpu.VMEM((SEQ, FFN), BF)],
        [], [], False, cid, "mlp_fwd", 6e9, ag)


WIDE = 512


def mlp_bwd_body(step, last, core, ins, outs, scratch):
    h_ref, dy_ref, w1_ref, w3_ref, w2_ref, gain_ref = ins
    gm_ref, gg_ref, down_mine, down_theirs, gate_mine, gate_theirs, up_mine, up_theirs, *y_ref = outs
    nt_ref, at_ref, act_ref, dgate_ref, dup_ref, dy_all = scratch
    steps = dy_all.shape[0] // SEQ

    @pl.when(step < steps)
    def _():
        h32 = h_ref[0].astype(F32)
        inv = inv_rms(h32)
        gain = gain_ref[...]
        normed = (h32 * inv * gain).astype(BF)
        tokens = pl.ds(pl.multiple_of(step * SEQ, SEQ), SEQ)
        nt_ref[:, tokens] = normed.T
        dy = dy_ref[0]
        dy_all[tokens] = dy
        for c in range(0, FFN, CHUNK):
            cols = slice(c, c + CHUNK)
            gate = dot(normed, w1_ref[:, cols])
            up = dot(normed, w3_ref[:, cols])
            grad_act = dot(dy, w2_ref[cols, :], ((1,), (1,)))
            sig = jax.nn.sigmoid(gate)
            silu = gate * sig
            act = (silu * up).astype(BF)
            act_ref[:, cols] = act
            at_ref[cols, tokens] = act.T
            dup_ref[tokens, cols] = (grad_act * silu).astype(BF)
            dgate_ref[tokens, cols] = (grad_act * up * sig * (1.0 + gate * (1.0 - sig))).astype(BF)
        if y_ref:
            y_ref[0][0] = (h32 + dot(act_ref[...], w2_ref[...])).astype(BF)
        grad_normed = dot(dgate_ref[tokens], w1_ref[...], ((1,), (1,))) + dot(dup_ref[tokens], w3_ref[...], ((1,), (1,)))
        grad_h, grad_gain = rms_back(h32, inv, gain, grad_normed)
        gm_ref[0] = dy.astype(F32) + grad_h
        gg_ref[0] = grad_gain

    @pl.when((step >= steps) & (step < steps + 4))
    def _():
        span = 2 * FFN // 8
        full = dot(at_ref[pl.ds(pl.multiple_of((step - steps) * span, span), span)], dy_all[...])
        split_rows(full, core, down_mine, down_theirs)

    @pl.when(step >= steps + 4)
    def _():
        cols = pl.ds(pl.multiple_of((step - steps - 4) * WIDE, WIDE), WIDE)
        split_rows(dot(nt_ref[...], dgate_ref[:, cols]), core, gate_mine, gate_theirs)
        split_rows(dot(nt_ref[...], dup_ref[:, cols]), core, up_mine, up_theirs)


def mlp_bwd(h, dy, w1, w3, w2, gain, with_out, ca, bs, cid):
    n = h.shape[0]
    tok = n * SEQ
    extra = 1 if with_out else 0
    r, rd = DIM // 8, FFN // 8
    early = lambda dims: pl.BlockSpec((1,) + dims, lambda i: (jnp.minimum(i, n - 1),) + (0,) * len(dims))
    down = pl.BlockSpec((1, rd, DIM), lambda i: (jnp.clip(i - n, 0, 3), 0, 0))
    wide = pl.BlockSpec((4, r, WIDE), lambda i: (0, 0, jnp.clip(i - n - 4, 0, FFN // WIDE - 1)))
    return fused(
        mlp_bwd_body, n + 4 + FFN // WIDE, [h, dy, w1, w3, w2, gain],
        [early((SEQ, DIM)), early((SEQ, DIM)), whole(w1.shape), whole(w3.shape), whole(w2.shape), whole(gain.shape)],
        [shape((n, SEQ, DIM), F32), shape((n, 1, DIM), F32)] + [shape((4, rd, DIM), F32)] * 2 + [shape((4, r, FFN), F32)] * 4 + [shape((n, SEQ, DIM), BF)] * extra,
        [early((SEQ, DIM)), early((1, DIM)), down, down, wide, wide, wide, wide] + [early((SEQ, DIM))] * extra,
        [pltpu.VMEM((DIM, tok), BF), pltpu.VMEM((FFN, tok), BF), pltpu.VMEM((SEQ, FFN), BF), pltpu.VMEM((tok, FFN), BF), pltpu.VMEM((tok, FFN), BF), pltpu.VMEM((tok, DIM), BF)],
        ca, bs, False, cid, "mlp_bwd", 2e10)


def split_rows(full, core, mine_ref, theirs_ref):
    blocks, r = mine_ref.shape[0], mine_ref.shape[1]

    @pl.when(core == 0)
    def _():
        for i in range(blocks):
            mine_ref[i] = full[2 * i * r:(2 * i + 1) * r]
            theirs_ref[i] = full[(2 * i + 1) * r:(2 * i + 2) * r]

    @pl.when(core == 1)
    def _():
        for i in range(blocks):
            theirs_ref[i] = full[2 * i * r:(2 * i + 1) * r]
            mine_ref[i] = full[(2 * i + 1) * r:(2 * i + 2) * r]


def attn_bwd_body(step, last, core, ins, outs, scratch):
    gm_ref, x_ref, qkv_ref, p0_ref, p1_ref, o_ref, wqkv_ref, wo_ref, gain_ref, cos_ref, sin_ref = ins
    dx_ref, gg_ref, qkv_mine, qkv_theirs, out_mine, out_theirs = outs
    do_ref, dqk_ref, dqkv_ref, acc_qkv, acc_out = scratch
    gm = gm_ref[0]
    gmb = gm.astype(BF)
    x32 = x_ref[0].astype(F32)
    inv = inv_rms(x32)
    gain = gain_ref[...]
    normed = (x32 * inv * gain).astype(BF)
    do_ref[...] = dot(gmb, wo_ref[...], ((1,), (1,))).astype(BF)
    half = SEQ // 2
    for kv in range(KV_HEADS):
        kcol = DIM + HEAD * kv
        vcol = 768 + HEAD * kv
        keys = qkv_ref[0, :, kcol:kcol + HEAD]
        vals = qkv_ref[0, :, vcol:vcol + HEAD]
        dk, dv = [], []
        for blk, p_ref in enumerate((p0_ref, p1_ref)):
            lo, length = half * blk, half * (blk + 1)
            p = p_ref[0, kv]
            d_o = stack_heads(do_ref, kv, lo)
            q = stack_heads(qkv_ref.at[0], kv, lo)
            dp = dot(d_o, vals[:length], ((1,), (1,)))
            p32 = p.astype(F32)
            ds = (p32 * (dp - jnp.sum(p32 * dp, axis=-1, keepdims=True)) * HEAD ** -0.5).astype(BF)
            dq = dot(ds, keys[:length])
            for g in range(GROUP):
                head = GROUP * kv + g
                dqk_ref[lo:lo + half, HEAD * head:HEAD * (head + 1)] = dq[half * g:half * (g + 1)]
            dk.append(dot(q, ds, ((0,), (0,))))
            dv.append(dot(d_o, p, ((0,), (0,))))
        dk, dv = [jnp.concatenate([a[0] + a[1][:, :half], a[1][:, half:]], axis=1).T for a in (dk, dv)]
        dqk_ref[:, kcol:kcol + HEAD] = dk
        dqkv_ref[:, vcol:vcol + HEAD] = dv.astype(BF)
    cos, sin = cos_ref[...], -sin_ref[...]
    for i in range(6):
        cols = slice(128 * i, 128 * (i + 1))
        dqkv_ref[:, cols] = rope(dqk_ref[:, cols], cos, sin).astype(BF)
    grad_normed = dot(dqkv_ref[...], wqkv_ref[...], ((1,), (1,)))
    grad_x, grad_gain = rms_back(x32, inv, gain, grad_normed)
    dx_ref[0] = (gm + grad_x).astype(BF)
    gg_ref[0] = grad_gain
    part_qkv = dot(normed, dqkv_ref[...], ((0,), (0,)))
    part_out = dot(o_ref[0], gmb, ((0,), (0,)))

    @pl.when(step == 0)
    def _():
        acc_qkv[...] = part_qkv
        acc_out[...] = part_out

    @pl.when(step > 0)
    def _():
        acc_qkv[...] += part_qkv
        acc_out[...] += part_out

    @pl.when(step == last)
    def _():
        split_rows(acc_qkv, core, qkv_mine, qkv_theirs)
        split_rows(acc_out, core, out_mine, out_theirs)


def attn_bwd(gm, x, qkv, p0, p1, o, wqkv, wo, gain, cos, sin, ca, bs, cid):
    n = x.shape[0]
    r = DIM // 8
    return fused(
        attn_bwd_body, n, [gm, x, qkv, p0, p1, o, wqkv, wo, gain, cos, sin],
        [rows((SEQ, DIM)), rows((SEQ, DIM)), rows((SEQ, QKV)), rows(P_DIMS[0]), rows(P_DIMS[1]), rows((SEQ, DIM)), whole(wqkv.shape), whole(wo.shape), whole(gain.shape), whole(cos.shape), whole(sin.shape)],
        [shape((n, SEQ, DIM), BF), shape((n, 1, DIM), F32), shape((4, r, QKV), F32), shape((4, r, QKV), F32), shape((4, r, DIM), F32), shape((4, r, DIM), F32)],
        [rows((SEQ, DIM)), rows((1, DIM)), whole((4, r, QKV)), whole((4, r, QKV)), whole((4, r, DIM)), whole((4, r, DIM))],
        [pltpu.VMEM((SEQ, DIM), BF), pltpu.VMEM((SEQ, 768), F32), pltpu.VMEM((SEQ, QKV), BF), pltpu.VMEM((DIM, QKV), F32), pltpu.VMEM((DIM, DIM), F32)],
        ca, bs, False, cid, "attn_bwd", 1e10)


def pick(stacked, index, axis):
    return lax.dynamic_index_in_dim(stacked, index, axis, keepdims=False)


def solution(mesh):
    shard_spec = P(None, "fsdp")
    batch_spec = P("fsdp")

    def local_step(w_query, w_key, w_value, w_out, w_gate, w_up, w_down, gain_attn, gain_mlp, rope_cos, rope_sin, x_in, y_cot):
        me = lax.axis_index("fsdp")
        bits = (me % 2, (me // 2) % 2, me // 4)
        num_layers = w_query.shape[0]
        cos = jnp.tile(rope_cos, (1, 4))
        sin = jnp.concatenate([-rope_sin, rope_sin, -rope_sin, rope_sin], 1)
        attn_ag = lambda i: [gather_of(False, i, (w_query, w_key, w_value)), gather_of(True, i, (w_out,))]
        mlp_ag = lambda i: [gather_of(True, i, (w_gate,)), gather_of(False, i, (w_up,)), gather_of(i == 0, i, (w_down,))]
        merge = lambda v: v.reshape(-1, v.shape[2])
        first = fused(None, 1, [], [], [], [], [], [], [], False, 10, "ag_head", 1e6, attn_ag(0) + [gather_gains(gain_attn, gain_mlp)])
        attn_w = [merge(v) for v in first[:2]]
        gains = first[2][:, :2 * num_layers, :w_query.shape[1]].astype(F32).transpose(1, 0, 2).reshape(2 * num_layers, 1, DIM)
        weights = []
        hidden = x_in
        saved = []
        for i in range(num_layers):
            g1, g2 = gains[i], gains[num_layers + i]
            mid, qkv, p0, p1, attn, *mlp_w = attn_fwd(hidden, *attn_w, g1, cos, sin, mlp_ag(i), 11 + 2 * i)
            mlp_w = [merge(v) for v in mlp_w]
            weights.append((*attn_w, *mlp_w, g1, g2))
            saved.append((hidden, mid, qkv, p0, p1, attn))
            if i < num_layers - 1:
                hidden, *attn_w = mlp_fwd(mid, *mlp_w, g2, attn_ag(i + 1), 12 + 2 * i)
                attn_w = [merge(v) for v in attn_w]
        grad = y_cot
        grads = [None] * num_layers
        gain_grads = []
        y_out = None
        r, rd = w_query.shape[1], w_down.shape[1]
        pending = []
        done = {}
        for i in reversed(range(num_layers)):
            qkv_w, out_w, gate_w, up_w, down_w, g1, g2 = weights[i]
            hidden, mid, qkv, p0, p1, attn = saved[i]
            last = i == num_layers - 1
            ca, bs = pending if pending else ([], [])
            res = mlp_bwd(mid, grad, gate_w, up_w, down_w, g2, last, ca, bs, 2 * i)
            gm, gg2 = res[:2]
            d_down, d_gate, d_up = res[2:4], res[4:6], res[6:8]
            if last:
                y_out = res[8]
            kept = [(p[0], v) for p, v in zip(ca, res[len(res) - len(ca) - len(bs):])]
            done[i + 1, "mlp"] = res[len(res) - len(bs):]
            ca = [(Part(True, rd // 2, DIM, 0), *d_down), (Part(False, rd // 2, DIM, rd // 2), *d_down),
                  (Part(True, r, FFN), *d_gate), (Part(False, r, FFN), *d_up)]
            res = attn_bwd(gm, hidden, qkv, p0, p1, attn, qkv_w, out_w, g1, cos, sin, ca, kept, 2 * i + 1)
            grad, gg1, q_mine, q_theirs, o_mine, o_theirs = res[:6]
            done[i + 1, "attn"] = res[6 + len(ca):]
            bs = [(p[0], v) for p, v in zip(ca, res[6:6 + len(ca)])]
            ca = [(Part(i == 0, r, QKV), q_mine, q_theirs), (Part(i == 1, r, DIM), o_mine, o_theirs)]
            pending = (ca, bs)
            gain_grads = [gg1.sum((0, 1)), gg2.sum((0, 1))] + gain_grads
        gains = jnp.stack(gain_grads).reshape(2 * num_layers, 4, 2, r)
        gains = jnp.pad(gains.transpose(2, 1, 0, 3).reshape(2, 4, 2 * num_layers * r), ((0, 0), (0, 0), (0, 1024 - 2 * num_layers * r))).reshape(2, 4, 8, 128)
        ca, bs = pending
        ca = ca + [(Part(True, 8, 128), pick(gains, bits[0], 0), pick(gains, 1 - bits[0], 0))]
        res = fused(None, 1, [], [], [], [], [], ca, bs, True, 2 * num_layers, "rs_tail", 1e6)
        done[0, "attn"] = res[:2]
        done[0, "mlp"] = res[3:]
        s_gains = res[2].reshape(1024)[:2 * num_layers * r].reshape(2 * num_layers, r)
        for i in range(num_layers):
            s_qkv, s_out = done[i, "attn"]
            down0, down1, s_gate, s_up = done[i, "mlp"]
            grads[i] = (s_qkv[:, :576], s_qkv[:, 576:768], s_qkv[:, 768:960], s_out, s_gate, s_up, jnp.concatenate([down0, down1], 0))
        stacked = tuple(jnp.stack(parts) for parts in zip(*grads))
        return (y_out, grad) + stacked + (s_gains[0::2], s_gains[1::2])

    in_specs = (shard_spec,) * 9 + (P(), P(), batch_spec, batch_spec)
    out_specs = (batch_spec, batch_spec) + (shard_spec,) * 9
    return jax.shard_map(local_step, mesh=mesh, in_specs=in_specs, out_specs=out_specs, check_vma=False)
```

```python
import functools

import jax
import jax.numpy as jnp
from jax import lax
from jax.experimental import pallas as pl
from jax.experimental.pallas import tpu as pltpu
from jax.sharding import PartitionSpec as P

NORM_EPS = 1e-5
MASK_VALUE = -1e30
HEAD = 64
LAST = dict(axis=-1, keepdims=True)
KV_HEADS = 3
GROUP = 3
SEQ = 256
DIM = 576
FFN = 1536
QKV = 960
BF = jnp.bfloat16
F32 = jnp.float32


ROWS = ((1,), (1,))
COLS = ((0,), (0,))
PAIR = range(2)
HALF = SEQ // 2
LANES = 128
V_COL = DIM + KV_HEADS * HEAD


def origin(dims):
    return (0,) * len(dims)


def nth(width, index):
    return slice(width * index, width * (index + 1))


def dot(a, b, dims=((1,), (0,))):
    return lax.dot_general(a, b, (dims, ((), ())), preferred_element_type=F32)


def params(**kw):
    return pltpu.CompilerParams(dimension_semantics=("arbitrary",), vmem_limit_bytes=60 * 1024 * 1024, **kw)


def cost(flops, bytes_accessed):
    return pl.CostEstimate(flops=int(flops), bytes_accessed=int(bytes_accessed), transcendentals=0)


def shape(dims, dtype):
    return jax.ShapeDtypeStruct(dims, dtype)


def whole(dims):
    return pl.BlockSpec(dims, lambda i: origin(dims), pipeline_mode=pl.Buffered(1))


def rows(dims, base=0):
    return pl.BlockSpec((1,) + dims, lambda i: (i + base,) + origin(dims))


def one_of(dims, index):
    return pl.BlockSpec((1,) + dims, lambda i: (index,) + origin(dims), pipeline_mode=pl.Buffered(1))


def inv_rms(vals32):
    return lax.rsqrt(jnp.mean(vals32 * vals32, **LAST) + NORM_EPS)


def rms_back(vals32, inv, gain, grad_normed):
    scaled = vals32 * inv
    grad_scaled = grad_normed * gain
    grad_gain = jnp.sum(grad_normed * scaled, axis=0, keepdims=True)
    return inv * (grad_scaled - scaled * jnp.mean(grad_scaled * scaled, **LAST)), grad_gain


def rope(vals32, cos, sin):
    lane = lax.broadcasted_iota(jnp.int32, vals32.shape, 1)
    swapped = jnp.where(lane % HEAD < HEAD // 2, pltpu.roll(vals32, 96, 1), pltpu.roll(vals32, 32, 1))
    return vals32 * cos + swapped * sin


MESH = pl.DeviceIdType.MESH
ANY = pl.BlockSpec(memory_space=pl.ANY)


class Part:
    def __init__(self, x_first, r, c, stages, at, arrays=(), local=(), lo=0):
        self.x_first, self.r, self.c, self.stages, self.at = x_first, r, c, stages, at
        self.arrays, self.local, self.lo = list(arrays), list(local), lo
        full, two, one = (4, r, c), (2, r, c), (r, c)
        self.result = {"c": full, "a": two, "b": one}[stages[-1]]
        self.bufs = {}
        if "c" in stages:
            self.bufs["recv_c"] = full
            if not local:
                self.bufs["mine"] = full
        if "a" in stages:
            self.bufs["recv_a"] = two
        if "b" in stages:
            self.bufs["recv_b"] = one
        if stages[0] != "c":
            self.bufs["keep"] = two if stages[0] == "a" else one


class Gather:
    def __init__(self, x_first, r, c, srcs, specs, fill):
        self.x_first, self.r, self.c, self.srcs, self.specs, self.fill = x_first, r, c, srcs, specs, fill


def gather_of(x_first, layer, masters):
    widths = [m.shape[2] for m in masters]

    def fill(refs, dst):
        lo = 0
        for ref, width in zip(refs, widths):
            dst[:, lo:lo + width] = ref[0].astype(BF)
            lo += width

    specs = [pl.BlockSpec((1,) + m.shape[1:], lambda i: (layer, 0, 0)) for m in masters]
    return Gather(x_first, masters[0].shape[1], sum(widths), list(masters), specs, fill)


def gather_gains(gain_attn, gain_mlp):
    layers, r = gain_attn.shape

    def fill(refs, dst):
        dst[:] = jnp.zeros(dst.shape, BF)
        dst[0:layers, 0:r] = refs[0][:].astype(BF)
        dst[layers:2 * layers, 0:r] = refs[1][:].astype(BF)

    return Gather(True, 16, 128, [gain_attn, gain_mlp], [whole((layers, r))] * 2, fill)


def fused(body, steps, ins, in_specs, outs, out_specs, scratch, parts, cid, name, flops):
    n_in, n_out, n_scr, n_p = len(ins), len(outs), len(scratch), len(parts)
    comm = n_p > 0
    last = steps - 1

    def kernel(*refs):
        refs = list(refs)
        take = lambda k: [refs.pop(0) for _ in range(k)]
        in_refs = take(n_in)
        p_in = [take(len(p.arrays)) for p in parts]
        out_refs = take(n_out)
        p_out = take(n_p)
        scr = take(n_scr)
        p_scr = [dict(zip(p.bufs, take(len(p.bufs)))) for p in parts]
        step = pl.program_id(0)
        me = lax.axis_index("fsdp")
        core, x_bit, y_bit = lax.rem(me, 2), lax.rem(me // 2, 2), me // 4
        if not comm:
            body(step, last, core, in_refs, out_refs, scr)
            return
        (p_sem,) = take(1)
        pair, x_dev, y_dev = me + 1 - 2 * core, me + 2 - 4 * x_bit, me + 4 - 8 * y_bit

        def remote(src, dst, send, recv, dev):
            return pltpu.make_async_remote_copy(src_ref=src, dst_ref=dst, send_sem=send, recv_sem=recv, device_id=(dev,), device_id_type=MESH)

        def stages_of(t):
            part, bufs, arrays, out = parts[t], p_scr[t], p_in[t], p_out[t]
            sem = lambda k: p_sem.at[t, k]
            if part.x_first:
                sent, kept, dev_a, bit, dev_b = (lambda j: 2 * j + 1 - x_bit), (lambda j: 2 * j + x_bit), x_dev, y_bit, y_dev
            else:
                sent, kept, dev_a, bit, dev_b = (lambda j: 2 * (1 - y_bit) + j), (lambda j: 2 * y_bit + j), y_dev, x_bit, x_dev
            first, end = part.stages[0], part.stages[-1]
            span = pl.ds(part.lo, part.r)

            def copy_c():
                theirs = scr[part.local[1]] if part.local else arrays[1]
                return remote(theirs.at[:, span], bufs["recv_c"], sem(1), sem(2), pair)

            def copy_mine():
                return pltpu.make_async_copy(arrays[0].at[:, span], bufs["mine"], sem(0))

            def copy_a(j):
                src = arrays[0] if first == "a" else bufs["recv_c"]
                return remote(src.at[sent(j)], bufs["recv_a"].at[j], sem(3 + j), sem(5 + j), dev_a)

            def copy_keep(j):
                if first == "b":
                    return pltpu.make_async_copy(arrays[0].at[bit], bufs["keep"], sem(7))
                return pltpu.make_async_copy(arrays[0].at[kept(j)], bufs["keep"].at[j], sem(7 + j))

            def copy_b():
                src = arrays[0] if first == "b" else bufs["recv_a"]
                return remote(src.at[1 - bit], bufs["recv_b"], sem(9), sem(10), dev_b)

            def copy_out():
                return pltpu.make_async_copy(bufs["recv_" + end], out, sem(11))

            def mine_block(i):
                return scr[part.local[0]][i, part.lo:part.lo + part.r] if part.local else bufs["mine"][i]

            def begin():
                if first == "c":
                    copy_c().start()
                    if not part.local:
                        copy_mine().start()
                elif first == "a":
                    for j in PAIR:
                        copy_a(j).start()
                    for j in PAIR:
                        copy_keep(j).start()
                else:
                    copy_b().start()
                    copy_keep(0).start()

            def done_c():
                copy_c().wait()
                if not part.local:
                    copy_mine().wait()
                sums = bufs["recv_c"]
                for j in PAIR:
                    sums[sent(j)] = sums[sent(j)] + mine_block(sent(j))
                    if end != "c":
                        copy_a(j).start()
                for j in PAIR:
                    sums[kept(j)] = sums[kept(j)] + mine_block(kept(j))
                if end == "c":
                    copy_out().start()

            def done_a():
                for j in PAIR:
                    copy_a(j).wait()
                    if first == "a":
                        copy_keep(j).wait()
                for j in PAIR:
                    bufs["recv_a"][j] = bufs["recv_a"][j] + (bufs["keep"][j] if first == "a" else bufs["recv_c"][kept(j)])
                if end == "a":
                    copy_out().start()
                else:
                    copy_b().start()

            def done_b():
                copy_b().wait()
                if first == "b":
                    copy_keep(0).wait()
                bufs["recv_b"][:] = bufs["recv_b"][:] + (bufs["keep"][:] if first == "b" else bufs["recv_a"][bit])
                copy_out().start()

            calls = [begin] + [{"c": done_c, "a": done_a, "b": done_b}[stage] for stage in part.stages]
            return list(zip(part.at, calls)), copy_out

        def enter():
            barrier = pltpu.get_barrier_semaphore()
            for dev in (pair, x_dev, y_dev):
                pl.semaphore_signal(barrier, inc=1, device_id=(dev,), device_id_type=MESH)
            pl.semaphore_wait(barrier, 3)

        events = [(-1, enter)]
        outs_of = []
        for t in range(n_p):
            calls, copy_out = stages_of(t)
            events += calls
            outs_of.append(copy_out)
        events.sort(key=lambda event: event[0])

        def leave():
            for copy_out in outs_of:
                copy_out().wait()

        events.append((float("inf"), leave))
        if steps == 1:
            for _, call in events:
                call()
            return

        def at_step(lo, hi):
            calls = [call for at, call in events if lo <= at < hi]

            def run():
                for call in calls:
                    call()

            return run, len(calls)

        for index in range(steps):
            run, count = at_step(-1 if index == 0 else index, index + 1)
            if count:
                pl.when(step == index)(run)
        body(step, last, core, in_refs, out_refs, scr)
        pl.when(step == last)(at_step(steps, float("inf"))[0])
        pl.when(step == last)(leave)

    args = list(ins)
    in_specs, out_specs, outs, scratch = list(in_specs), list(out_specs), list(outs), list(scratch)
    for part in parts:
        args += part.arrays
        in_specs += [ANY] * len(part.arrays)
        outs.append(shape(part.result, F32))
        out_specs.append(ANY)
    for part in parts:
        scratch += [pltpu.VMEM(dims, F32) for dims in part.bufs.values()]
    extra = {}
    if comm:
        scratch += [pltpu.SemaphoreType.DMA((n_p, 12))]
        extra = dict(collective_id=cid, has_side_effects=True)
    return pl.pallas_call(
        kernel, grid=(steps,), in_specs=in_specs, out_specs=out_specs, out_shape=outs, scratch_shapes=scratch,
        compiler_params=params(**extra), cost_estimate=cost(flops, 2e7), name=name)(*args)


CHUNK = 512


def stack_heads(ref, kv, lo):
    return jnp.concatenate([ref[lo:lo + HALF, nth(HEAD, head)] for head in range(GROUP * kv, GROUP * (kv + 1))], axis=0)


P_DIMS = ((KV_HEADS, GROUP * HALF, HALF), (KV_HEADS, GROUP * HALF, SEQ))


def as_matrix(blocks):
    return blocks.reshape(8 * blocks.shape[1], blocks.shape[2])


class Ring:
    def __init__(self, me, ag, own, full, sems):
        self.me, self.ag, self.own, self.full, self.sems = me, ag, own, full, sems
        core, x_bit, y_bit = lax.rem(me, 2), lax.rem(me // 2, 2), me // 4
        self.pair, self.x_dev, self.y_dev = me + 1 - 2 * core, me + 2 - 4 * x_bit, me + 4 - 8 * y_bit

    def enter(self):
        barrier = pltpu.get_barrier_semaphore()
        for dev in (self.pair, self.x_dev, self.y_dev):
            pl.semaphore_signal(barrier, inc=1, device_id=(dev,), device_id_type=MESH)
        pl.semaphore_wait(barrier, 3)

    def copy(self, t, k):
        me, pair = self.me, self.pair
        one, two = (self.x_dev, self.y_dev) if self.ag[t].x_first else (self.y_dev, self.x_dev)
        blk = (me, me, me, one, one, two, one + two - me)[k]
        dev = (one, two, pair, two, pair, pair, pair)[k]
        src = self.own[t] if k < 3 else self.full[t].at[blk]
        return pltpu.make_async_remote_copy(src_ref=src, dst_ref=self.full[t].at[blk], send_sem=self.sems.at[t, k], recv_sem=self.sems.at[t, 7 + k], device_id=(dev,), device_id_type=MESH)

    def local(self, t):
        return pltpu.make_async_copy(self.own[t], self.full[t].at[self.me], self.sems.at[t, 14])

    def begin(self, group):
        for t in group:
            for k in range(3):
                self.copy(t, k).start()
            self.local(t).start()

    def forward(self, group):
        for t in group:
            self.copy(t, 0).wait_recv()
            self.copy(t, 3).start()
            self.copy(t, 4).start()
        for t in group:
            self.copy(t, 1).wait_recv()
            self.copy(t, 5).start()

    def end(self, group):
        for t in group:
            self.copy(t, 3).wait_recv()
            self.copy(t, 6).start()
        for t in group:
            for k in (2, 4, 5, 6):
                self.copy(t, k).wait_recv()
            for k in range(7):
                self.copy(t, k).wait_send()
            self.local(t).wait()


def attn_fwd_step(x32, wqkv, wo, gain, cos, sin, qkv_ref, p0_ref, p1_ref, o_ref):
    normed = (x32 * inv_rms(x32) * gain).astype(BF)
    proj = dot(normed, wqkv)
    for i in range(6):
        qkv_ref[0, :, nth(LANES, i)] = rope(proj[:, nth(LANES, i)], cos, sin).astype(BF)
    qkv_ref[0, :, V_COL:QKV] = proj[:, V_COL:QKV].astype(BF)
    half = HALF
    causal = lax.broadcasted_iota(jnp.int32, (GROUP * half, half), 0) % half >= lax.broadcasted_iota(jnp.int32, (GROUP * half, half), 1)
    for kv in range(KV_HEADS):
        keys = qkv_ref[0, :, DIM + HEAD * kv:DIM + HEAD * kv + HEAD]
        vals = qkv_ref[0, :, V_COL + HEAD * kv:V_COL + HEAD * kv + HEAD]
        for blk, p_ref in enumerate((p0_ref, p1_ref)):
            lo, length = half * blk, half * (blk + 1)
            s = dot(stack_heads(qkv_ref.at[0], kv, lo), keys[:length], ROWS) * HEAD ** -0.5
            diag = jnp.where(causal, s[:, lo:], MASK_VALUE)
            s = diag if blk == 0 else jnp.concatenate([s[:, :lo], diag], axis=1)
            e = jnp.exp(s - jnp.max(s, **LAST))
            p = (e * (1.0 / jnp.sum(e, **LAST))).astype(BF)
            p_ref[0, kv] = p
            o = dot(p, vals[:length]).astype(BF)
            for g in range(GROUP):
                head = GROUP * kv + g
                o_ref[0, lo:lo + half, nth(HEAD, head)] = o[nth(half, g)]
    return (x32 + dot(o_ref[0], wo)).astype(BF)


def forward(x_t, cos_t, sin_t, ag, cid):
    n = x_t.shape[0]
    n_g = len(ag)
    n_src = [len(g.srcs) for g in ag]
    head, mlp0, attn1, mlp1 = (0, 1, 2), (3, 4, 5), (6, 7), (8, 9, 10)

    def kernel(*refs):
        refs = list(refs)
        take = lambda k: [refs.pop(0) for _ in range(k)]
        x_ref, cos_ref, sin_ref = take(3)
        srcs = [take(k) for k in n_src]
        hid_ref, qkv_ref, p0_ref, p1_ref, o_ref, mid_ref, cos2_ref, sin2_ref, gains_ref = take(9)
        full = take(n_g)
        stream, mids, wqkv, wo, w1, w3, w2, g_all, act_ref = take(9)
        own = take(n_g)
        sems, load = take(2)
        step = pl.program_id(0)
        ring = Ring(lax.axis_index("fsdp"), ag, own, full, sems)

        def load_weights(pairs):
            copies = [pltpu.make_async_copy(full[t], dst, load.at[k]) for k, (t, dst) in enumerate(pairs)]
            for copy in copies:
                copy.start()
            for copy in copies:
                copy.wait()

        @pl.when(step == 0)
        def _():
            for t in head:
                ag[t].fill(srcs[t], own[t])
            ring.enter()
            ring.begin(head)
            for t in mlp0 + attn1 + mlp1:
                ag[t].fill(srcs[t], own[t])
            cos = cos_ref[:].T
            sin = sin_ref[:].T
            cos2_ref[:] = jnp.concatenate([cos] * 4, axis=1)
            sin2_ref[:] = jnp.concatenate([-sin, sin, -sin, sin], axis=1)
            ring.forward(head)
            ring.begin(mlp0)
            ring.end(head)
            load_weights([(0, wqkv), (1, wo), (2, g_all)])
            r = DIM // 8
            for d in range(8):
                for k in range(4):
                    gains_ref[k, :, nth(r, d)] = g_all[d, k:k + 1, :r].astype(F32)

        pl.when(step == n - 2)(lambda: ring.forward(mlp0[:2]))

        @pl.when(step == n - 1)
        def _():
            ring.forward(mlp0[2:])
            ring.begin(attn1)

        @pl.when(step == n)
        def _():
            ring.end(mlp0)
            load_weights([(3, w1), (4, w3), (5, w2)])

        @pl.when(step == n + 1)
        def _():
            ring.forward(attn1)
            ring.begin(mlp1)

        @pl.when(step == 2 * n)
        def _():
            ring.end(attn1)
            load_weights([(6, wqkv), (7, wo)])

        pl.when(step == 3 * n - 2)(lambda: ring.forward(mlp1[:2]))
        pl.when(step == 3 * n - 1)(lambda: ring.forward(mlp1[2:]))
        layer = step // (2 * n)
        seq = lax.rem(step, n)

        @pl.when(step < n)
        def _():
            stream[seq] = x_ref[0].T

        @pl.when((step < n) | (step >= 2 * n))
        def _():
            x = stream[seq]
            hid_ref[0] = x
            mid = attn_fwd_step(x.astype(F32), as_matrix(wqkv[:]), as_matrix(wo[:]), gains_ref[layer], cos2_ref[:], sin2_ref[:], qkv_ref, p0_ref, p1_ref, o_ref)
            mid_ref[0] = mid
            mids[seq] = mid

        @pl.when((step >= n) & (step < 2 * n))
        def _():
            h32 = mids[seq].astype(F32)
            normed = (h32 * inv_rms(h32) * gains_ref[2]).astype(BF)
            for c in range(0, FFN, CHUNK):
                gate = dot(normed, as_matrix(w1[:, :, c:c + CHUNK]))
                up = dot(normed, as_matrix(w3[:, :, c:c + CHUNK]))
                act_ref[:, c:c + CHUNK] = (gate * jax.nn.sigmoid(gate) * up).astype(BF)
            stream[seq] = (h32 + dot(act_ref[:], as_matrix(w2[:]))).astype(BF)

        pl.when(step == 3 * n - 1)(lambda: ring.end(mlp1))

    block = lambda i: jnp.where(i < n, i, jnp.where(i < 2 * n, n - 1, i - n))
    stacked = lambda dims: pl.BlockSpec((1,) + dims, lambda i: (block(i),) + origin(dims))
    saved = [(SEQ, DIM), (SEQ, QKV), P_DIMS[0], P_DIMS[1], (SEQ, DIM), (SEQ, DIM)]
    table = (SEQ, 2 * HEAD)
    bf_scratch = lambda dims: pltpu.VMEM(dims, BF)
    w_dims = [(8, ag[t].r, ag[t].c) for t in (0, 1, 3, 4, 5, 2)]
    return pl.pallas_call(
        kernel, grid=(3 * n,),
        in_specs=[pl.BlockSpec((1, DIM, SEQ), lambda i: (jnp.minimum(i, n - 1), 0, 0)), whole(cos_t.shape), whole(sin_t.shape)] + [spec for g in ag for spec in g.specs],
        out_specs=[stacked(dims) for dims in saved] + [whole(table), whole(table), whole((4, 1, DIM))] + [ANY] * n_g,
        out_shape=[shape((2 * n,) + dims, BF) for dims in saved] + [shape(table, F32), shape(table, F32), shape((4, 1, DIM), F32)] + [shape((8, g.r, g.c), BF) for g in ag],
        scratch_shapes=[bf_scratch((n, SEQ, DIM)), bf_scratch((n, SEQ, DIM))] + [bf_scratch(dims) for dims in w_dims] + [bf_scratch((SEQ, FFN))]
        + [bf_scratch((g.r, g.c)) for g in ag] + [pltpu.SemaphoreType.DMA((n_g, 15)), pltpu.SemaphoreType.DMA((3,))],
        compiler_params=params(collective_id=cid, has_side_effects=True), cost_estimate=cost(2e10, 4e7), name="forward",
    )(x_t, cos_t, sin_t, *[src for g in ag for src in g.srcs])


WIDE = 512
DOWN, GATE, UP = (6, 7), (8, 9), (10, 11)
TILES = FFN // WIDE


def mlp_bwd_body(step, last, core, ins, outs, scratch):
    h_ref, dy_ref, w1_ref, w3_ref, w2_ref, gain_ref = ins
    gm_ref, gg_ref, *y_ref = outs
    nt_ref, at_ref, act_ref, dgate_ref, dup_ref, dy_all, down_mine, down_theirs, gate_mine, gate_theirs, up_mine, up_theirs = scratch
    n = dy_all.shape[0] // SEQ
    gain = gain_ref[0]

    @pl.when(step < n)
    def _():
        h32 = h_ref[0].astype(F32)
        normed = (h32 * inv_rms(h32) * gain).astype(BF)
        tokens = pl.ds(pl.multiple_of(step * SEQ, SEQ), SEQ)
        nt_ref[:, tokens] = normed.T
        dy = dy_ref[0].T if y_ref else dy_ref[0]
        dy_all[tokens] = dy
        for c in range(0, FFN, CHUNK):
            cols = slice(c, c + CHUNK)
            gate = dot(normed, w1_ref[:, cols])
            up = dot(normed, w3_ref[:, cols])
            grad_act = dot(dy, w2_ref[cols, :], ROWS)
            sig = jax.nn.sigmoid(gate)
            silu = gate * sig
            act = (silu * up).astype(BF)
            if y_ref:
                act_ref[tokens, cols] = act
            at_ref[cols, tokens] = act.T
            dup_ref[tokens, cols] = (grad_act * silu).astype(BF)
            dgate_ref[tokens, cols] = (grad_act * up * sig * (1.0 + gate * (1.0 - sig))).astype(BF)

    @pl.when((step >= n) & (step < n + 4))
    def _():
        block = step - n
        span = 2 * FFN // 8
        full = dot(at_ref[pl.ds(pl.multiple_of(block * span, span), span)], dy_all[:])
        split_rows(full, core, down_mine.at[pl.ds(block, 1)], down_theirs.at[pl.ds(block, 1)])

    @pl.when((step >= n + 4) & (step < n + 4 + TILES))
    def _():
        cols = pl.ds(pl.multiple_of((step - n - 4) * WIDE, WIDE), WIDE)
        split_rows(dot(nt_ref[:], dgate_ref[:, cols]), core, gate_mine.at[:, :, cols], gate_theirs.at[:, :, cols])
        split_rows(dot(nt_ref[:], dup_ref[:, cols]), core, up_mine.at[:, :, cols], up_theirs.at[:, :, cols])

    @pl.when(step >= n + 4 + TILES)
    def _():
        tokens = pl.ds(pl.multiple_of((step - n - 4 - TILES) * SEQ, SEQ), SEQ)
        h32 = h_ref[0].astype(F32)
        if y_ref:
            y_ref[0][0] = (h32 + dot(act_ref[tokens], w2_ref[:])).astype(BF).T
        grad_normed = dot(dgate_ref[tokens], w1_ref[:], ROWS) + dot(dup_ref[tokens], w3_ref[:], ROWS)
        grad_h, grad_gain = rms_back(h32, inv_rms(h32), gain, grad_normed)
        gm_ref[0] = dy_all[tokens].astype(F32) + grad_h
        gg_ref[0] = grad_gain


def mlp_bwd(mid, dy, w1, w3, w2, gains, layer, with_out, parts, cid):
    n = dy.shape[0]
    base = layer * n
    tok = n * SEQ
    extra = 1 if with_out else 0
    r, rd = DIM // 8, FFN // 8
    tail = n + 4 + TILES
    steps = tail + n
    twice = pl.BlockSpec((1, SEQ, DIM), lambda i: (base + jnp.where(i < tail, jnp.minimum(i, n - 1), i - tail), 0, 0))
    early = pl.BlockSpec((1,) + dy.shape[1:], lambda i: (jnp.minimum(i, n - 1), 0, 0))
    late = lambda dims: pl.BlockSpec((1,) + dims, lambda i: (jnp.maximum(i - tail, 0),) + origin(dims))
    down_at = [n + 4, n + 6, steps]
    wide_at = [tail, steps]
    mine = [Part(True, rd // 2, DIM, "ca", down_at, local=DOWN), Part(False, rd // 2, DIM, "ca", down_at, local=DOWN, lo=rd // 2),
            Part(True, r, FFN, "c", wide_at, local=GATE), Part(False, r, FFN, "c", wide_at, local=UP)]
    return fused(
        mlp_bwd_body, steps, [mid, dy, w1, w3, w2, gains],
        [twice, early, whole(w1.shape), whole(w3.shape), whole(w2.shape), one_of((1, DIM), 2 + layer)],
        [shape((n, SEQ, DIM), F32), shape((n, 1, DIM), F32)] + [shape((n, DIM, SEQ), BF)] * extra,
        [late((SEQ, DIM)), late((1, DIM))] + [late((DIM, SEQ))] * extra,
        [pltpu.VMEM((DIM, tok), BF), pltpu.VMEM((FFN, tok), BF), pltpu.VMEM((tok if with_out else SEQ, FFN), BF), pltpu.VMEM((tok, FFN), BF), pltpu.VMEM((tok, FFN), BF), pltpu.VMEM((tok, DIM), BF)]
        + [pltpu.VMEM((4, rd, DIM), F32)] * 2 + [pltpu.VMEM((4, r, FFN), F32)] * 4,
        parts + mine, cid, "mlp_bwd", 2e10)


def split_rows(full, core, mine_ref, theirs_ref):
    blocks, r = mine_ref.shape[0], mine_ref.shape[1]

    @pl.when(core == 0)
    def _():
        for i in range(blocks):
            mine_ref[i] = full[2 * i * r:(2 * i + 1) * r]
            theirs_ref[i] = full[(2 * i + 1) * r:(2 * i + 2) * r]

    @pl.when(core == 1)
    def _():
        for i in range(blocks):
            theirs_ref[i] = full[2 * i * r:(2 * i + 1) * r]
            mine_ref[i] = full[(2 * i + 1) * r:(2 * i + 2) * r]


def attn_bwd_body(transposed, step, last, core, ins, outs, scratch):
    gm_ref, x_ref, qkv_ref, p0_ref, p1_ref, o_ref, wqkv_ref, wo_ref, gain_ref, cos_ref, sin_ref = ins
    dx_ref, gg_ref, qkv_mine, qkv_theirs, out_mine, out_theirs = outs
    do_ref, dqk_ref, dqkv_ref, acc_qkv, acc_out = scratch
    gm = gm_ref[0]
    gmb = gm.astype(BF)
    x32 = x_ref[0].astype(F32)
    inv = inv_rms(x32)
    gain = gain_ref[0]
    normed = (x32 * inv * gain).astype(BF)
    do_ref[:] = dot(gmb, wo_ref[:], ROWS).astype(BF)
    half = HALF
    for kv in range(KV_HEADS):
        kcol = DIM + HEAD * kv
        vcol = V_COL + HEAD * kv
        keys = qkv_ref[0, :, kcol:kcol + HEAD]
        vals = qkv_ref[0, :, vcol:vcol + HEAD]
        dk, dv = [], []
        for blk, p_ref in enumerate((p0_ref, p1_ref)):
            lo, length = half * blk, half * (blk + 1)
            p = p_ref[0, kv]
            d_o = stack_heads(do_ref, kv, lo)
            q = stack_heads(qkv_ref.at[0], kv, lo)
            dp = dot(d_o, vals[:length], ROWS)
            p32 = p.astype(F32)
            ds = (p32 * (dp - jnp.sum(p32 * dp, **LAST)) * HEAD ** -0.5).astype(BF)
            dq = dot(ds, keys[:length])
            for g in range(GROUP):
                head = GROUP * kv + g
                dqk_ref[lo:lo + half, nth(HEAD, head)] = dq[nth(half, g)]
            dk.append(dot(q, ds, COLS))
            dv.append(dot(d_o, p, COLS))
        dk, dv = [jnp.concatenate([a[0] + a[1][:, :half], a[1][:, half:]], axis=1).T for a in (dk, dv)]
        dqk_ref[:, kcol:kcol + HEAD] = dk
        dqkv_ref[:, vcol:vcol + HEAD] = dv.astype(BF)
    cos, sin = cos_ref[:], -sin_ref[:]
    for i in range(6):
        cols = nth(LANES, i)
        dqkv_ref[:, cols] = rope(dqk_ref[:, cols], cos, sin).astype(BF)
    grad_normed = dot(dqkv_ref[:], wqkv_ref[:], ROWS)
    grad_x, grad_gain = rms_back(x32, inv, gain, grad_normed)
    dx = (gm + grad_x).astype(BF)
    dx_ref[0] = dx.T if transposed else dx
    gg_ref[0] = grad_gain
    part_qkv = dot(normed, dqkv_ref[:], COLS)
    part_out = dot(o_ref[0], gmb, COLS)

    @pl.when(step == 0)
    def _():
        acc_qkv[:] = part_qkv
        acc_out[:] = part_out

    @pl.when(step > 0)
    def _():
        acc_qkv[:] += part_qkv
        acc_out[:] += part_out

    @pl.when(step == last)
    def _():
        split_rows(acc_qkv, core, qkv_mine, qkv_theirs)
        split_rows(acc_out, core, out_mine, out_theirs)


def attn_bwd(gm, saved, wqkv, wo, gains, cos, sin, layer, parts, cid):
    hid, qkv, p0, p1, o = saved
    n = gm.shape[0]
    base = layer * n
    r = DIM // 8
    dx, dx_spec = (shape((n, SEQ, DIM), BF), rows((SEQ, DIM))) if layer else (shape((n, DIM, SEQ), BF), rows((DIM, SEQ)))
    return fused(
        functools.partial(attn_bwd_body, layer == 0), n, [gm, hid, qkv, p0, p1, o, wqkv, wo, gains, cos, sin],
        [rows((SEQ, DIM)), rows((SEQ, DIM), base), rows((SEQ, QKV), base), rows(P_DIMS[0], base), rows(P_DIMS[1], base), rows((SEQ, DIM), base), whole(wqkv.shape), whole(wo.shape), one_of((1, DIM), layer), whole(cos.shape), whole(sin.shape)],
        [dx, shape((n, 1, DIM), F32), shape((4, r, QKV), F32), shape((4, r, QKV), F32), shape((4, r, DIM), F32), shape((4, r, DIM), F32)],
        [dx_spec, rows((1, DIM)), whole((4, r, QKV)), whole((4, r, QKV)), whole((4, r, DIM)), whole((4, r, DIM))],
        [pltpu.VMEM((SEQ, DIM), BF), pltpu.VMEM((SEQ, 768), F32), pltpu.VMEM((SEQ, QKV), BF), pltpu.VMEM((DIM, QKV), F32), pltpu.VMEM((DIM, DIM), F32)],
        parts, cid, "attn_bwd", 1e10)


def pick(stacked, index, axis):
    return lax.dynamic_index_in_dim(stacked, index, axis, keepdims=False)


def solution(mesh):
    shard_spec = P(None, "fsdp")
    batch_spec = P("fsdp")

    def local_step(w_query, w_key, w_value, w_out, w_gate, w_up, w_down, gain_attn, gain_mlp, rope_cos, rope_sin, x_in, y_cot):
        me = lax.axis_index("fsdp")
        bits = (me % 2, (me // 2) % 2, me // 4)
        num_layers = w_query.shape[0]
        attn_ag = lambda i: [gather_of(False, i, (w_query, w_key, w_value)), gather_of(True, i, (w_out,))]
        mlp_ag = lambda i: [gather_of(True, i, (w_gate,)), gather_of(False, i, (w_up,)), gather_of(i == 0, i, (w_down,))]
        merge = lambda v: v.reshape(-1, v.shape[2])
        ag = attn_ag(0) + [gather_gains(gain_attn, gain_mlp)] + mlp_ag(0) + attn_ag(1) + mlp_ag(1)
        hid, qkv, p0, p1, attn, mid, cos, sin, gains, *full = forward(jnp.swapaxes(x_in, 1, 2), rope_cos.T, rope_sin.T, ag, 2 * num_layers + 1)
        full = [merge(v) for v in full]
        weights = [full[:2] + full[3:6], full[6:]]
        grad = jnp.swapaxes(y_cot, 1, 2)
        grads = [None] * num_layers
        gain_grads = []
        y_out = None
        r, rd = w_query.shape[1], w_down.shape[1]
        done = {}
        wide, heads = [], []
        for i in reversed(range(num_layers)):
            qkv_w, out_w, gate_w, up_w, down_w = weights[i]
            last = i == num_layers - 1
            seqs = x_in.shape[0]
            at_b = [0, seqs + 4]
            at_cab = [0, 2, seqs + 4, 2 * seqs + 4 + TILES]
            parts = [Part(first == 0, r, width, "cab", at_cab, arrays=pair) for first, (width, pair) in enumerate(heads)]
            parts = [Part(first == 0, r, FFN, "b", at_b, arrays=[v]) for first, v in enumerate(wide)] + parts
            res = mlp_bwd(mid, grad, gate_w, up_w, down_w, gains, i, last, parts, 2 * i)
            gm, gg2 = res[:2]
            if last:
                y_out = res[2]
            rest = res[3 if last else 2:]
            done[i + 1] = list(rest[:len(parts)])
            down0, down1, gate_s, up_s = rest[len(parts):]
            parts = [Part(True, r, FFN, "a", [0, seqs], arrays=[gate_s]), Part(False, r, FFN, "a", [0, seqs], arrays=[up_s]),
                     Part(True, rd // 2, DIM, "b", [0, seqs], arrays=[down0]), Part(False, rd // 2, DIM, "b", [0, seqs], arrays=[down1])]
            res = attn_bwd(gm, (hid, qkv, p0, p1, attn), qkv_w, out_w, gains, cos, sin, i, parts, 2 * i + 1)
            grad, gg1, q_mine, q_theirs, o_mine, o_theirs = res[:6]
            wide = list(res[6:8])
            done[i, "down"] = res[8:10]
            heads = [(QKV, [q_mine, q_theirs]), (DIM, [o_mine, o_theirs])]
            gain_grads = [gg1.sum((0, 1)), gg2.sum((0, 1))] + gain_grads
        gsum = jnp.stack(gain_grads).reshape(2 * num_layers, 4, 2, r)
        gsum = jnp.pad(gsum.transpose(2, 1, 0, 3).reshape(2, 4, 2 * num_layers * r), ((0, 0), (0, 0), (0, 1024 - 2 * num_layers * r))).reshape(2, 4, 8, 128)
        parts = [Part(first == 0, r, FFN, "b", [1.5, 4], arrays=[v]) for first, v in enumerate(wide)]
        parts += [Part(first == 0, r, width, "cab", [0, 1, 2, 3], arrays=pair) for first, (width, pair) in enumerate(heads)]
        parts += [Part(True, 8, 128, "cab", [0, 1, 2, 3], arrays=[pick(gsum, bits[0], 0), pick(gsum, 1 - bits[0], 0)])]
        *done[0], gain_sums = fused(None, 1, [], [], [], [], [], parts, 2 * num_layers, "rs_tail", 1e6)
        s_gains = gain_sums.reshape(1024)[:2 * num_layers * r].reshape(2 * num_layers, r)
        for i in range(num_layers):
            s_gate, s_up, s_qkv, s_out = done[i]
            down0, down1 = done[i, "down"]
            grads[i] = (s_qkv[:, :576], s_qkv[:, 576:768], s_qkv[:, 768:960], s_out, s_gate, s_up, jnp.concatenate([down0, down1], 0))
        stacked = tuple(jnp.stack(parts) for parts in zip(*grads))
        return (jnp.swapaxes(y_out, 1, 2), jnp.swapaxes(grad, 1, 2)) + stacked + (s_gains[0::2], s_gains[1::2])

    in_specs = (shard_spec,) * 9 + (P(), P(), batch_spec, batch_spec)
    out_specs = (batch_spec, batch_spec) + (shard_spec,) * 9
    return jax.shard_map(local_step, mesh=mesh, in_specs=in_specs, out_specs=out_specs, check_vma=False)
```

```python
import functools

import jax
import jax.numpy as jnp
from jax import lax
from jax.experimental import pallas as pl
from jax.experimental.pallas import tpu as pltpu
from jax.sharding import PartitionSpec as P

NORM_EPS = 1e-5
MASK_VALUE = -1e30
HEAD = 64
LAST = dict(axis=-1, keepdims=True)
KV_HEADS = 3
GROUP = 3
SEQ = 256
DIM = 576
FFN = 1536
QKV = 960
BF = jnp.bfloat16
F32 = jnp.float32


ROWS = ((1,), (1,))
COLS = ((0,), (0,))
PAIR = range(2)
HALF = SEQ // 2
LANES = 128
VMEM_BYTES = 66 * 10 ** 6
V_COL = DIM + KV_HEADS * HEAD


def origin(dims):
    return (0,) * len(dims)


def nth(width, index):
    return slice(width * index, width * (index + 1))


def dot(a, b, dims=((1,), (0,))):
    return lax.dot_general(a, b, (dims, ((), ())), preferred_element_type=F32)


def params(**kw):
    return pltpu.CompilerParams(dimension_semantics=("arbitrary",), vmem_limit_bytes=VMEM_BYTES, **kw)


def cost(flops, bytes_accessed):
    return pl.CostEstimate(flops=int(flops), bytes_accessed=int(bytes_accessed), transcendentals=0)


def shape(dims, dtype):
    return jax.ShapeDtypeStruct(dims, dtype)


def whole(dims):
    return pl.BlockSpec(dims, lambda i: origin(dims), pipeline_mode=pl.Buffered(1))


def rows(dims, base=0):
    return pl.BlockSpec((1,) + dims, lambda i: (i + base,) + origin(dims))


def one_of(dims, index):
    return pl.BlockSpec((1,) + dims, lambda i: (index,) + origin(dims), pipeline_mode=pl.Buffered(1))


def inv_rms(vals32):
    return lax.rsqrt(jnp.mean(vals32 * vals32, **LAST) + NORM_EPS)


def rms_back(vals32, inv, gain, grad_normed):
    scaled = vals32 * inv
    grad_scaled = grad_normed * gain
    grad_gain = jnp.sum(grad_normed * scaled, axis=0, keepdims=True)
    return inv * (grad_scaled - scaled * jnp.mean(grad_scaled * scaled, **LAST)), grad_gain


def rope(vals32, cos, sin):
    lane = lax.broadcasted_iota(jnp.int32, vals32.shape, 1)
    swapped = jnp.where(lane % HEAD < HEAD // 2, pltpu.roll(vals32, 96, 1), pltpu.roll(vals32, 32, 1))
    return vals32 * cos + swapped * sin


MESH = pl.DeviceIdType.MESH
ANY = pl.BlockSpec(memory_space=pl.ANY)


class Part:
    def __init__(self, x_first, r, c, stages, at, arrays=(), local=(), lo=0):
        self.x_first, self.r, self.c, self.stages, self.at = x_first, r, c, stages, at
        self.arrays, self.local, self.lo = list(arrays), list(local), lo
        full, two, one = (4, r, c), (2, r, c), (r, c)
        self.result = {"c": full, "a": two, "b": one}[stages[-1]]
        self.bufs = {}
        if "c" in stages:
            self.bufs["recv_c"] = full
            if not local:
                self.bufs["mine"] = full
        if "a" in stages:
            self.bufs["recv_a"] = two
        if "b" in stages:
            self.bufs["recv_b"] = one
        if stages[0] != "c":
            self.bufs["keep"] = two if stages[0] == "a" else one


class Gather:
    def __init__(self, x_first, r, c, srcs, specs, fill):
        self.x_first, self.r, self.c, self.srcs, self.specs, self.fill = x_first, r, c, srcs, specs, fill


def gather_of(x_first, layer, masters):
    widths = [m.shape[2] for m in masters]

    def fill(refs, dst):
        lo = 0
        for ref, width in zip(refs, widths):
            dst[:, lo:lo + width] = ref[0].astype(BF)
            lo += width

    specs = [pl.BlockSpec((1,) + m.shape[1:], lambda i: (layer, 0, 0)) for m in masters]
    return Gather(x_first, masters[0].shape[1], sum(widths), list(masters), specs, fill)


def gather_gains(gain_attn, gain_mlp):
    layers, r = gain_attn.shape

    def fill(refs, dst):
        dst[:] = jnp.zeros(dst.shape, BF)
        dst[0:layers, 0:r] = refs[0][:].astype(BF)
        dst[layers:2 * layers, 0:r] = refs[1][:].astype(BF)

    return Gather(True, 16, 128, [gain_attn, gain_mlp], [whole((layers, r))] * 2, fill)


def fused(body, steps, ins, in_specs, outs, out_specs, scratch, parts, cid, name, flops):
    n_in, n_out, n_scr, n_p = len(ins), len(outs), len(scratch), len(parts)
    comm = n_p > 0
    last = steps - 1

    def kernel(*refs):
        refs = list(refs)
        take = lambda k: [refs.pop(0) for _ in range(k)]
        in_refs = take(n_in)
        p_in = [take(len(p.arrays)) for p in parts]
        out_refs = take(n_out)
        p_out = take(n_p)
        scr = take(n_scr)
        p_scr = [dict(zip(p.bufs, take(len(p.bufs)))) for p in parts]
        step = pl.program_id(0)
        me = lax.axis_index("fsdp")
        core, x_bit, y_bit = lax.rem(me, 2), lax.rem(me // 2, 2), me // 4
        if not comm:
            body(step, last, core, in_refs, out_refs, scr)
            return
        (p_sem,) = take(1)
        pair, x_dev, y_dev = me + 1 - 2 * core, me + 2 - 4 * x_bit, me + 4 - 8 * y_bit

        def remote(src, dst, send, recv, dev):
            return pltpu.make_async_remote_copy(src_ref=src, dst_ref=dst, send_sem=send, recv_sem=recv, device_id=(dev,), device_id_type=MESH)

        def stages_of(t):
            part, bufs, arrays, out = parts[t], p_scr[t], p_in[t], p_out[t]
            sem = lambda k: p_sem.at[t, k]
            if part.x_first:
                sent, kept, dev_a, bit, dev_b = (lambda j: 2 * j + 1 - x_bit), (lambda j: 2 * j + x_bit), x_dev, y_bit, y_dev
            else:
                sent, kept, dev_a, bit, dev_b = (lambda j: 2 * (1 - y_bit) + j), (lambda j: 2 * y_bit + j), y_dev, x_bit, x_dev
            first, end = part.stages[0], part.stages[-1]
            span = pl.ds(part.lo, part.r)

            def copy_c():
                theirs = scr[part.local[1]] if part.local else arrays[1]
                return remote(theirs.at[:, span], bufs["recv_c"], sem(1), sem(2), pair)

            def copy_mine():
                return pltpu.make_async_copy(arrays[0].at[:, span], bufs["mine"], sem(0))

            def copy_a(j):
                src = arrays[0] if first == "a" else bufs["recv_c"]
                return remote(src.at[sent(j)], bufs["recv_a"].at[j], sem(3 + j), sem(5 + j), dev_a)

            def copy_keep(j):
                if first == "b":
                    return pltpu.make_async_copy(arrays[0].at[bit], bufs["keep"], sem(7))
                return pltpu.make_async_copy(arrays[0].at[kept(j)], bufs["keep"].at[j], sem(7 + j))

            def copy_b():
                src = arrays[0] if first == "b" else bufs["recv_a"]
                return remote(src.at[1 - bit], bufs["recv_b"], sem(9), sem(10), dev_b)

            def copy_out():
                return pltpu.make_async_copy(bufs["recv_" + end], out, sem(11))

            def mine_block(i):
                return scr[part.local[0]][i, part.lo:part.lo + part.r] if part.local else bufs["mine"][i]

            def begin():
                if first == "c":
                    copy_c().start()
                    if not part.local:
                        copy_mine().start()
                elif first == "a":
                    for j in PAIR:
                        copy_a(j).start()
                    for j in PAIR:
                        copy_keep(j).start()
                else:
                    copy_b().start()
                    copy_keep(0).start()

            def done_c():
                copy_c().wait()
                if not part.local:
                    copy_mine().wait()
                sums = bufs["recv_c"]
                for j in PAIR:
                    sums[sent(j)] = sums[sent(j)] + mine_block(sent(j))
                    if end != "c":
                        copy_a(j).start()
                for j in PAIR:
                    sums[kept(j)] = sums[kept(j)] + mine_block(kept(j))
                if end == "c":
                    copy_out().start()

            def done_a():
                for j in PAIR:
                    copy_a(j).wait()
                    if first == "a":
                        copy_keep(j).wait()
                for j in PAIR:
                    bufs["recv_a"][j] = bufs["recv_a"][j] + (bufs["keep"][j] if first == "a" else bufs["recv_c"][kept(j)])
                if end == "a":
                    copy_out().start()
                else:
                    copy_b().start()

            def done_b():
                copy_b().wait()
                if first == "b":
                    copy_keep(0).wait()
                bufs["recv_b"][:] = bufs["recv_b"][:] + (bufs["keep"][:] if first == "b" else bufs["recv_a"][bit])
                copy_out().start()

            calls = [begin] + [{"c": done_c, "a": done_a, "b": done_b}[stage] for stage in part.stages]
            return list(zip(part.at, calls)), copy_out

        def enter():
            barrier = pltpu.get_barrier_semaphore()
            for dev in (pair, x_dev, y_dev):
                pl.semaphore_signal(barrier, inc=1, device_id=(dev,), device_id_type=MESH)
            pl.semaphore_wait(barrier, 3)

        events = [(-1, enter)]
        outs_of = []
        for t in range(n_p):
            calls, copy_out = stages_of(t)
            events += calls
            outs_of.append(copy_out)
        events.sort(key=lambda event: event[0])

        def leave():
            for copy_out in outs_of:
                copy_out().wait()

        events.append((float("inf"), leave))
        if steps == 1:
            for _, call in events:
                call()
            return

        def at_step(lo, hi):
            calls = [call for at, call in events if lo <= at < hi]

            def run():
                for call in calls:
                    call()

            return run, len(calls)

        for index in range(steps):
            run, count = at_step(-1 if index == 0 else index, index + 1)
            if count:
                pl.when(step == index)(run)
        body(step, last, core, in_refs, out_refs, scr)
        pl.when(step == last)(at_step(steps, float("inf"))[0])
        pl.when(step == last)(leave)

    args = list(ins)
    in_specs, out_specs, outs, scratch = list(in_specs), list(out_specs), list(outs), list(scratch)
    for part in parts:
        args += part.arrays
        in_specs += [ANY] * len(part.arrays)
        outs.append(shape(part.result, F32))
        out_specs.append(ANY)
    for part in parts:
        scratch += [pltpu.VMEM(dims, F32) for dims in part.bufs.values()]
    extra = {}
    if comm:
        scratch += [pltpu.SemaphoreType.DMA((n_p, 12))]
        extra = dict(collective_id=cid, has_side_effects=True)
    return pl.pallas_call(
        kernel, grid=(steps,), in_specs=in_specs, out_specs=out_specs, out_shape=outs, scratch_shapes=scratch,
        compiler_params=params(**extra), cost_estimate=cost(flops, 2e7), name=name)(*args)


CHUNK = 512


def stack_heads(ref, kv, lo):
    return jnp.concatenate([ref[lo:lo + HALF, nth(HEAD, head)] for head in range(GROUP * kv, GROUP * (kv + 1))], axis=0)


P_DIMS = ((KV_HEADS, GROUP * HALF, HALF), (KV_HEADS, GROUP * HALF, SEQ))


def as_matrix(blocks):
    return blocks.reshape(8 * blocks.shape[1], blocks.shape[2])


class Ring:
    def __init__(self, me, ag, own, full, sems):
        self.me, self.ag, self.own, self.full, self.sems = me, ag, own, full, sems
        core, x_bit, y_bit = lax.rem(me, 2), lax.rem(me // 2, 2), me // 4
        self.pair, self.x_dev, self.y_dev = me + 1 - 2 * core, me + 2 - 4 * x_bit, me + 4 - 8 * y_bit

    def enter(self):
        barrier = pltpu.get_barrier_semaphore()
        for dev in (self.pair, self.x_dev, self.y_dev):
            pl.semaphore_signal(barrier, inc=1, device_id=(dev,), device_id_type=MESH)
        pl.semaphore_wait(barrier, 3)

    def copy(self, t, k):
        me, pair = self.me, self.pair
        one, two = (self.x_dev, self.y_dev) if self.ag[t].x_first else (self.y_dev, self.x_dev)
        blk = (me, me, me, one, one, two, one + two - me)[k]
        dev = (one, two, pair, two, pair, pair, pair)[k]
        src = self.own[t] if k < 3 else self.full[t].at[blk]
        return pltpu.make_async_remote_copy(src_ref=src, dst_ref=self.full[t].at[blk], send_sem=self.sems.at[t, k], recv_sem=self.sems.at[t, 7 + k], device_id=(dev,), device_id_type=MESH)

    def local(self, t):
        return pltpu.make_async_copy(self.own[t], self.full[t].at[self.me], self.sems.at[t, 14])

    def begin(self, group):
        for t in group:
            for k in range(3):
                self.copy(t, k).start()
            self.local(t).start()

    def forward(self, group):
        for t in group:
            self.copy(t, 0).wait_recv()
            self.copy(t, 3).start()
            self.copy(t, 4).start()
        for t in group:
            self.copy(t, 1).wait_recv()
            self.copy(t, 5).start()

    def end(self, group):
        for t in group:
            self.copy(t, 3).wait_recv()
            self.copy(t, 6).start()
        for t in group:
            for k in (2, 4, 5, 6):
                self.copy(t, k).wait_recv()
            for k in range(7):
                self.copy(t, k).wait_send()
            self.local(t).wait()


def attn_fwd_step(x32, wqkv, wo, gain, cos, sin, qkv_ref, p0_ref, p1_ref, o_ref):
    normed = (x32 * inv_rms(x32) * gain).astype(BF)
    proj = dot(normed, wqkv)
    for i in range(6):
        qkv_ref[0, :, nth(LANES, i)] = rope(proj[:, nth(LANES, i)], cos, sin).astype(BF)
    qkv_ref[0, :, V_COL:QKV] = proj[:, V_COL:QKV].astype(BF)
    half = HALF
    causal = lax.broadcasted_iota(jnp.int32, (GROUP * half, half), 0) % half >= lax.broadcasted_iota(jnp.int32, (GROUP * half, half), 1)
    for kv in range(KV_HEADS):
        keys = qkv_ref[0, :, DIM + HEAD * kv:DIM + HEAD * kv + HEAD]
        vals = qkv_ref[0, :, V_COL + HEAD * kv:V_COL + HEAD * kv + HEAD]
        for blk, p_ref in enumerate((p0_ref, p1_ref)):
            lo, length = half * blk, half * (blk + 1)
            s = dot(stack_heads(qkv_ref.at[0], kv, lo), keys[:length], ROWS) * HEAD ** -0.5
            diag = jnp.where(causal, s[:, lo:], MASK_VALUE)
            s = diag if blk == 0 else jnp.concatenate([s[:, :lo], diag], axis=1)
            e = jnp.exp(s - jnp.max(s, **LAST))
            p = (e * (1.0 / jnp.sum(e, **LAST))).astype(BF)
            p_ref[0, kv] = p
            o = dot(p, vals[:length]).astype(BF)
            for g in range(GROUP):
                head = GROUP * kv + g
                o_ref[0, lo:lo + half, nth(HEAD, head)] = o[nth(half, g)]
    return (x32 + dot(o_ref[0], wo)).astype(BF)


def forward(x_t, cos_t, sin_t, ag, cid):
    n = x_t.shape[0]
    n_g = len(ag)
    n_src = [len(g.srcs) for g in ag]
    head, mlp0, attn1, mlp1 = (0, 1, 2), (3, 4, 5), (6, 7), (8, 9, 10)

    def kernel(*refs):
        refs = list(refs)
        take = lambda k: [refs.pop(0) for _ in range(k)]
        x_ref, cos_ref, sin_ref = take(3)
        srcs = [take(k) for k in n_src]
        hid_ref, qkv_ref, p0_ref, p1_ref, o_ref, mid_ref, cos2_ref, sin2_ref, gains_ref = take(9)
        full = take(n_g)
        stream, mids, wqkv, wo, w1, w3, w2, g_all, act_ref = take(9)
        own = take(n_g)
        sems, load = take(2)
        step = pl.program_id(0)
        ring = Ring(lax.axis_index("fsdp"), ag, own, full, sems)

        def load_weights(pairs):
            copies = [pltpu.make_async_copy(full[t], dst, load.at[k]) for k, (t, dst) in enumerate(pairs)]
            for copy in copies:
                copy.start()
            for copy in copies:
                copy.wait()

        @pl.when(step == 0)
        def _():
            for t in head:
                ag[t].fill(srcs[t], own[t])
            ring.enter()
            ring.begin(head)
            for t in mlp0 + attn1 + mlp1:
                ag[t].fill(srcs[t], own[t])
            cos = cos_ref[:].T
            sin = sin_ref[:].T
            cos2_ref[:] = jnp.concatenate([cos] * 4, axis=1)
            sin2_ref[:] = jnp.concatenate([-sin, sin, -sin, sin], axis=1)
            ring.forward(head)
            ring.begin(mlp0)
            ring.end(head)
            load_weights([(0, wqkv), (1, wo), (2, g_all)])
            r = DIM // 8
            for d in range(8):
                for k in range(4):
                    gains_ref[k, :, nth(r, d)] = g_all[d, k:k + 1, :r].astype(F32)

        pl.when(step == n - 2)(lambda: ring.forward(mlp0[:2]))

        @pl.when(step == n - 1)
        def _():
            ring.forward(mlp0[2:])
            ring.begin(attn1)

        @pl.when(step == n)
        def _():
            ring.end(mlp0)
            load_weights([(3, w1), (4, w3), (5, w2)])

        @pl.when(step == n + 1)
        def _():
            ring.forward(attn1)
            ring.begin(mlp1)

        @pl.when(step == 2 * n)
        def _():
            ring.end(attn1)
            load_weights([(6, wqkv), (7, wo)])

        pl.when(step == 3 * n - 2)(lambda: ring.forward(mlp1[:2]))
        pl.when(step == 3 * n - 1)(lambda: ring.forward(mlp1[2:]))
        layer = step // (2 * n)
        seq = lax.rem(step, n)

        @pl.when(step < n)
        def _():
            stream[seq] = x_ref[0].T

        @pl.when((step < n) | (step >= 2 * n))
        def _():
            x = stream[seq]
            hid_ref[0] = x
            mid = attn_fwd_step(x.astype(F32), as_matrix(wqkv[:]), as_matrix(wo[:]), gains_ref[layer], cos2_ref[:], sin2_ref[:], qkv_ref, p0_ref, p1_ref, o_ref)
            mid_ref[0] = mid
            mids[seq] = mid

        @pl.when((step >= n) & (step < 2 * n))
        def _():
            h32 = mids[seq].astype(F32)
            normed = (h32 * inv_rms(h32) * gains_ref[2]).astype(BF)
            for c in range(0, FFN, CHUNK):
                gate = dot(normed, as_matrix(w1[:, :, c:c + CHUNK]))
                up = dot(normed, as_matrix(w3[:, :, c:c + CHUNK]))
                act_ref[:, c:c + CHUNK] = (gate * jax.nn.sigmoid(gate) * up).astype(BF)
            stream[seq] = (h32 + dot(act_ref[:], as_matrix(w2[:]))).astype(BF)

        pl.when(step == 3 * n - 1)(lambda: ring.end(mlp1))

    block = lambda i: jnp.where(i < n, i, jnp.where(i < 2 * n, n - 1, i - n))
    stacked = lambda dims: pl.BlockSpec((1,) + dims, lambda i: (block(i),) + origin(dims))
    saved = [(SEQ, DIM), (SEQ, QKV), P_DIMS[0], P_DIMS[1], (SEQ, DIM), (SEQ, DIM)]
    table = (SEQ, 2 * HEAD)
    bf_scratch = lambda dims: pltpu.VMEM(dims, BF)
    w_dims = [(8, ag[t].r, ag[t].c) for t in (0, 1, 3, 4, 5, 2)]
    return pl.pallas_call(
        kernel, grid=(3 * n,),
        in_specs=[pl.BlockSpec((1, DIM, SEQ), lambda i: (jnp.minimum(i, n - 1), 0, 0)), whole(cos_t.shape), whole(sin_t.shape)] + [spec for g in ag for spec in g.specs],
        out_specs=[stacked(dims) for dims in saved] + [whole(table), whole(table), whole((4, 1, DIM))] + [ANY] * n_g,
        out_shape=[shape((2 * n,) + dims, BF) for dims in saved] + [shape(table, F32), shape(table, F32), shape((4, 1, DIM), F32)] + [shape((8, g.r, g.c), BF) for g in ag],
        scratch_shapes=[bf_scratch((n, SEQ, DIM)), bf_scratch((n, SEQ, DIM))] + [bf_scratch(dims) for dims in w_dims] + [bf_scratch((SEQ, FFN))]
        + [bf_scratch((g.r, g.c)) for g in ag] + [pltpu.SemaphoreType.DMA((n_g, 15)), pltpu.SemaphoreType.DMA((3,))],
        compiler_params=params(collective_id=cid, has_side_effects=True), cost_estimate=cost(2e10, 4e7), name="forward",
    )(x_t, cos_t, sin_t, *[src for g in ag for src in g.srcs])


WIDE = 512
DOWN, GATE, UP = (6, 7), (8, 9), (10, 11)
TILES = FFN // WIDE


def mlp_bwd_body(step, core, ins, outs, scratch):
    h_ref, dy_ref, w1_ref, w3_ref, w2_ref, gain_ref = ins
    gg_ref, *y_ref = outs
    nt_ref, at_ref, act_ref, dgate_ref, dup_ref, dy_all, down_mine, down_theirs, gate_mine, gate_theirs, up_mine, up_theirs, gm_ref = scratch
    n = dy_all.shape[0] // SEQ
    gain = gain_ref[0]

    @pl.when(step < n)
    def _():
        h32 = h_ref[0].astype(F32)
        normed = (h32 * inv_rms(h32) * gain).astype(BF)
        tokens = pl.ds(pl.multiple_of(step * SEQ, SEQ), SEQ)
        nt_ref[:, tokens] = normed.T
        dy = dy_ref[0].T if y_ref else dy_ref[0]
        dy_all[tokens] = dy
        for c in range(0, FFN, CHUNK):
            cols = slice(c, c + CHUNK)
            gate = dot(normed, w1_ref[:, cols])
            up = dot(normed, w3_ref[:, cols])
            grad_act = dot(dy, w2_ref[cols, :], ROWS)
            sig = jax.nn.sigmoid(gate)
            silu = gate * sig
            act = (silu * up).astype(BF)
            if y_ref:
                act_ref[tokens, cols] = act
            at_ref[cols, tokens] = act.T
            dup_ref[tokens, cols] = (grad_act * silu).astype(BF)
            dgate_ref[tokens, cols] = (grad_act * up * sig * (1.0 + gate * (1.0 - sig))).astype(BF)

    @pl.when((step >= n) & (step < n + 4))
    def _():
        block = step - n
        span = 2 * FFN // 8
        full = dot(at_ref[pl.ds(pl.multiple_of(block * span, span), span)], dy_all[:])
        split_rows(full, core, down_mine.at[pl.ds(block, 1)], down_theirs.at[pl.ds(block, 1)])

    @pl.when((step >= n + 4) & (step < n + 4 + TILES))
    def _():
        cols = pl.ds(pl.multiple_of((step - n - 4) * WIDE, WIDE), WIDE)
        split_rows(dot(nt_ref[:], dgate_ref[:, cols]), core, gate_mine.at[:, :, cols], gate_theirs.at[:, :, cols])
        split_rows(dot(nt_ref[:], dup_ref[:, cols]), core, up_mine.at[:, :, cols], up_theirs.at[:, :, cols])

    @pl.when((step >= n + 4 + TILES) & (step < n + 4 + TILES + n))
    def _():
        tokens = pl.ds(pl.multiple_of((step - n - 4 - TILES) * SEQ, SEQ), SEQ)
        h32 = h_ref[0].astype(F32)
        if y_ref:
            y_ref[0][0] = (h32 + dot(act_ref[tokens], w2_ref[:])).astype(BF).T
        grad_normed = dot(dgate_ref[tokens], w1_ref[:], ROWS) + dot(dup_ref[tokens], w3_ref[:], ROWS)
        grad_h, grad_gain = rms_back(h32, inv_rms(h32), gain, grad_normed)
        gm_ref[step - n - 4 - TILES] = dy_all[tokens].astype(F32) + grad_h
        gg_ref[0] = grad_gain


def split_rows(full, core, mine_ref, theirs_ref):
    blocks, r = mine_ref.shape[0], mine_ref.shape[1]

    @pl.when(core == 0)
    def _():
        for i in range(blocks):
            mine_ref[i] = full[2 * i * r:(2 * i + 1) * r]
            theirs_ref[i] = full[(2 * i + 1) * r:(2 * i + 2) * r]

    @pl.when(core == 1)
    def _():
        for i in range(blocks):
            theirs_ref[i] = full[2 * i * r:(2 * i + 1) * r]
            mine_ref[i] = full[(2 * i + 1) * r:(2 * i + 2) * r]


def attn_bwd_body(transposed, step, last, core, gm, ins, outs, scratch):
    x_ref, qkv_ref, p0_ref, p1_ref, o_ref, wqkv_ref, wo_ref, gain_ref, cos_ref, sin_ref = ins
    dx_ref, gg_ref, qkv_mine, qkv_theirs, out_mine, out_theirs = outs
    do_ref, dqk_ref, dqkv_ref, acc_qkv, acc_out, sems = scratch
    gmb = gm.astype(BF)
    x32 = x_ref[0].astype(F32)
    inv = inv_rms(x32)
    gain = gain_ref[0]
    normed = (x32 * inv * gain).astype(BF)
    do_ref[:] = dot(gmb, wo_ref[:], ROWS).astype(BF)
    half = HALF
    for kv in range(KV_HEADS):
        kcol = DIM + HEAD * kv
        vcol = V_COL + HEAD * kv
        keys = qkv_ref[0, :, kcol:kcol + HEAD]
        vals = qkv_ref[0, :, vcol:vcol + HEAD]
        dk, dv = [], []
        for blk, p_ref in enumerate((p0_ref, p1_ref)):
            lo, length = half * blk, half * (blk + 1)
            p = p_ref[0, kv]
            d_o = stack_heads(do_ref, kv, lo)
            q = stack_heads(qkv_ref.at[0], kv, lo)
            dp = dot(d_o, vals[:length], ROWS)
            p32 = p.astype(F32)
            ds = (p32 * (dp - jnp.sum(p32 * dp, **LAST)) * HEAD ** -0.5).astype(BF)
            dq = dot(ds, keys[:length])
            for g in range(GROUP):
                head = GROUP * kv + g
                dqk_ref[lo:lo + half, nth(HEAD, head)] = dq[nth(half, g)]
            dk.append(dot(q, ds, COLS))
            dv.append(dot(d_o, p, COLS))
        dk, dv = [jnp.concatenate([a[0] + a[1][:, :half], a[1][:, half:]], axis=1).T for a in (dk, dv)]
        dqk_ref[:, kcol:kcol + HEAD] = dk
        dqkv_ref[:, vcol:vcol + HEAD] = dv.astype(BF)
    cos, sin = cos_ref[:], -sin_ref[:]
    for i in range(6):
        cols = nth(LANES, i)
        dqkv_ref[:, cols] = rope(dqk_ref[:, cols], cos, sin).astype(BF)
    grad_normed = dot(dqkv_ref[:, :QKV], wqkv_ref[:], ROWS)
    grad_x, grad_gain = rms_back(x32, inv, gain, grad_normed)
    dx = (gm + grad_x).astype(BF)
    dx_ref[0] = dx.T if transposed else dx
    gg_ref[0] = grad_gain
    part_qkv = dot(normed, dqkv_ref[:, :QKV], COLS)
    part_out = dot(o_ref[0], gmb, COLS)

    @pl.when(step == 0)
    def _():
        acc_qkv[:] = part_qkv
        acc_out[:] = part_out

    @pl.when(step > 0)
    def _():
        acc_qkv[:] += part_qkv
        acc_out[:] += part_out

    @pl.when(step == last)
    def _():
        copies = []
        for acc, mine, theirs in ((acc_qkv, qkv_mine, qkv_theirs), (acc_out, out_mine, out_theirs)):
            r = mine.shape[1]
            for dst, side in ((mine, core), (theirs, 1 - core)):
                for i in range(4):
                    src = acc.at[pl.ds(pl.multiple_of((2 * i + side) * r, 8), r)]
                    copies.append(pltpu.make_async_copy(src, dst.at[i], sems.at[len(copies)]))
        for copy in copies:
            copy.start()
        for copy in copies:
            copy.wait()


def layer_bwd(mid, dy, saved, weights, gains, cos, sin, layer, with_out, parts, cid):
    hid, qkv, p0, p1, o = saved
    wqkv, wo, w1, w3, w2 = weights
    n = dy.shape[0]
    base = layer * n
    tok = n * SEQ
    extra = 1 if with_out else 0
    r, rd = DIM // 8, FFN // 8
    tail = n + 4 + TILES
    head = tail + n
    steps = head + n

    def body(step, last, core, ins, outs, scratch):
        mid_ref, dy_ref, w1_ref, w3_ref, w2_ref, gain_ref, *attn_ins = ins
        dx_ref, gg_attn, q_mine, q_theirs, o_mine, o_theirs, *mlp_outs = outs
        mlp_scratch, (dqk, acc_qkv, acc_out, sems) = scratch[:-4], scratch[-4:]
        attn_scratch = mlp_scratch[5].at[:SEQ], dqk, mlp_scratch[3].at[:SEQ], acc_qkv, acc_out, sems
        mlp_bwd_body(step, core, (mid_ref, dy_ref, w1_ref, w3_ref, w2_ref, gain_ref), mlp_outs, mlp_scratch)

        @pl.when(step >= head)
        def _():
            gm = mlp_scratch[-1][step - head]
            attn_bwd_body(layer == 0, step - head, n - 1, core, gm, attn_ins, (dx_ref, gg_attn, q_mine, q_theirs, o_mine, o_theirs), attn_scratch)

    def block(dims, first, offset=0):
        return pl.BlockSpec((1,) + dims, lambda i: (offset + jnp.clip(i - first, 0, n - 1),) + origin(dims))

    twice = pl.BlockSpec((1, SEQ, DIM), lambda i: (base + jnp.where(i < tail, jnp.minimum(i, n - 1), jnp.minimum(i - tail, n - 1)), 0, 0))
    down_at = [n + 4, n + 6, head + 1, steps]
    wide_at = [tail, tail + 2, steps]
    mine = [Part(True, rd // 2, DIM, "cab", down_at, local=DOWN), Part(False, rd // 2, DIM, "cab", down_at, local=DOWN, lo=rd // 2),
            Part(True, r, FFN, "ca", wide_at, local=GATE), Part(False, r, FFN, "ca", wide_at, local=UP)]
    dx = (DIM, SEQ) if layer == 0 else (SEQ, DIM)
    halves = [(4, r, QKV)] * 2 + [(4, r, DIM)] * 2
    return fused(
        body, steps, [mid, dy, w1, w3, w2, gains, hid, qkv, p0, p1, o, wqkv, wo, gains, cos, sin],
        [twice, block(dy.shape[1:], 0), whole(w1.shape), whole(w3.shape), whole(w2.shape), one_of((1, DIM), 2 + layer)]
        + [block(v.shape[1:], head, base) for v in saved] + [whole(wqkv.shape), whole(wo.shape), one_of((1, DIM), layer), whole(cos.shape), whole(sin.shape)],
        [shape((n,) + dx, BF), shape((n, 1, DIM), F32)] + [shape(dims, F32) for dims in halves] + [shape((n, 1, DIM), F32)] + [shape((n, DIM, SEQ), BF)] * extra,
        [block(dx, head), block((1, DIM), head)] + [ANY] * 4 + [block((1, DIM), tail)] + [block((DIM, SEQ), tail)] * extra,
        [pltpu.VMEM((DIM, tok), BF), pltpu.VMEM((FFN, tok), BF), pltpu.VMEM((tok, FFN) if with_out else (16, LANES), BF), pltpu.VMEM((tok, FFN), BF), pltpu.VMEM((tok, FFN), BF), pltpu.VMEM((tok, DIM), BF)]
        + [pltpu.VMEM((4, rd, DIM), F32)] * 2 + [pltpu.VMEM((4, r, FFN), F32)] * 4 + [pltpu.VMEM((n, SEQ, DIM), F32)]
        + [pltpu.VMEM((SEQ, V_COL), F32), pltpu.VMEM((DIM, QKV), F32), pltpu.VMEM((DIM, DIM), F32), pltpu.SemaphoreType.DMA((16,))],
        parts + mine, cid, "layer_bwd", 3e10)


def pick(stacked, index, axis):
    return lax.dynamic_index_in_dim(stacked, index, axis, keepdims=False)


def solution(mesh):
    shard_spec = P(None, "fsdp")
    batch_spec = P("fsdp")

    def local_step(w_query, w_key, w_value, w_out, w_gate, w_up, w_down, gain_attn, gain_mlp, rope_cos, rope_sin, x_in, y_cot):
        me = lax.axis_index("fsdp")
        bits = (me % 2, (me // 2) % 2, me // 4)
        num_layers = w_query.shape[0]
        attn_ag = lambda i: [gather_of(False, i, (w_query, w_key, w_value)), gather_of(True, i, (w_out,))]
        mlp_ag = lambda i: [gather_of(True, i, (w_gate,)), gather_of(False, i, (w_up,)), gather_of(i == 0, i, (w_down,))]
        merge = lambda v: v.reshape(-1, v.shape[2])
        ag = attn_ag(0) + [gather_gains(gain_attn, gain_mlp)] + mlp_ag(0) + attn_ag(1) + mlp_ag(1)
        hid, qkv, p0, p1, attn, mid, cos, sin, gains, *full = forward(jnp.swapaxes(x_in, 1, 2), rope_cos.T, rope_sin.T, ag, 2 * num_layers + 1)
        full = [merge(v) for v in full]
        weights = [full[:2] + full[3:6], full[6:]]
        grad = jnp.swapaxes(y_cot, 1, 2)
        grads = [None] * num_layers
        gain_grads = []
        y_out = None
        r, rd = w_query.shape[1], w_down.shape[1]
        done = {}
        wide, heads = [], []
        for i in reversed(range(num_layers)):
            last = i == num_layers - 1
            seqs = x_in.shape[0]
            at_b = [0, seqs + 4]
            at_cab = [0, 2, seqs + 5, 2 * seqs + 4 + TILES]
            parts = [Part(first == 0, r, FFN, "b", at_b, arrays=[v]) for first, v in enumerate(wide)]
            parts += [Part(first == 0, r, width, "cab", at_cab, arrays=pair) for first, (width, pair) in enumerate(heads)]
            res = layer_bwd(mid, grad, (hid, qkv, p0, p1, attn), weights[i], gains, cos, sin, i, last, parts, i)
            grad, gg1, q_mine, q_theirs, o_mine, o_theirs, gg2 = res[:7]
            if last:
                y_out = res[7]
            rest = res[8 if last else 7:]
            done[i + 1] = list(rest[:len(parts)])
            done[i, "down"] = rest[len(parts):len(parts) + 2]
            wide = list(rest[len(parts) + 2:])
            heads = [(QKV, [q_mine, q_theirs]), (DIM, [o_mine, o_theirs])]
            gain_grads = [gg1.sum((0, 1)), gg2.sum((0, 1))] + gain_grads
        gsum = jnp.stack(gain_grads).reshape(2 * num_layers, 4, 2, r)
        gsum = jnp.pad(gsum.transpose(2, 1, 0, 3).reshape(2, 4, 2 * num_layers * r), ((0, 0), (0, 0), (0, 1024 - 2 * num_layers * r))).reshape(2, 4, 8, 128)
        parts = [Part(first == 0, r, FFN, "b", [1.5, 4], arrays=[v]) for first, v in enumerate(wide)]
        parts += [Part(first == 0, r, width, "cab", [0, 1, 2, 3], arrays=pair) for first, (width, pair) in enumerate(heads)]
        parts += [Part(True, 8, 128, "cab", [0, 1, 2, 3], arrays=[pick(gsum, bits[0], 0), pick(gsum, 1 - bits[0], 0)])]
        *done[0], gain_sums = fused(None, 1, [], [], [], [], [], parts, 2 * num_layers, "rs_tail", 1e6)
        s_gains = gain_sums.reshape(1024)[:2 * num_layers * r].reshape(2 * num_layers, r)
        for i in range(num_layers):
            s_gate, s_up, s_qkv, s_out = done[i]
            down0, down1 = done[i, "down"]
            grads[i] = (s_qkv[:, :576], s_qkv[:, 576:768], s_qkv[:, 768:960], s_out, s_gate, s_up, jnp.concatenate([down0, down1], 0))
        stacked = tuple(jnp.stack(parts) for parts in zip(*grads))
        return (jnp.swapaxes(y_out, 1, 2), jnp.swapaxes(grad, 1, 2)) + stacked + (s_gains[0::2], s_gains[1::2])

    in_specs = (shard_spec,) * 9 + (P(), P(), batch_spec, batch_spec)
    out_specs = (batch_spec, batch_spec) + (shard_spec,) * 9
    return jax.shard_map(local_step, mesh=mesh, in_specs=in_specs, out_specs=out_specs, check_vma=False)
```

```python
import functools

import jax
import jax.numpy as jnp
from jax import lax
from jax.experimental import pallas as pl
from jax.experimental.pallas import tpu as pltpu
from jax.sharding import PartitionSpec as P

NORM_EPS = 1e-5
MASK_VALUE = -1e30
HEAD = 64
LAST = dict(axis=-1, keepdims=True)
KV_HEADS = 3
GROUP = 3
SEQ = 256
DIM = 576
FFN = 1536
QKV = 960
BF = jnp.bfloat16
F32 = jnp.float32


ROWS = ((1,), (1,))
COLS = ((0,), (0,))
PAIR = range(2)
HALF = SEQ // 2
LANES = 128
VMEM_BYTES = 66 * 10 ** 6
V_COL = DIM + KV_HEADS * HEAD


def origin(dims):
    return (0,) * len(dims)


def nth(width, index):
    return slice(width * index, width * (index + 1))


def dot(a, b, dims=((1,), (0,))):
    return lax.dot_general(a, b, (dims, ((), ())), preferred_element_type=F32)


def params(**kw):
    return pltpu.CompilerParams(dimension_semantics=("arbitrary",), vmem_limit_bytes=VMEM_BYTES, **kw)


def cost(flops, bytes_accessed):
    return pl.CostEstimate(flops=int(flops), bytes_accessed=int(bytes_accessed), transcendentals=0)


def shape(dims, dtype):
    return jax.ShapeDtypeStruct(dims, dtype)


def whole(dims):
    return pl.BlockSpec(dims, lambda i: origin(dims), pipeline_mode=pl.Buffered(1))


def rows(dims, base=0):
    return pl.BlockSpec((1,) + dims, lambda i: (i + base,) + origin(dims))


def one_of(dims, index):
    return pl.BlockSpec((1,) + dims, lambda i: (index,) + origin(dims), pipeline_mode=pl.Buffered(1))


def inv_rms(vals32):
    return lax.rsqrt(jnp.mean(vals32 * vals32, **LAST) + NORM_EPS)


def rms_back(vals32, inv, gain, grad_normed):
    scaled = vals32 * inv
    grad_scaled = grad_normed * gain
    grad_gain = jnp.sum(grad_normed * scaled, axis=0, keepdims=True)
    return inv * (grad_scaled - scaled * jnp.mean(grad_scaled * scaled, **LAST)), grad_gain


def rope(vals32, cos, sin):
    lane = lax.broadcasted_iota(jnp.int32, vals32.shape, 1)
    swapped = jnp.where(lane % HEAD < HEAD // 2, pltpu.roll(vals32, 96, 1), pltpu.roll(vals32, 32, 1))
    return vals32 * cos + swapped * sin


MESH = pl.DeviceIdType.MESH
ANY = pl.BlockSpec(memory_space=pl.ANY)


class Part:
    def __init__(self, x_first, r, c, stages, at, arrays=(), local=(), lo=0):
        self.x_first, self.r, self.c, self.stages, self.at = x_first, r, c, stages, at
        self.arrays, self.local, self.lo = list(arrays), list(local), lo
        full, two, one = (4, r, c), (2, r, c), (r, c)
        self.result = {"c": full, "a": two, "b": one}[stages[-1]]
        self.bufs = {}
        if "c" in stages:
            self.bufs["recv_c"] = full
            if not local:
                self.bufs["mine"] = full
        if "a" in stages:
            self.bufs["recv_a"] = two
        if "b" in stages:
            self.bufs["recv_b"] = one
        if stages[0] != "c":
            self.bufs["keep"] = two if stages[0] == "a" else one


class Gather:
    def __init__(self, x_first, r, c, srcs, specs, fill):
        self.x_first, self.r, self.c, self.srcs, self.specs, self.fill = x_first, r, c, srcs, specs, fill


def gather_of(x_first, layer, masters):
    widths = [m.shape[2] for m in masters]

    def fill(refs, dst):
        lo = 0
        for ref, width in zip(refs, widths):
            dst[:, lo:lo + width] = ref[0].astype(BF)
            lo += width

    specs = [pl.BlockSpec((1,) + m.shape[1:], lambda i: (layer, 0, 0)) for m in masters]
    return Gather(x_first, masters[0].shape[1], sum(widths), list(masters), specs, fill)


def gather_gains(gain_attn, gain_mlp):
    layers, r = gain_attn.shape

    def fill(refs, dst):
        dst[:] = jnp.zeros(dst.shape, BF)
        dst[0:layers, 0:r] = refs[0][:].astype(BF)
        dst[layers:2 * layers, 0:r] = refs[1][:].astype(BF)

    return Gather(True, 16, 128, [gain_attn, gain_mlp], [whole((layers, r))] * 2, fill)


def fused(body, steps, ins, in_specs, outs, out_specs, scratch, parts, cid, name, flops):
    n_in, n_out, n_scr, n_p = len(ins), len(outs), len(scratch), len(parts)
    comm = n_p > 0
    last = steps - 1

    def kernel(*refs):
        refs = list(refs)
        take = lambda k: [refs.pop(0) for _ in range(k)]
        in_refs = take(n_in)
        p_in = [take(len(p.arrays)) for p in parts]
        out_refs = take(n_out)
        p_out = take(n_p)
        scr = take(n_scr)
        p_scr = [dict(zip(p.bufs, take(len(p.bufs)))) for p in parts]
        step = pl.program_id(0)
        me = lax.axis_index("fsdp")
        core, x_bit, y_bit = lax.rem(me, 2), lax.rem(me // 2, 2), me // 4
        if not comm:
            body(step, last, core, in_refs, out_refs, scr)
            return
        (p_sem,) = take(1)
        pair, x_dev, y_dev = me + 1 - 2 * core, me + 2 - 4 * x_bit, me + 4 - 8 * y_bit

        def remote(src, dst, send, recv, dev):
            return pltpu.make_async_remote_copy(src_ref=src, dst_ref=dst, send_sem=send, recv_sem=recv, device_id=(dev,), device_id_type=MESH)

        def stages_of(t):
            part, bufs, arrays, out = parts[t], p_scr[t], p_in[t], p_out[t]
            sem = lambda k: p_sem.at[t, k]
            if part.x_first:
                sent, kept, dev_a, bit, dev_b = (lambda j: 2 * j + 1 - x_bit), (lambda j: 2 * j + x_bit), x_dev, y_bit, y_dev
            else:
                sent, kept, dev_a, bit, dev_b = (lambda j: 2 * (1 - y_bit) + j), (lambda j: 2 * y_bit + j), y_dev, x_bit, x_dev
            first, end = part.stages[0], part.stages[-1]
            span = pl.ds(part.lo, part.r)

            def copy_c():
                theirs = scr[part.local[1]] if part.local else arrays[1]
                return remote(theirs.at[:, span], bufs["recv_c"], sem(1), sem(2), pair)

            def copy_mine():
                return pltpu.make_async_copy(arrays[0].at[:, span], bufs["mine"], sem(0))

            def copy_a(j):
                src = arrays[0] if first == "a" else bufs["recv_c"]
                return remote(src.at[sent(j)], bufs["recv_a"].at[j], sem(3 + j), sem(5 + j), dev_a)

            def copy_keep(j):
                if first == "b":
                    return pltpu.make_async_copy(arrays[0].at[bit], bufs["keep"], sem(7))
                return pltpu.make_async_copy(arrays[0].at[kept(j)], bufs["keep"].at[j], sem(7 + j))

            def copy_b():
                src = arrays[0] if first == "b" else bufs["recv_a"]
                return remote(src.at[1 - bit], bufs["recv_b"], sem(9), sem(10), dev_b)

            def copy_out():
                return pltpu.make_async_copy(bufs["recv_" + end], out, sem(11))

            def mine_block(i):
                return scr[part.local[0]][i, part.lo:part.lo + part.r] if part.local else bufs["mine"][i]

            def begin():
                if first == "c":
                    copy_c().start()
                    if not part.local:
                        copy_mine().start()
                elif first == "a":
                    for j in PAIR:
                        copy_a(j).start()
                    for j in PAIR:
                        copy_keep(j).start()
                else:
                    copy_b().start()
                    copy_keep(0).start()

            def done_c():
                copy_c().wait()
                if not part.local:
                    copy_mine().wait()
                sums = bufs["recv_c"]
                for j in PAIR:
                    sums[sent(j)] = sums[sent(j)] + mine_block(sent(j))
                    if end != "c":
                        copy_a(j).start()
                for j in PAIR:
                    sums[kept(j)] = sums[kept(j)] + mine_block(kept(j))
                if end == "c":
                    copy_out().start()

            def done_a():
                for j in PAIR:
                    copy_a(j).wait()
                    if first == "a":
                        copy_keep(j).wait()
                for j in PAIR:
                    bufs["recv_a"][j] = bufs["recv_a"][j] + (bufs["keep"][j] if first == "a" else bufs["recv_c"][kept(j)])
                if end == "a":
                    copy_out().start()
                else:
                    copy_b().start()

            def done_b():
                copy_b().wait()
                if first == "b":
                    copy_keep(0).wait()
                bufs["recv_b"][:] = bufs["recv_b"][:] + (bufs["keep"][:] if first == "b" else bufs["recv_a"][bit])
                copy_out().start()

            calls = [begin] + [{"c": done_c, "a": done_a, "b": done_b}[stage] for stage in part.stages]
            return list(zip(part.at, calls)), copy_out

        def enter():
            barrier = pltpu.get_barrier_semaphore()
            for dev in (pair, x_dev, y_dev):
                pl.semaphore_signal(barrier, inc=1, device_id=(dev,), device_id_type=MESH)
            pl.semaphore_wait(barrier, 3)

        events = [(-1, enter)]
        outs_of = []
        for t in range(n_p):
            calls, copy_out = stages_of(t)
            events += calls
            outs_of.append(copy_out)
        events.sort(key=lambda event: event[0])

        def leave():
            for copy_out in outs_of:
                copy_out().wait()

        events.append((float("inf"), leave))
        if steps == 1:
            for _, call in events:
                call()
            return

        def at_step(lo, hi):
            calls = [call for at, call in events if lo <= at < hi]

            def run():
                for call in calls:
                    call()

            return run, len(calls)

        for index in range(steps):
            run, count = at_step(-1 if index == 0 else index, index + 1)
            if count:
                pl.when(step == index)(run)
        body(step, last, core, in_refs, out_refs, scr)
        pl.when(step == last)(at_step(steps, float("inf"))[0])
        pl.when(step == last)(leave)

    args = list(ins)
    in_specs, out_specs, outs, scratch = list(in_specs), list(out_specs), list(outs), list(scratch)
    for part in parts:
        args += part.arrays
        in_specs += [ANY] * len(part.arrays)
        outs.append(shape(part.result, F32))
        out_specs.append(ANY)
    for part in parts:
        scratch += [pltpu.VMEM(dims, F32) for dims in part.bufs.values()]
    extra = {}
    if comm:
        scratch += [pltpu.SemaphoreType.DMA((n_p, 12))]
        extra = dict(collective_id=cid, has_side_effects=True)
    return pl.pallas_call(
        kernel, grid=(steps,), in_specs=in_specs, out_specs=out_specs, out_shape=outs, scratch_shapes=scratch,
        compiler_params=params(**extra), cost_estimate=cost(flops, 2e7), name=name)(*args)


CHUNK = 512


def stack_heads(ref, kv, lo):
    return jnp.concatenate([ref[lo:lo + HALF, nth(HEAD, head)] for head in range(GROUP * kv, GROUP * (kv + 1))], axis=0)


P_DIMS = ((KV_HEADS, GROUP * HALF, HALF), (KV_HEADS, GROUP * HALF, SEQ))


def as_matrix(blocks):
    return blocks.reshape(8 * blocks.shape[1], blocks.shape[2])


class Ring:
    def __init__(self, me, ag, own, full, sems):
        self.me, self.ag, self.own, self.full, self.sems = me, ag, own, full, sems
        core, x_bit, y_bit = lax.rem(me, 2), lax.rem(me // 2, 2), me // 4
        self.pair, self.x_dev, self.y_dev = me + 1 - 2 * core, me + 2 - 4 * x_bit, me + 4 - 8 * y_bit

    def enter(self):
        barrier = pltpu.get_barrier_semaphore()
        for dev in (self.pair, self.x_dev, self.y_dev):
            pl.semaphore_signal(barrier, inc=1, device_id=(dev,), device_id_type=MESH)
        pl.semaphore_wait(barrier, 3)

    def copy(self, t, k):
        me, pair = self.me, self.pair
        one, two = (self.x_dev, self.y_dev) if self.ag[t].x_first else (self.y_dev, self.x_dev)
        blk = (me, me, me, one, one, two, one + two - me)[k]
        dev = (one, two, pair, two, pair, pair, pair)[k]
        src = self.own[t] if k < 3 else self.full[t].at[blk]
        return pltpu.make_async_remote_copy(src_ref=src, dst_ref=self.full[t].at[blk], send_sem=self.sems.at[t, k], recv_sem=self.sems.at[t, 7 + k], device_id=(dev,), device_id_type=MESH)

    def local(self, t):
        return pltpu.make_async_copy(self.own[t], self.full[t].at[self.me], self.sems.at[t, 14])

    def begin(self, group):
        for t in group:
            for k in range(3):
                self.copy(t, k).start()
            self.local(t).start()

    def forward(self, group):
        for t in group:
            self.copy(t, 0).wait_recv()
            self.copy(t, 3).start()
            self.copy(t, 4).start()
        for t in group:
            self.copy(t, 1).wait_recv()
            self.copy(t, 5).start()

    def end(self, group):
        for t in group:
            self.copy(t, 3).wait_recv()
            self.copy(t, 6).start()
        for t in group:
            for k in (2, 4, 5, 6):
                self.copy(t, k).wait_recv()
            for k in range(7):
                self.copy(t, k).wait_send()
            self.local(t).wait()


def attn_fwd_step(x32, wqkv, wo, gain, cos, sin, qkv_ref, p0_ref, p1_ref, o_ref):
    normed = (x32 * inv_rms(x32) * gain).astype(BF)
    proj = dot(normed, wqkv)
    for i in range(6):
        qkv_ref[0, :, nth(LANES, i)] = rope(proj[:, nth(LANES, i)], cos, sin).astype(BF)
    qkv_ref[0, :, V_COL:QKV] = proj[:, V_COL:QKV].astype(BF)
    half = HALF
    causal = lax.broadcasted_iota(jnp.int32, (GROUP * half, half), 0) % half >= lax.broadcasted_iota(jnp.int32, (GROUP * half, half), 1)
    for kv in range(KV_HEADS):
        keys = qkv_ref[0, :, DIM + HEAD * kv:DIM + HEAD * kv + HEAD]
        vals = qkv_ref[0, :, V_COL + HEAD * kv:V_COL + HEAD * kv + HEAD]
        for blk, p_ref in enumerate((p0_ref, p1_ref)):
            lo, length = half * blk, half * (blk + 1)
            s = dot(stack_heads(qkv_ref.at[0], kv, lo), keys[:length], ROWS) * HEAD ** -0.5
            diag = jnp.where(causal, s[:, lo:], MASK_VALUE)
            s = diag if blk == 0 else jnp.concatenate([s[:, :lo], diag], axis=1)
            e = jnp.exp(s - jnp.max(s, **LAST))
            p = (e * (1.0 / jnp.sum(e, **LAST))).astype(BF)
            p_ref[0, kv] = p
            o = dot(p, vals[:length]).astype(BF)
            for g in range(GROUP):
                head = GROUP * kv + g
                o_ref[0, lo:lo + half, nth(HEAD, head)] = o[nth(half, g)]
    return (x32 + dot(o_ref[0], wo)).astype(BF)


def forward(x_t, cos_t, sin_t, ag, cid):
    n = x_t.shape[0]
    n_g = len(ag)
    n_src = [len(g.srcs) for g in ag]
    head, mlp0, attn1, mlp1 = (0, 1, 2), (3, 4, 5), (6, 7), (8, 9, 10)

    def kernel(*refs):
        refs = list(refs)
        take = lambda k: [refs.pop(0) for _ in range(k)]
        x_ref, cos_ref, sin_ref = take(3)
        srcs = [take(k) for k in n_src]
        hid_ref, qkv_ref, p0_ref, p1_ref, o_ref, mid_ref, cos2_ref, sin2_ref, gains_ref = take(9)
        full = take(n_g)
        stream, mids, wqkv, wo, w1, w3, w2, g_all, act_ref = take(9)
        own = take(n_g)
        sems, load = take(2)
        step = pl.program_id(0)
        ring = Ring(lax.axis_index("fsdp"), ag, own, full, sems)

        def load_weights(pairs):
            copies = [pltpu.make_async_copy(full[t], dst, load.at[k]) for k, (t, dst) in enumerate(pairs)]
            for copy in copies:
                copy.start()
            for copy in copies:
                copy.wait()

        @pl.when(step == 0)
        def _():
            for t in head:
                ag[t].fill(srcs[t], own[t])
            ring.enter()
            ring.begin(head)
            for t in mlp0 + attn1 + mlp1:
                ag[t].fill(srcs[t], own[t])
            cos = cos_ref[:].T
            sin = sin_ref[:].T
            cos2_ref[:] = jnp.concatenate([cos] * 4, axis=1)
            sin2_ref[:] = jnp.concatenate([-sin, sin, -sin, sin], axis=1)
            ring.forward(head)
            ring.begin(mlp0)
            ring.end(head)
            load_weights([(0, wqkv), (1, wo), (2, g_all)])
            r = DIM // 8
            for d in range(8):
                for k in range(4):
                    gains_ref[k, :, nth(r, d)] = g_all[d, k:k + 1, :r].astype(F32)

        @pl.when(step == n - 2)
        def _():
            ring.forward(mlp0[:2])

        @pl.when(step == n - 1)
        def _():
            ring.forward(mlp0[2:])
            ring.begin(attn1)

        @pl.when(step == n)
        def _():
            ring.end(mlp0)
            ring.begin(mlp1[:1])
            load_weights([(3, w1), (4, w3), (5, w2)])

        @pl.when(step == n + 1)
        def _():
            ring.forward(attn1)
            ring.begin(mlp1[1:])

        @pl.when(step == 2 * n)
        def _():
            ring.end(attn1)
            load_weights([(6, wqkv), (7, wo)])

        @pl.when(step == 2 * n + 1)
        def _():
            ring.forward(mlp1[:1])

        @pl.when(step == 3 * n - 2)
        def _():
            ring.forward(mlp1[1:2])

        @pl.when(step == 3 * n - 1)
        def _():
            ring.forward(mlp1[2:])

        layer = step // (2 * n)
        seq = lax.rem(step, n)

        @pl.when(step < n)
        def _():
            stream[seq] = x_ref[0].T

        @pl.when((step < n) | (step >= 2 * n))
        def _():
            x = stream[seq]
            hid_ref[0] = x
            mid = attn_fwd_step(x.astype(F32), as_matrix(wqkv[:]), as_matrix(wo[:]), gains_ref[layer], cos2_ref[:], sin2_ref[:], qkv_ref, p0_ref, p1_ref, o_ref)
            mid_ref[0] = mid
            mids[seq] = mid

        @pl.when((step >= n) & (step < 2 * n))
        def _():
            h32 = mids[seq].astype(F32)
            normed = (h32 * inv_rms(h32) * gains_ref[2]).astype(BF)
            for c in range(0, FFN, CHUNK):
                gate = dot(normed, as_matrix(w1[:, :, c:c + CHUNK]))
                up = dot(normed, as_matrix(w3[:, :, c:c + CHUNK]))
                act_ref[:, c:c + CHUNK] = (gate * jax.nn.sigmoid(gate) * up).astype(BF)
            stream[seq] = (h32 + dot(act_ref[:], as_matrix(w2[:]))).astype(BF)

        pl.when(step == 3 * n - 1)(lambda: ring.end(mlp1))

    block = lambda i: jnp.where(i < n, i, jnp.where(i < 2 * n, n - 1, i - n))
    stacked = lambda dims: pl.BlockSpec((1,) + dims, lambda i: (block(i),) + origin(dims))
    saved = [(SEQ, DIM), (SEQ, QKV), P_DIMS[0], P_DIMS[1], (SEQ, DIM), (SEQ, DIM)]
    table = (SEQ, 2 * HEAD)
    bf_scratch = lambda dims: pltpu.VMEM(dims, BF)
    w_dims = [(8, ag[t].r, ag[t].c) for t in (0, 1, 3, 4, 5, 2)]
    return pl.pallas_call(
        kernel, grid=(3 * n,),
        in_specs=[pl.BlockSpec((1, DIM, SEQ), lambda i: (jnp.minimum(i, n - 1), 0, 0)), whole(cos_t.shape), whole(sin_t.shape)] + [spec for g in ag for spec in g.specs],
        out_specs=[stacked(dims) for dims in saved] + [whole(table), whole(table), whole((4, 1, DIM))] + [ANY] * n_g,
        out_shape=[shape((2 * n,) + dims, BF) for dims in saved] + [shape(table, F32), shape(table, F32), shape((4, 1, DIM), F32)] + [shape((8, g.r, g.c), BF) for g in ag],
        scratch_shapes=[bf_scratch((n, SEQ, DIM)), bf_scratch((n, SEQ, DIM))] + [bf_scratch(dims) for dims in w_dims] + [bf_scratch((SEQ, FFN))]
        + [bf_scratch((g.r, g.c)) for g in ag] + [pltpu.SemaphoreType.DMA((n_g, 15)), pltpu.SemaphoreType.DMA((3,))],
        compiler_params=params(collective_id=cid, has_side_effects=True), cost_estimate=cost(2e10, 4e7), name="forward",
    )(x_t, cos_t, sin_t, *[src for g in ag for src in g.srcs])


WIDE = 512
DOWN, GATE, UP = (6, 7), (8, 9), (10, 11)
TILES = FFN // WIDE


def mlp_bwd_body(step, core, ins, outs, scratch):
    h_ref, dy_ref, w1_ref, w3_ref, w2_ref, gain_ref = ins
    gg_ref, *y_ref = outs
    nt_ref, at_ref, act_ref, dgate_ref, dup_ref, dy_all, down_mine, down_theirs, gate_mine, gate_theirs, up_mine, up_theirs, gm_ref = scratch
    n = dy_all.shape[0] // SEQ
    gain = gain_ref[0]

    @pl.when(step < n)
    def _():
        h32 = h_ref[0].astype(F32)
        normed = (h32 * inv_rms(h32) * gain).astype(BF)
        tokens = pl.ds(pl.multiple_of(step * SEQ, SEQ), SEQ)
        nt_ref[:, tokens] = normed.T
        dy = dy_ref[0].T if y_ref else dy_ref[0]
        dy_all[tokens] = dy
        for c in range(0, FFN, CHUNK):
            cols = slice(c, c + CHUNK)
            gate = dot(normed, w1_ref[:, cols])
            up = dot(normed, w3_ref[:, cols])
            grad_act = dot(dy, w2_ref[cols, :], ROWS)
            sig = jax.nn.sigmoid(gate)
            silu = gate * sig
            act = (silu * up).astype(BF)
            if y_ref:
                act_ref[tokens, cols] = act
            at_ref[cols, tokens] = act.T
            dup_ref[tokens, cols] = (grad_act * silu).astype(BF)
            dgate_ref[tokens, cols] = (grad_act * up * sig * (1.0 + gate * (1.0 - sig))).astype(BF)

    @pl.when((step >= n) & (step < n + 4))
    def _():
        block = step - n
        span = 2 * FFN // 8
        full = dot(at_ref[pl.ds(pl.multiple_of(block * span, span), span)], dy_all[:])
        split_rows(full, core, down_mine.at[pl.ds(block, 1)], down_theirs.at[pl.ds(block, 1)])

    @pl.when((step >= n + 4) & (step < n + 4 + TILES))
    def _():
        cols = pl.ds(pl.multiple_of((step - n - 4) * WIDE, WIDE), WIDE)
        split_rows(dot(nt_ref[:], dgate_ref[:, cols]), core, gate_mine.at[:, :, cols], gate_theirs.at[:, :, cols])
        split_rows(dot(nt_ref[:], dup_ref[:, cols]), core, up_mine.at[:, :, cols], up_theirs.at[:, :, cols])

    @pl.when((step >= n + 4 + TILES) & (step < n + 4 + TILES + n))
    def _():
        tokens = pl.ds(pl.multiple_of((step - n - 4 - TILES) * SEQ, SEQ), SEQ)
        h32 = h_ref[0].astype(F32)
        if y_ref:
            y_ref[0][0] = (h32 + dot(act_ref[tokens], w2_ref[:])).astype(BF).T
        grad_normed = dot(dgate_ref[tokens], w1_ref[:], ROWS) + dot(dup_ref[tokens], w3_ref[:], ROWS)
        grad_h, grad_gain = rms_back(h32, inv_rms(h32), gain, grad_normed)
        gm_ref[step - n - 4 - TILES] = dy_all[tokens].astype(F32) + grad_h
        gg_ref[0] = grad_gain


def split_rows(full, core, mine_ref, theirs_ref):
    blocks, r = mine_ref.shape[0], mine_ref.shape[1]

    @pl.when(core == 0)
    def _():
        for i in range(blocks):
            mine_ref[i] = full[2 * i * r:(2 * i + 1) * r]
            theirs_ref[i] = full[(2 * i + 1) * r:(2 * i + 2) * r]

    @pl.when(core == 1)
    def _():
        for i in range(blocks):
            theirs_ref[i] = full[2 * i * r:(2 * i + 1) * r]
            mine_ref[i] = full[(2 * i + 1) * r:(2 * i + 2) * r]


def attn_bwd_body(transposed, step, last, core, gm, ins, outs, scratch):
    x_ref, qkv_ref, p0_ref, p1_ref, o_ref, wqkv_ref, wo_ref, gain_ref, cos_ref, sin_ref = ins
    dx_ref, gg_ref, qkv_mine, qkv_theirs, out_mine, out_theirs = outs
    do_ref, dqk_ref, dqkv_ref, acc_qkv, acc_out, sems = scratch
    gmb = gm.astype(BF)
    x32 = x_ref[0].astype(F32)
    inv = inv_rms(x32)
    gain = gain_ref[0]
    normed = (x32 * inv * gain).astype(BF)
    do_ref[:] = dot(gmb, wo_ref[:], ROWS).astype(BF)
    half = HALF
    for kv in range(KV_HEADS):
        kcol = DIM + HEAD * kv
        vcol = V_COL + HEAD * kv
        keys = qkv_ref[0, :, kcol:kcol + HEAD]
        vals = qkv_ref[0, :, vcol:vcol + HEAD]
        dk, dv = [], []
        for blk, p_ref in enumerate((p0_ref, p1_ref)):
            lo, length = half * blk, half * (blk + 1)
            p = p_ref[0, kv]
            d_o = stack_heads(do_ref, kv, lo)
            q = stack_heads(qkv_ref.at[0], kv, lo)
            dp = dot(d_o, vals[:length], ROWS)
            p32 = p.astype(F32)
            ds = (p32 * (dp - jnp.sum(p32 * dp, **LAST)) * HEAD ** -0.5).astype(BF)
            dq = dot(ds, keys[:length])
            for g in range(GROUP):
                head = GROUP * kv + g
                dqk_ref[lo:lo + half, nth(HEAD, head)] = dq[nth(half, g)]
            dk.append(dot(q, ds, COLS))
            dv.append(dot(d_o, p, COLS))
        dk, dv = [jnp.concatenate([a[0] + a[1][:, :half], a[1][:, half:]], axis=1).T for a in (dk, dv)]
        dqk_ref[:, kcol:kcol + HEAD] = dk
        dqkv_ref[:, vcol:vcol + HEAD] = dv.astype(BF)
    cos, sin = cos_ref[:], -sin_ref[:]
    for i in range(6):
        cols = nth(LANES, i)
        dqkv_ref[:, cols] = rope(dqk_ref[:, cols], cos, sin).astype(BF)
    grad_normed = dot(dqkv_ref[:, :QKV], wqkv_ref[:], ROWS)
    grad_x, grad_gain = rms_back(x32, inv, gain, grad_normed)
    dx = (gm + grad_x).astype(BF)
    dx_ref[0] = dx.T if transposed else dx
    gg_ref[0] = grad_gain
    part_qkv = dot(normed, dqkv_ref[:, :QKV], COLS)
    part_out = dot(o_ref[0], gmb, COLS)

    @pl.when(step == 0)
    def _():
        acc_qkv[:] = part_qkv
        acc_out[:] = part_out

    @pl.when(step > 0)
    def _():
        acc_qkv[:] += part_qkv
        acc_out[:] += part_out

    @pl.when(step == last)
    def _():
        copies = []
        for acc, mine, theirs in ((acc_qkv, qkv_mine, qkv_theirs), (acc_out, out_mine, out_theirs)):
            r = mine.shape[1]
            for dst, side in ((mine, core), (theirs, 1 - core)):
                for i in range(4):
                    src = acc.at[pl.ds(pl.multiple_of((2 * i + side) * r, 8), r)]
                    copies.append(pltpu.make_async_copy(src, dst.at[i], sems.at[len(copies)]))
        for copy in copies:
            copy.start()
        for copy in copies:
            copy.wait()


def layer_bwd(mid, dy, saved, weights, gains, cos, sin, layer, with_out, parts, cid):
    hid, qkv, p0, p1, o = saved
    wqkv, wo, w1, w3, w2 = weights
    n = dy.shape[0]
    base = layer * n
    tok = n * SEQ
    extra = 1 if with_out else 0
    r, rd = DIM // 8, FFN // 8
    tail = n + 4 + TILES
    head = tail + n
    steps = head + n

    def body(step, last, core, ins, outs, scratch):
        mid_ref, dy_ref, w1_ref, w3_ref, w2_ref, gain_ref, *attn_ins = ins
        dx_ref, gg_attn, q_mine, q_theirs, o_mine, o_theirs, *mlp_outs = outs
        mlp_scratch, (dqk, acc_qkv, acc_out, sems) = scratch[:-4], scratch[-4:]
        attn_scratch = mlp_scratch[5].at[:SEQ], dqk, mlp_scratch[3].at[:SEQ], acc_qkv, acc_out, sems
        mlp_bwd_body(step, core, (mid_ref, dy_ref, w1_ref, w3_ref, w2_ref, gain_ref), mlp_outs, mlp_scratch)

        @pl.when(step >= head)
        def _():
            gm = mlp_scratch[-1][step - head]
            attn_bwd_body(layer == 0, step - head, n - 1, core, gm, attn_ins, (dx_ref, gg_attn, q_mine, q_theirs, o_mine, o_theirs), attn_scratch)

    def block(dims, first, offset=0):
        return pl.BlockSpec((1,) + dims, lambda i: (offset + jnp.clip(i - first, 0, n - 1),) + origin(dims))

    twice = pl.BlockSpec((1, SEQ, DIM), lambda i: (base + jnp.where(i < tail, jnp.minimum(i, n - 1), jnp.minimum(i - tail, n - 1)), 0, 0))
    down_at = [n + 4, n + 6, head + 1, steps]
    wide_at = [tail, tail + 2, steps]
    mine = [Part(True, rd // 2, DIM, "cab", down_at, local=DOWN), Part(False, rd // 2, DIM, "cab", down_at, local=DOWN, lo=rd // 2),
            Part(True, r, FFN, "ca", wide_at, local=GATE), Part(False, r, FFN, "ca", wide_at, local=UP)]
    dx = (DIM, SEQ) if layer == 0 else (SEQ, DIM)
    halves = [(4, r, QKV)] * 2 + [(4, r, DIM)] * 2
    return fused(
        body, steps, [mid, dy, w1, w3, w2, gains, hid, qkv, p0, p1, o, wqkv, wo, gains, cos, sin],
        [twice, block(dy.shape[1:], 0), whole(w1.shape), whole(w3.shape), whole(w2.shape), one_of((1, DIM), 2 + layer)]
        + [block(v.shape[1:], head, base) for v in saved] + [whole(wqkv.shape), whole(wo.shape), one_of((1, DIM), layer), whole(cos.shape), whole(sin.shape)],
        [shape((n,) + dx, BF), shape((n, 1, DIM), F32)] + [shape(dims, F32) for dims in halves] + [shape((n, 1, DIM), F32)] + [shape((n, DIM, SEQ), BF)] * extra,
        [block(dx, head), block((1, DIM), head)] + [ANY] * 4 + [block((1, DIM), tail)] + [block((DIM, SEQ), tail)] * extra,
        [pltpu.VMEM((DIM, tok), BF), pltpu.VMEM((FFN, tok), BF), pltpu.VMEM((tok, FFN) if with_out else (16, LANES), BF), pltpu.VMEM((tok, FFN), BF), pltpu.VMEM((tok, FFN), BF), pltpu.VMEM((tok, DIM), BF)]
        + [pltpu.VMEM((4, rd, DIM), F32)] * 2 + [pltpu.VMEM((4, r, FFN), F32)] * 4 + [pltpu.VMEM((n, SEQ, DIM), F32)]
        + [pltpu.VMEM((SEQ, V_COL), F32), pltpu.VMEM((DIM, QKV), F32), pltpu.VMEM((DIM, DIM), F32), pltpu.SemaphoreType.DMA((16,))],
        parts + mine, cid, "layer_bwd", 3e10)


def pack_kernel(*refs):
    layers = refs[:6], refs[6:12]
    gain_sums, y_ref, dx_ref, wq, wk, wv, wo, wg, wu, wd, g1, g2, y_out, dx_out = refs[12:]
    y_out[:] = y_ref[:]
    dx_out[:] = dx_ref[:]
    for i, (gate, up, qkv, out, down0, down1) in enumerate(layers):
        wq[i], wk[i], wv[i] = qkv[:, :DIM], qkv[:, DIM:DIM + wk.shape[2]], qkv[:, DIM + wk.shape[2]:]
        wo[i], wg[i], wu[i] = out[:], gate[:], up[:]
        g1[i:i + 1] = gain_sums[2 * i:2 * i + 1, :g1.shape[1]]
        g2[i:i + 1] = gain_sums[2 * i + 1:2 * i + 2, :g2.shape[1]]
        half = down0.shape[0]
        wd[i, :half] = down0[:]
        wd[i, half:] = down1[:]


def pack(parts, shapes):
    vmem = pl.BlockSpec(memory_space=pltpu.VMEM)
    return pl.pallas_call(
        pack_kernel, in_specs=[vmem] * len(parts), out_specs=[vmem] * len(shapes), out_shape=shapes,
        compiler_params=pltpu.CompilerParams(vmem_limit_bytes=VMEM_BYTES), cost_estimate=cost(1e6, 7e6), name="pack")(*parts)


def pick(stacked, index, axis):
    return lax.dynamic_index_in_dim(stacked, index, axis, keepdims=False)


def solution(mesh):
    shard_spec = P(None, "fsdp")
    batch_spec = P("fsdp")

    def local_step(w_query, w_key, w_value, w_out, w_gate, w_up, w_down, gain_attn, gain_mlp, rope_cos, rope_sin, x_in, y_cot):
        me = lax.axis_index("fsdp")
        bits = (me % 2, (me // 2) % 2, me // 4)
        num_layers = w_query.shape[0]
        attn_ag = lambda i: [gather_of(False, i, (w_query, w_key, w_value)), gather_of(True, i, (w_out,))]
        mlp_ag = lambda i: [gather_of(True, i, (w_gate,)), gather_of(False, i, (w_up,)), gather_of(i == 0, i, (w_down,))]
        merge = lambda v: v.reshape(-1, v.shape[2])
        ag = attn_ag(0) + [gather_gains(gain_attn, gain_mlp)] + mlp_ag(0) + attn_ag(1) + mlp_ag(1)
        hid, qkv, p0, p1, attn, mid, cos, sin, gains, *full = forward(jnp.swapaxes(x_in, 1, 2), rope_cos.T, rope_sin.T, ag, 2 * num_layers + 1)
        full = [merge(v) for v in full]
        weights = [full[:2] + full[3:6], full[6:]]
        grad = jnp.swapaxes(y_cot, 1, 2)
        gain_grads = []
        y_out = None
        r, rd = w_query.shape[1], w_down.shape[1]
        done = {}
        wide, heads = [], []
        for i in reversed(range(num_layers)):
            last = i == num_layers - 1
            seqs = x_in.shape[0]
            at_b = [0, seqs + 4]
            at_cab = [0, 2, seqs + 5, 2 * seqs + 4 + TILES]
            parts = [Part(first == 0, r, FFN, "b", at_b, arrays=[v]) for first, v in enumerate(wide)]
            parts += [Part(first == 0, r, width, "cab", at_cab, arrays=pair) for first, (width, pair) in enumerate(heads)]
            res = layer_bwd(mid, grad, (hid, qkv, p0, p1, attn), weights[i], gains, cos, sin, i, last, parts, i)
            grad, gg1, q_mine, q_theirs, o_mine, o_theirs, gg2 = res[:7]
            if last:
                y_out = res[7]
            rest = res[8 if last else 7:]
            done[i + 1] = list(rest[:len(parts)])
            done[i, "down"] = rest[len(parts):len(parts) + 2]
            wide = list(rest[len(parts) + 2:])
            heads = [(QKV, [q_mine, q_theirs]), (DIM, [o_mine, o_theirs])]
            gain_grads = [gg1.sum((0, 1)), gg2.sum((0, 1))] + gain_grads
        gsum = jnp.stack(gain_grads).reshape(-1, 4, 2, r).transpose(2, 1, 0, 3)
        gsum = jnp.pad(gsum, ((0, 0), (0, 0), (0, 8 - gsum.shape[2]), (0, LANES - r)))
        parts = [Part(first == 0, r, FFN, "b", [1.5, 4], arrays=[v]) for first, v in enumerate(wide)]
        parts += [Part(first == 0, r, width, "cab", [0, 1, 2, 3], arrays=pair) for first, (width, pair) in enumerate(heads)]
        parts += [Part(True, 8, 128, "cab", [0, 1, 2, 3], arrays=[pick(gsum, bits[0], 0), pick(gsum, 1 - bits[0], 0)])]
        *done[0], gain_sums = fused(None, 1, [], [], [], [], [], parts, 2 * num_layers, "rs_tail", 1e6)
        masters = (w_query, w_key, w_value, w_out, w_gate, w_up, w_down, gain_attn, gain_mlp)
        last_parts = [v for i in range(num_layers) for v in (*done[i], *done[i, "down"])] + [gain_sums, y_out, grad]
        *stacked, y_out, grad = pack(last_parts, [shape(m.shape, F32) for m in masters] + [shape(v.shape, BF) for v in (y_out, grad)])
        return (jnp.swapaxes(y_out, 1, 2), jnp.swapaxes(grad, 1, 2), *stacked)

    in_specs = (shard_spec,) * 9 + (P(), P(), batch_spec, batch_spec)
    out_specs = (batch_spec, batch_spec) + (shard_spec,) * 9
    return jax.shard_map(local_step, mesh=mesh, in_specs=in_specs, out_specs=out_specs, check_vma=False)
```
